128 devices in a mesh: group: 16 (over x, z_lo, core), head: 8 (over y, z_hi).
Axes of the slice: x: 4, y: 4, z: 4 (z_hi: 2, z_lo: 2; z = z_hi * 2 + z_lo), core: 2. Of those that a mesh axis runs over, the one named last changes fastest.
Arguments:
- hidden_in: bfloat16 [256, 2560], P('group'), may hold values from -6 to 6
- ssm_state: float32 [256, 80, 64, 128], P('group', 'head'), may hold values from -6 to 6
- conv_x_state: bfloat16 [256, 3, 5120], P('group', None, 'head'), may hold values from -6 to 6
- conv_bc_state: bfloat16 [256, 3, 256], P('group'), may hold values from -6 to 6
- token_ids: int32 [256], P('group'), may hold values from 0 to 25599
- ref_logits: bfloat16 [256, 25600], P('group', 'head'), may hold values from -15 to 350
- in_z: bfloat16 [2560, 5120], P('group', 'head'), may hold values from -0.125 to 0.125
- in_x: bfloat16 [2560, 5120], P('group', 'head'), may hold values from -0.125 to 0.125
- in_bc: bfloat16 [2560, 256], P('group'), may hold values from -0.125 to 0.125
- in_dt: bfloat16 [2560, 80], P('group', 'head'), may hold values from -0.125 to 0.125
- out_t: bfloat16 [2560, 5120], P('group', 'head'), may hold values from -0.078125 to 0.078125
- lm_head: bfloat16 [25600, 2560], P('head', 'group'), may hold values from -6 to 6
- conv_wx: float32 [4, 5120], P(None, 'head'), may hold values from -3 to 3
- conv_bx: float32 [5120], P('head'), may hold values from -1.5 to 1.5
- conv_wbc: float32 [4, 256], replicated, may hold values from -3 to 3
- conv_bbc: float32 [256], replicated, may hold values from -1.5 to 1.5
- dt_bias: float32 [80], P('head'), may hold values from -4 to -1
- a_log: float32 [80], P('head'), may hold values from 0 to 2.77
- skip_gain: float32 [80], P('head'), may hold values from 0.5 to 1.5
- norm_in: float32 [2560], replicated, may hold values from 0.5 to 1.5
- norm_gain: float32 [5120], P('head'), may hold values from 0.5 to 1.5
- final_gain: float32 [2560], replicated, may hold values from 0.5 to 1.5
Outputs:
- new_state: float32 [256, 80, 64, 128], P('group', 'head')
- divergence: float32 [256], P('group')
- token_logprob: float32 [256], P('group')
- roll_z: bfloat16 [2560, 5120], P(None, 'head')
- roll_x: bfloat16 [2560, 5120], P(None, 'head')
- roll_bc: bfloat16 [2560, 256], replicated
- roll_dt: bfloat16 [2560, 80], P(None, 'head')
- roll_out: bfloat16 [2560, 5120], P(None, 'head')
The draws below stay inside these ranges and needn't reach their ends.
All inputs are finite; a program needn't handle non-finite values.
Results may differ from the reference program's by a relative error of at most 0.0102.
Values may be sent and summed in bfloat16 or wider, within the bound.
A program may use at most 128 MiB of HBM per device.

```python
import math
import jax
import jax.numpy as jnp
from jax import lax

D = 2560
H = 80
P_SIZE = 64
N = 128
KCONV = 4
V = 25600
SEQS = 16
DI = 5120
SEQ_ALL = 256
N_GROUP = 16


def draw_lm_head(key, part):
    subkeys = jax.random.split(key, 1)
    values = jax.random.normal(subkeys[0], (V, D), jnp.float32) * (3.0 / math.sqrt(D))
    return jnp.clip(values, -6.0, 6.0).astype(jnp.bfloat16)


def draw_ref_logits(key, part):
    subkeys = jax.random.split(key, 1)
    total_rows = SEQS * N_GROUP
    values = jnp.clip(jax.random.normal(subkeys[0], (total_rows, V), jnp.float32) * 3.0, -15.0, 15.0)
    return values.astype(jnp.bfloat16)


def place_ends(drawn, key, least, largest):
    place = [jax.random.randint(jax.random.fold_in(key, axis), (), 0, length) for axis, length in enumerate(drawn.shape)]
    longest = drawn.shape.index(max(drawn.shape))
    neighbour = place[:longest] + [(place[longest] + 1) % drawn.shape[longest]] + place[longest + 1:]
    return drawn.at[tuple(place)].set(least).at[tuple(neighbour)].set(largest)


def level_of(key, shape, pieces, smallest, top_value):
    level = 1.0
    for axis_at, shards_of in pieces:
        steps = jax.random.uniform(jax.random.fold_in(jax.random.fold_in(key, 6), axis_at), (shards_of,), jnp.float32, smallest / len(pieces), top_value / len(pieces))
        level = level * jnp.repeat(jnp.exp(steps), shape[axis_at] // shards_of).reshape((-1,) + (1,) * (len(shape) - 1 - axis_at))
    return level


def scatter_about(key, extent, scale, limit, pieces=(), held_as=jnp.bfloat16):
    entries = scale * jax.random.normal(key, extent, jnp.float32)
    if pieces:
        entries = entries * level_of(key, extent, pieces, -0.22, 0.18)
    return jnp.clip(entries, -limit, limit).astype(held_as)


def setup_inputs(seed: int = 0) -> dict:
    arg_keys = jax.random.split(jax.random.key(seed), 23)
    hidden_in = scatter_about(arg_keys[0], (SEQ_ALL, D), 1.0, 6.0, ((0, 16),))
    ssm_state = scatter_about(arg_keys[1], (SEQ_ALL, H, P_SIZE, N), 1.0, 6.0, ((0, 16), (1, 8)), jnp.float32)
    conv_x_state = scatter_about(arg_keys[2], (SEQ_ALL, KCONV - 1, DI), 1.0, 6.0, ((0, 16), (2, 8)))
    conv_bc_state = scatter_about(arg_keys[3], (SEQ_ALL, KCONV - 1, 2 * N), 1.0, 6.0, ((0, 16),))
    token_ids = place_ends(jax.random.randint(arg_keys[4], (SEQ_ALL,), 0, V), jax.random.fold_in(arg_keys[4], 1), 0, V - 1).astype(jnp.int32)
    ref_logits = draw_ref_logits(jax.random.fold_in(arg_keys[22], 71), 0)
    in_z = scatter_about(arg_keys[6], (D, DI), D ** -0.5, 0.125, ((0, 16), (1, 8)))
    in_x = scatter_about(arg_keys[7], (D, DI), D ** -0.5, 0.125, ((0, 16), (1, 8)))
    in_bc = scatter_about(arg_keys[8], (D, 2 * N), D ** -0.5, 0.125, ((0, 16),))
    in_dt = scatter_about(arg_keys[9], (D, H), D ** -0.5, 0.125, ((0, 16), (1, 8)))
    out_t = scatter_about(arg_keys[10], (D, DI), DI ** -0.5, 0.078125, ((0, 16), (1, 8)))
    lm_head = draw_lm_head(jax.random.fold_in(arg_keys[22], 71), 0)
    conv_wx = scatter_about(arg_keys[12], (KCONV, DI), KCONV ** -0.5, 3.0, ((1, 8),), jnp.float32)
    conv_bx = scatter_about(arg_keys[13], (DI,), 0.3, 1.5, ((0, 8),), jnp.float32)
    conv_wbc = scatter_about(arg_keys[14], (KCONV, 2 * N), KCONV ** -0.5, 3.0, (), jnp.float32)
    conv_bbc = scatter_about(arg_keys[15], (2 * N,), 0.3, 1.5, (), jnp.float32)
    dt_bias = jnp.clip(-4.0 + 3.0 * jax.random.uniform(arg_keys[16], (H,), jnp.float32) ** level_of(arg_keys[16], (H,), ((0, 8),), -0.2, 0.2), -4.0, -1.0)
    a_log = jnp.clip(2.77 * jax.random.uniform(arg_keys[17], (H,), jnp.float32) ** level_of(arg_keys[17], (H,), ((0, 8),), -0.2, 0.2), 0.0, 2.77)
    skip_gain = jnp.clip(0.5 + 1.0 * jax.random.uniform(arg_keys[18], (H,), jnp.float32) ** level_of(arg_keys[18], (H,), ((0, 8),), -0.2, 0.2), 0.5, 1.5)
    norm_in = jnp.clip(1.0 + 0.1 * jax.random.normal(arg_keys[19], (D,), jnp.float32), 0.5, 1.5)
    norm_gain = jnp.clip(1.0 + 0.1 * jax.random.normal(arg_keys[20], (DI,), jnp.float32), 0.5, 1.5)
    final_gain = jnp.clip(1.0 + 0.1 * jax.random.normal(arg_keys[21], (D,), jnp.float32), 0.5, 1.5)
    return {"hidden_in": hidden_in, "ssm_state": ssm_state, "conv_x_state": conv_x_state, "conv_bc_state": conv_bc_state, "token_ids": token_ids, "ref_logits": ref_logits, "in_z": in_z, "in_x": in_x, "in_bc": in_bc, "in_dt": in_dt, "out_t": out_t, "lm_head": lm_head, "conv_wx": conv_wx, "conv_bx": conv_bx, "conv_wbc": conv_wbc, "conv_bbc": conv_bbc, "dt_bias": dt_bias, "a_log": a_log, "skip_gain": skip_gain, "norm_in": norm_in, "norm_gain": norm_gain, "final_gain": final_gain}


EPSILON = 1e-05

def rms_norm(values, gain):
    return values * lax.rsqrt(lax.optimization_barrier(jnp.mean(values * values, axis=-1, keepdims=True)) + EPSILON) * gain

def causal_conv(history, newest, taps, offset):
    window = jnp.concatenate([history, newest[:, None, :]], axis=1).astype(jnp.float32)
    return jax.nn.silu(lax.optimization_barrier(jnp.sum(window * taps[None, :, :], axis=1)) + offset)

def reference(hidden_in, ssm_state, conv_x_state, conv_bc_state, token_ids, ref_logits, in_z, in_x, in_bc, in_dt, out_t, lm_head, conv_wx, conv_bx, conv_wbc, conv_bbc, dt_bias, a_log, skip_gain, norm_in, norm_gain, final_gain):
    stream_in = hidden_in.astype(jnp.float32)
    normed = rms_norm(stream_in, norm_in).astype(jnp.bfloat16)
    gate_branch = jnp.dot(normed, in_z, preferred_element_type=jnp.float32).astype(jnp.bfloat16)
    x_branch = jnp.dot(normed, in_x, preferred_element_type=jnp.float32).astype(jnp.bfloat16)
    bc_branch = jnp.dot(normed, in_bc, preferred_element_type=jnp.float32).astype(jnp.bfloat16)
    step_raw = jnp.dot(normed, in_dt, preferred_element_type=jnp.float32).astype(jnp.bfloat16)
    x_conv = causal_conv(conv_x_state, x_branch, conv_wx, conv_bx)
    bc_conv = causal_conv(conv_bc_state, bc_branch, conv_wbc, conv_bbc)
    b_vals = bc_conv[:, :N]
    c_vals = bc_conv[:, N:]
    step = jax.nn.softplus(step_raw.astype(jnp.float32) + dt_bias)
    decay = jnp.exp(-step * jnp.exp(a_log))
    seq_count = x_conv.shape[0]
    x_heads = x_conv.reshape(seq_count, H, P_SIZE)
    inflow = (step[:, :, None] * x_heads)[:, :, :, None] * b_vals[:, None, None, :]
    new_state = decay[:, :, None, None] * ssm_state + inflow
    ssm_out = jnp.einsum('shpn,sn->shp', new_state, c_vals, precision=lax.Precision.HIGHEST)
    ssm_out = (ssm_out + skip_gain[None, :, None] * x_heads).reshape(seq_count, H * P_SIZE)
    gated = ssm_out * jax.nn.silu(gate_branch.astype(jnp.float32))
    gated_out = rms_norm(gated, norm_gain).astype(jnp.bfloat16)
    mixed = lax.dot_general(gated_out, out_t, (((1,), (1,)), ((), ())), preferred_element_type=jnp.float32)
    final_hidden = rms_norm(stream_in + mixed, final_gain).astype(jnp.bfloat16)
    logits = lax.dot_general(final_hidden, lm_head, (((1,), (1,)), ((), ())), preferred_element_type=jnp.float32)
    lse_roll = jax.nn.logsumexp(logits, axis=-1)
    reference_rows = ref_logits.astype(jnp.float32)
    lse_ref = jax.nn.logsumexp(reference_rows, axis=-1)
    log_ref = reference_rows - lse_ref[:, None]
    divergence = lax.optimization_barrier(jnp.sum(jnp.exp(log_ref) * (log_ref - (logits - lse_roll[:, None])), axis=-1))
    picked = jnp.take_along_axis(logits, token_ids[:, None].astype(jnp.int32), axis=1)[:, 0]
    token_logprob = picked - lse_roll
    return (new_state, divergence, token_logprob, in_z, in_x, in_bc, in_dt, out_t)
```

```python
import functools

import jax
import jax.numpy as jnp
from jax import lax
from jax.experimental import pallas as pl
from jax.experimental.pallas import tpu as pltpu
from jax.sharding import PartitionSpec as P

MESH = pl.DeviceIdType.MESH
EPSILON = 1e-05
SEQS, D, DI, HEADS, P_SIZE, N = 16, 2560, 640, 10, 64, 128
SHARD = 160
SLICE = 320
CHIPS = 8
VL = 3200
F32 = jnp.float32
BF16 = jnp.bfloat16

PIECES = {
    "X": ("x", 0, 160, False),
    "OL": ("o", 0, 80, False),
    "DT": ("d", 0, 160, False),
    "Z": ("z", 0, 160, True),
    "BC": ("b", 0, 160, True),
    "OH": ("o", 80, 80, True),
}
ORDER = {name: at for at, name in enumerate(PIECES)}


def silu(v):
    return v / (1.0 + jnp.exp(-v))


def per_head(values):
    rows = values.shape[0]
    lane = lax.broadcasted_iota(jnp.int32, (rows, 128), 1)
    parts = []
    for pair in range(HEADS // 2):
        left = jnp.broadcast_to(values[:, 2 * pair : 2 * pair + 1], (rows, 128))
        right = jnp.broadcast_to(values[:, 2 * pair + 1 : 2 * pair + 2], (rows, 128))
        parts.append(jnp.where(lane < P_SIZE, left, right))
    return jnp.concatenate(parts, axis=1)


def as_column(row):
    r = lax.broadcasted_iota(jnp.int32, (SEQS, SEQS), 0)
    c = lax.broadcasted_iota(jnp.int32, (SEQS, SEQS), 1)
    return jnp.sum(jnp.where(r == c, jnp.broadcast_to(row, (SEQS, SEQS)), 0.0), axis=1, keepdims=True)


def as_row(column):
    r = lax.broadcasted_iota(jnp.int32, (SEQS, 128), 0)
    c = lax.broadcasted_iota(jnp.int32, (SEQS, 128), 1)
    return jnp.sum(jnp.where(r == c, jnp.broadcast_to(column, (SEQS, 128)), 0.0), axis=0, keepdims=True)


def two_parts(values, width):
    high = values.astype(BF16)
    low = (values - high.astype(F32)).astype(BF16)
    rows = values.shape[0]
    return jnp.concatenate(
        [jnp.broadcast_to(high.astype(F32), (rows, width)), jnp.broadcast_to(low.astype(F32), (rows, width))], axis=1
    )


def kernel(
    hidden, state_in, conv_x, conv_bc, tokens, ref_in, in_z, in_x, in_bc, in_dt, out_t, lm_in,
    conv_wx, conv_bx, conv_wbc, conv_bbc, dt_bias, a_log, skip_gain, norm_in, norm_gain, final_gain,
    state, stats_out, zg, xg, bg, dt_out, og,
    dg, lm, refs, hsend, hrecv, gains, psend, precv, gsend, grecv, rsend, rrecv, usend, urecv, lsend, lrecv,
    ssend, srecv, decays, b_parts, x_cols, c_rows, y_acc,
    loc, chain_s, chain_r, ag_s, ag_r, d2_s, d2_r,
):
    g = lax.axis_index("group")
    h = lax.axis_index("head")
    k = g // 2
    c = g % 2
    x = k // 2
    zl = k % 2
    sibling = (2 * k + 1 - c, h)

    barrier = pltpu.get_barrier_semaphore()
    pl.semaphore_signal(barrier, inc=1, device_id=sibling, device_id_type=MESH)
    for d in range(1, 8):
        pl.semaphore_signal(barrier, inc=1, device_id=(2 * ((k + d) % 8) + c, h), device_id_type=MESH)
        pl.semaphore_signal(barrier, inc=1, device_id=(g, (h + d) % 8), device_id_type=MESH)

    rows_mine = pl.ds(pl.multiple_of(g * SHARD, SHARD), SHARD)
    lm_rows = pl.ds(pl.multiple_of(c * SHARD, SHARD), SHARD)
    local = [
        pltpu.make_async_copy(in_x, xg.at[rows_mine], loc.at[0]),
        pltpu.make_async_copy(in_bc, bg.at[rows_mine], loc.at[1]),
        pltpu.make_async_copy(in_dt, dg.at[rows_mine], loc.at[2]),
        pltpu.make_async_copy(in_z, zg.at[rows_mine], loc.at[3]),
        pltpu.make_async_copy(out_t, og.at[rows_mine], loc.at[4]),
        pltpu.make_async_copy(lm_in, lm.at[lm_rows], loc.at[5]),
        pltpu.make_async_copy(state_in, state, loc.at[6]),
        pltpu.make_async_copy(ref_in, refs, loc.at[7]),
    ]
    for copy in local:
        copy.start()

    for j in range(CHIPS):
        hsend[j] = hidden[:, SLICE * j : SLICE * (j + 1)]
        gains[0, j] = norm_in[:, SLICE * j : SLICE * (j + 1)]
        gains[1, j] = final_gain[:, SLICE * j : SLICE * (j + 1)]
    whole = hidden[...].astype(F32)
    scale_in = lax.rsqrt(jnp.mean(whole * whole, axis=-1, keepdims=True) + EPSILON)

    pl.semaphore_wait(barrier, 15)

    pending = []

    def chain_copy(phase, d, src, dst, device):
        return pltpu.make_async_remote_copy(
            src_ref=src, dst_ref=dst, send_sem=chain_s.at[phase, d], recv_sem=chain_r.at[phase, d],
            device_id=device, device_id_type=MESH,
        )

    def to_chips(phase, send_slot, recv):
        for d in range(1, 8):
            j = (k + d) % 8
            copy = chain_copy(phase, d, send_slot(j), recv.at[k], (2 * j + c, h))
            copy.start()
            pending.append(copy)

    def from_chips(phase, recv):
        for d in range(1, 8):
            j = (k + 8 - d) % 8
            chain_copy(phase, d, recv.at[j], recv.at[j], (2 * j + c, h)).wait_recv()

    def to_heads(phase, send_slot, recv):
        for d in range(1, 8):
            j = (h + d) % 8
            copy = chain_copy(phase, d, send_slot(j), recv.at[h], (g, j))
            copy.start()
            pending.append(copy)

    def from_heads(phase, recv):
        for d in range(1, 8):
            j = (h + 8 - d) % 8
            chain_copy(phase, d, recv.at[j], recv.at[j], (g, j)).wait_recv()

    buffers = {"x": xg, "z": zg, "o": og, "b": bg, "d": dg}

    def region(piece, dx, dz, core):
        name, first, rows, _ = PIECES[piece]
        at = ((((x + dx) % 4) * 2 + (zl + dz) % 2) * 2 + core) * SHARD + first
        return buffers[name].at[pl.ds(pl.multiple_of(at, 16), rows)]

    count = [0]

    def ici(piece, dx, dz, way):
        move = {"+": 1, "-": 3, "z": 0}[way]
        rx, rz = (dx - move) % 4, (dz + (way == "z")) % 2
        chip = ((x + move) % 4) * 2 + (zl + (way == "z")) % 2
        block = region(piece, dx, dz, c)
        copy = pltpu.make_async_remote_copy(
            src_ref=block, dst_ref=block, send_sem=ag_s.at[count[0]], recv_sem=ag_r.at[ORDER[piece], rx, rz],
            device_id=(2 * chip + c, h), device_id_type=MESH,
        )
        count[0] += 1
        copy.start()
        pending.append(copy)

    def on_chip(piece, dx, dz):
        block = region(piece, dx, dz, c)
        copy = pltpu.make_async_remote_copy(
            src_ref=block, dst_ref=block, send_sem=d2_s.at[ORDER[piece], dx, dz], recv_sem=d2_r.at[ORDER[piece], dx, dz],
            device_id=sibling, device_id_type=MESH,
        )
        copy.start()
        pending.append(copy)

    waited = set()

    def arrived(piece, dx, dz):
        block = region(piece, dx, dz, c)
        pltpu.make_async_remote_copy(
            src_ref=block, dst_ref=block, send_sem=d2_s.at[ORDER[piece], dx, dz], recv_sem=ag_r.at[ORDER[piece], dx, dz],
            device_id=sibling, device_id_type=MESH,
        ).wait_recv()
        waited.add((piece, dx, dz))
        on_chip(piece, dx, dz)

    chip_waited = set()

    def from_sibling(piece, dx, dz):
        block = region(piece, dx, dz, 1 - c)
        pltpu.make_async_remote_copy(
            src_ref=block, dst_ref=block, send_sem=d2_s.at[ORDER[piece], dx, dz], recv_sem=d2_r.at[ORDER[piece], dx, dz],
            device_id=sibling, device_id_type=MESH,
        ).wait_recv()
        chip_waited.add((piece, dx, dz))

    to_chips(0, lambda j: hsend.at[j], hrecv)
    hrecv[k] = hsend[k]
    local[0].wait()
    on_chip("X", 0, 0)
    local[1].wait()
    on_chip("BC", 0, 0)
    local[2].wait()
    on_chip("DT", 0, 0)
    local[3].wait()
    on_chip("Z", 0, 0)
    ici("X", 0, 0, "+")
    ici("X", 0, 0, "-")
    ici("Z", 0, 0, "z")
    local[4].wait()
    on_chip("OL", 0, 0)
    on_chip("OH", 0, 0)
    local[5].wait()
    lm_copy = pltpu.make_async_remote_copy(
        src_ref=lm.at[lm_rows], dst_ref=lm.at[lm_rows], send_sem=loc.at[8], recv_sem=loc.at[9],
        device_id=sibling, device_id_type=MESH,
    )
    lm_copy.start()
    pending.append(lm_copy)

    from_chips(0, hrecv)
    gain = gains[0, k]
    lhs = (hrecv[...].astype(F32) * gain[None]).astype(BF16).reshape(CHIPS * SEQS, SLICE)
    slice_rows = pl.ds(pl.multiple_of(k * SLICE, SLICE), SLICE)

    def partial(weights, at, width):
        product = jnp.dot(lhs, weights[slice_rows, :], preferred_element_type=F32)
        psend[:, :, at : at + width] = product.astype(BF16).reshape(CHIPS, SEQS, width)

    from_sibling("X", 0, 0)
    partial(xg, 0, 640)
    from_sibling("BC", 0, 0)
    partial(bg, 640, 256)
    from_sibling("DT", 0, 0)
    partial(dg, 896, 128)
    to_chips(1, lambda j: psend.at[j, :, pl.ds(0, 1024)], precv.at[:, :, pl.ds(0, 1024)])
    from_sibling("Z", 0, 0)
    partial(zg, 1024, 640)
    to_chips(2, lambda j: psend.at[j, :, pl.ds(1024, 640)], precv.at[:, :, pl.ds(1024, 640)])
    precv[k] = psend[k]
    arrived("Z", 0, 1)
    ici("Z", 0, 0, "+")
    ici("Z", 0, 0, "-")
    ici("X", 0, 0, "z")

    from_chips(1, precv.at[:, :, pl.ds(0, 1024)])
    summed = jnp.sum(precv[:, :, 0:1024].astype(F32), axis=0) * scale_in
    x_new = summed[:, 0:640]
    bc_new = summed[:, 640:896]
    step_raw = summed[:, 896 : 896 + HEADS]
    acc = x_new * conv_wx[3:4, :] + conv_bx[...]
    acc_bc = bc_new * conv_wbc[3:4, :] + conv_bbc[...]
    for tap in range(3):
        acc = acc + conv_x[tap].astype(F32) * conv_wx[tap : tap + 1, :]
        acc_bc = acc_bc + conv_bc[tap].astype(F32) * conv_wbc[tap : tap + 1, :]
    x_conv = silu(acc)
    bc_conv = silu(acc_bc)
    b_vals = bc_conv[:, :N]
    c_vals = bc_conv[:, N:]
    biased = step_raw + dt_bias[...]
    step = jnp.maximum(biased, 0.0) + jnp.log1p(jnp.exp(-jnp.abs(biased)))
    decays[:, 0:HEADS] = jnp.exp(-step * jnp.exp(a_log[...]))
    inflow = per_head(step) * x_conv
    in_high = inflow.astype(BF16).astype(F32)
    in_low = inflow - in_high
    stacked = jnp.concatenate([in_high, in_low, in_high, jnp.zeros_like(in_high)], axis=0)
    x_cols[...] = jnp.transpose(jnp.concatenate([stacked, jnp.zeros_like(stacked)], axis=0)).astype(BF16)
    b_high = b_vals.astype(BF16).astype(F32)
    b_low = b_vals - b_high
    b_parts[...] = jnp.concatenate([b_high, b_high, b_low, jnp.zeros((5 * SEQS, N), F32)], axis=0)
    c_high = c_vals.astype(BF16)
    c_low = (c_vals - c_high.astype(F32)).astype(BF16)
    c_rows[...] = jnp.concatenate([c_high, c_low], axis=0)
    y_acc[...] = jnp.zeros_like(y_acc)
    local[6].wait()

    def one_sequence(s, _):
        row = lax.broadcasted_iota(jnp.int32, (8 * SEQS, N), 0)
        picked_b = jnp.where(row % SEQS == s, b_parts[...], 0.0).astype(BF16)
        added = jnp.dot(x_cols[...], picked_b, preferred_element_type=F32)
        decay_row = decays[pl.ds(s, 1), :]
        for head in range(HEADS):
            rows = slice(head * P_SIZE, (head + 1) * P_SIZE)
            factor = jnp.broadcast_to(decay_row[:, head : head + 1], (P_SIZE, N))
            state[s, rows] = state[s, rows] * factor + added[rows]
        seen = lax.dot_general(
            c_rows[...], state[s].astype(BF16), (((1,), (1,)), ((), ())), preferred_element_type=F32
        )
        seen = seen[0:SEQS] + seen[SEQS:]
        which = lax.broadcasted_iota(jnp.int32, (SEQS, DI), 0)
        y_acc[...] += jnp.where(which == s, seen, 0.0)
        return 0

    lax.fori_loop(0, SEQS, one_sequence, 0)
    from_chips(2, precv.at[:, :, pl.ds(1024, 640)])
    gate = jnp.sum(precv[:, :, 1024:1664].astype(F32), axis=0) * scale_in
    ssm_out = y_acc[...] + per_head(skip_gain[...]) * x_conv
    gated = ssm_out * silu(gate)
    squares = jnp.sum(gated * gated, axis=-1, keepdims=True)
    gsend[:, 0:640] = (gated * norm_gain[...]).astype(BF16)
    gsend[:, 640:768] = two_parts(squares, 64).astype(BF16)

    to_chips(3, lambda j: gsend, grecv)
    grecv[k] = gsend[...]
    arrived("X", 3, 0)
    ici("X", 3, 0, "+")
    ici("X", 3, 0, "z")
    arrived("X", 1, 0)
    ici("X", 1, 0, "z")
    ici("Z", 0, 1, "+")
    ici("Z", 0, 1, "-")
    ici("OL", 0, 0, "+")
    ici("OL", 0, 0, "-")

    from_sibling("OL", 0, 0)
    from_sibling("OH", 0, 0)
    from_chips(3, grecv)
    mixed = lax.dot_general(
        grecv[:, :, 0:640].reshape(CHIPS * SEQS, 640), og[slice_rows, :], (((1,), (1,)), ((), ())),
        preferred_element_type=F32,
    )
    parts = grecv[:, :, 640:768].astype(F32)
    sq = (parts[:, :, 0:1] + parts[:, :, 64:65])
    rsend[:, :, 0:SLICE] = mixed.reshape(CHIPS, SEQS, SLICE)
    rsend[:, :, 384:512] = jnp.broadcast_to(sq, (CHIPS, SEQS, 128))
    to_heads(4, lambda j: rsend.at[j], rrecv)
    rrecv[h] = rsend[h]
    ici("BC", 0, 0, "z")
    ici("OH", 0, 0, "z")
    ici("DT", 0, 0, "z")
    ici("OL", 0, 0, "z")
    from_heads(4, rrecv)
    total = jnp.sum(rrecv[...], axis=0)
    scale_gate = lax.rsqrt(total[:, 384:385] / (8.0 * DI) + EPSILON)
    stream = hrecv[h].astype(F32) + total[:, 0:SLICE] * scale_gate
    usend[:, 0:SLICE] = (stream * gains[1, k]).astype(BF16)
    usend[:, 384:512] = two_parts(jnp.sum(stream * stream, axis=-1, keepdims=True), 64).astype(BF16)

    to_heads(5, lambda j: usend, urecv)
    urecv[h] = usend[...]

    local[5 + 2].wait()
    pltpu.make_async_remote_copy(
        src_ref=lm.at[pl.ds(pl.multiple_of((1 - c) * SHARD, SHARD), SHARD)],
        dst_ref=lm.at[pl.ds(pl.multiple_of((1 - c) * SHARD, SHARD), SHARD)], send_sem=loc.at[8], recv_sem=loc.at[9],
        device_id=sibling, device_id_type=MESH,
    ).wait_recv()
    from_heads(5, urecv)
    final = urecv[:, :, 0:SLICE].reshape(CHIPS * SEQS, SLICE)

    def some_logits(block, _):
        at = pl.ds(pl.multiple_of(block * 640, 640), 640)
        product = jnp.dot(final, lm[:, at], preferred_element_type=F32)
        lsend[:, :, at] = product.astype(BF16).reshape(CHIPS, SEQS, 640)
        return 0

    lax.fori_loop(0, VL // 640, some_logits, 0)
    lsend[:, :, VL : VL + 128] = urecv[:, :, 384:512]
    to_chips(6, lambda j: lsend.at[j], lrecv)
    lrecv[k] = lsend[k]

    for way in "+-":
        ici("BC", 0, 0, way)
        ici("OH", 0, 0, way)
        ici("DT", 0, 0, way)
    arrived("X", 2, 0)
    ici("X", 2, 0, "z")
    arrived("Z", 3, 0)
    ici("Z", 3, 0, "+")
    arrived("Z", 1, 1)
    ici("Z", 1, 1, "-")
    arrived("OL", 1, 0)
    ici("OL", 1, 0, "-")
    ici("OL", 1, 0, "z")
    arrived("OL", 3, 0)
    ici("OL", 3, 0, "z")
    arrived("BC", 0, 1)
    arrived("OH", 0, 1)
    for way in "+-":
        ici("BC", 0, 1, way)
        ici("OH", 0, 1, way)

    reference = refs[...].astype(F32)
    ref_max = jnp.max(reference, axis=-1, keepdims=True)
    weight = jnp.exp(reference - ref_max)
    ref_sum = jnp.sum(weight, axis=-1, keepdims=True)

    arrived("DT", 1, 0)
    ici("DT", 1, 0, "-")
    ici("DT", 1, 0, "z")
    arrived("DT", 3, 0)
    ici("DT", 3, 0, "z")
    from_chips(6, lrecv)
    logits = jnp.sum(lrecv[:, :, 0:VL].astype(F32), axis=0)
    tail = jnp.sum(lrecv[:, :, VL : VL + 128].astype(F32), axis=0)
    logits = logits * lax.rsqrt((tail[:, 0:1] + tail[:, 64:65]) / D + EPSILON)
    roll_max = jnp.max(logits, axis=-1, keepdims=True)
    roll_sum = jnp.sum(jnp.exp(logits - roll_max), axis=-1, keepdims=True)
    cross = jnp.sum(weight * (reference - logits), axis=-1, keepdims=True)
    token = as_column(tokens[...].astype(F32)).astype(jnp.int32)
    column = lax.broadcasted_iota(jnp.int32, (SEQS, VL), 1) + h * VL
    picked = jnp.sum(jnp.where(column == token, logits, 0.0), axis=-1, keepdims=True)
    lane = lax.broadcasted_iota(jnp.int32, (SEQS, 128), 1)
    packed = jnp.zeros((SEQS, 128), F32)
    for at, value in enumerate((roll_max, roll_sum, ref_max, ref_sum, cross, picked)):
        packed = jnp.where(lane == at, jnp.broadcast_to(value, (SEQS, 128)), packed)
    ssend[...] = packed

    to_heads(7, lambda j: ssend, srecv)
    srecv[h] = ssend[...]

    arrived("BC", 3, 0)
    ici("BC", 3, 0, "+")
    arrived("OH", 3, 0)
    ici("OH", 3, 0, "+")
    arrived("BC", 1, 1)
    ici("BC", 1, 1, "-")
    arrived("OH", 1, 1)
    ici("OH", 1, 1, "-")
    arrived("OL", 2, 0)
    ici("OL", 2, 0, "z")
    arrived("DT", 2, 0)
    ici("DT", 2, 0, "z")

    from_heads(7, srecv)
    every = srecv[...]
    m_all, s_all, rm_all, rs_all, x_all, p_all = (every[:, :, at : at + 1] for at in range(6))
    roll_top = jnp.max(m_all, axis=0)
    roll_total = jnp.sum(s_all * jnp.exp(m_all - roll_top[None]), axis=0)
    ref_top = jnp.max(rm_all, axis=0)
    ref_scale = jnp.exp(rm_all - ref_top[None])
    ref_total = jnp.sum(rs_all * ref_scale, axis=0)
    cross_total = jnp.sum(x_all * ref_scale, axis=0)
    lse_roll = roll_top + jnp.log(roll_total)
    lse_ref = ref_top + jnp.log(ref_total)
    divergence = cross_total / ref_total - lse_ref + lse_roll
    logprob = jnp.sum(p_all, axis=0) - lse_roll
    stats_out[0:1, :] = as_row(divergence)
    stats_out[1:2, :] = as_row(logprob)

    for piece in PIECES:
        for dz in range(2):
            for dx in range(4):
                if (dx, dz) != (0, 0) and (piece, dx, dz) not in waited:
                    arrived(piece, dx, dz)
    for piece in PIECES:
        for dz in range(2):
            for dx in range(4):
                if (piece, dx, dz) not in chip_waited:
                    from_sibling(piece, dx, dz)
    for block in range(2):
        turned = jnp.transpose(dg[block * 1280 : (block + 1) * 1280, :].astype(F32))
        dt_out[:, block * 1280 : (block + 1) * 1280] = turned[0:HEADS].astype(BF16)
    for copy in pending:
        copy.wait_send()


ANY = pl.BlockSpec(memory_space=pl.ANY)
VMEM = pl.BlockSpec(memory_space=pltpu.VMEM)
SENDS = 64


def shards(
    hidden_in, ssm_state, conv_x_state, conv_bc_state, token_ids, ref_logits, in_z, in_x, in_bc, in_dt, out_t,
    lm_head, conv_wx, conv_bx, conv_wbc, conv_bbc, dt_bias, a_log, skip_gain, norm_in, norm_gain, final_gain,
):
    row = lambda v: v.reshape(1, -1)
    state, stats, roll_z, roll_x, roll_bc, dt_rows, roll_out = pl.pallas_call(
        kernel,
        out_shape=(
            jax.ShapeDtypeStruct((SEQS, DI, N), F32),
            jax.ShapeDtypeStruct((8, 128), F32),
            jax.ShapeDtypeStruct((D, DI), BF16),
            jax.ShapeDtypeStruct((D, DI), BF16),
            jax.ShapeDtypeStruct((D, 256), BF16),
            jax.ShapeDtypeStruct((HEADS, D), BF16),
            jax.ShapeDtypeStruct((D, DI), BF16),
        ),
        in_specs=[VMEM, ANY, VMEM, VMEM, VMEM, ANY, ANY, ANY, ANY, ANY, ANY, ANY] + [VMEM] * 10,
        out_specs=(VMEM,) * 7,
        scratch_shapes=[
            pltpu.VMEM((D, 128), BF16),
            pltpu.VMEM((SLICE, VL), BF16),
            pltpu.VMEM((SEQS, VL), BF16),
            pltpu.VMEM((CHIPS, SEQS, SLICE), BF16),
            pltpu.VMEM((CHIPS, SEQS, SLICE), BF16),
            pltpu.VMEM((2, CHIPS, 1, SLICE), F32),
            pltpu.VMEM((CHIPS, SEQS, 1664), BF16),
            pltpu.VMEM((CHIPS, SEQS, 1664), BF16),
            pltpu.VMEM((SEQS, 768), BF16),
            pltpu.VMEM((CHIPS, SEQS, 768), BF16),
            pltpu.VMEM((CHIPS, SEQS, 512), F32),
            pltpu.VMEM((CHIPS, SEQS, 512), F32),
            pltpu.VMEM((SEQS, 512), BF16),
            pltpu.VMEM((CHIPS, SEQS, 512), BF16),
            pltpu.VMEM((CHIPS, SEQS, VL + 128), BF16),
            pltpu.VMEM((CHIPS, SEQS, VL + 128), BF16),
            pltpu.VMEM((SEQS, 128), F32),
            pltpu.VMEM((CHIPS, SEQS, 128), F32),
            pltpu.VMEM((SEQS, 128), F32),
            pltpu.VMEM((8 * SEQS, N), F32),
            pltpu.VMEM((DI, 8 * SEQS), BF16),
            pltpu.VMEM((2 * SEQS, N), BF16),
            pltpu.VMEM((SEQS, DI), F32),
            pltpu.SemaphoreType.DMA((10,)),
            pltpu.SemaphoreType.DMA((8, 8)),
            pltpu.SemaphoreType.DMA((8, 8)),
            pltpu.SemaphoreType.DMA((SENDS,)),
            pltpu.SemaphoreType.DMA((6, 4, 2)),
            pltpu.SemaphoreType.DMA((6, 4, 2)),
            pltpu.SemaphoreType.DMA((6, 4, 2)),
        ],
        compiler_params=pltpu.CompilerParams(
            collective_id=0, has_side_effects=True, vmem_limit_bytes=60000 * 1024
        ),
    )(
        hidden_in, ssm_state.reshape(SEQS, DI, N), conv_x_state.transpose(1, 0, 2), conv_bc_state.transpose(1, 0, 2),
        row(token_ids), ref_logits, in_z, in_x, in_bc, jnp.pad(in_dt, ((0, 0), (0, 128 - HEADS))), out_t, lm_head.T,
        conv_wx, row(conv_bx), conv_wbc, row(conv_bbc), row(dt_bias), row(a_log), row(skip_gain), row(norm_in),
        row(norm_gain), row(final_gain),
    )
    return (
        state.reshape(ssm_state.shape), stats[0, :SEQS], stats[1, :SEQS], roll_z, roll_x, roll_bc, dt_rows.T, roll_out,
    )


def solution(mesh):
    spread = P("group", "head")
    return jax.shard_map(
        shards,
        mesh=mesh,
        in_specs=(
            P("group", None), P("group", "head", None, None), P("group", None, "head"), P("group", None, None),
            P("group"), spread, spread, spread, P("group", None), spread, spread, P("head", "group"),
            P(None, "head"), P("head"), P(), P(), P("head"), P("head"), P("head"), P(), P("head"), P(),
        ),
        out_specs=(
            P("group", "head", None, None), P("group"), P("group"), P(None, "head"), P(None, "head"), P(),
            P(None, "head"), P(None, "head"),
        ),
        check_vma=False,
    )
```

```python
import functools

import jax
import jax.numpy as jnp
from jax import lax
from jax.experimental import pallas as pl
from jax.experimental.pallas import tpu as pltpu
from jax.sharding import PartitionSpec as P

MESH = pl.DeviceIdType.MESH
EPSILON = 1e-05
SEQS, D, DI, HEADS, P_SIZE, N = 16, 2560, 640, 10, 64, 128
SHARD = 160
SLICE = 320
CHIPS = 8
VL = 3200
F32 = jnp.float32
BF16 = jnp.bfloat16

PIECES = {
    "X": ("x", 0, 160, False),
    "OL": ("o", 0, 80, False),
    "DT": ("d", 0, 160, False),
    "Z": ("z", 0, 160, True),
    "BC": ("b", 0, 160, True),
    "OH": ("o", 80, 80, True),
}
ORDER = {name: at for at, name in enumerate(PIECES)}


def silu(v):
    return v / (1.0 + jnp.exp(-v))


def per_head(values):
    rows = values.shape[0]
    lane = lax.broadcasted_iota(jnp.int32, (rows, 128), 1)
    parts = []
    for pair in range(HEADS // 2):
        left = jnp.broadcast_to(values[:, 2 * pair : 2 * pair + 1], (rows, 128))
        right = jnp.broadcast_to(values[:, 2 * pair + 1 : 2 * pair + 2], (rows, 128))
        parts.append(jnp.where(lane < P_SIZE, left, right))
    return jnp.concatenate(parts, axis=1)


def as_column(row):
    r = lax.broadcasted_iota(jnp.int32, (SEQS, SEQS), 0)
    c = lax.broadcasted_iota(jnp.int32, (SEQS, SEQS), 1)
    return jnp.sum(jnp.where(r == c, jnp.broadcast_to(row, (SEQS, SEQS)), 0.0), axis=1, keepdims=True)


def as_row(column):
    r = lax.broadcasted_iota(jnp.int32, (SEQS, 128), 0)
    c = lax.broadcasted_iota(jnp.int32, (SEQS, 128), 1)
    return jnp.sum(jnp.where(r == c, jnp.broadcast_to(column, (SEQS, 128)), 0.0), axis=0, keepdims=True)


def two_parts(values, width):
    high = values.astype(BF16)
    low = (values - high.astype(F32)).astype(BF16)
    rows = values.shape[0]
    return jnp.concatenate(
        [jnp.broadcast_to(high.astype(F32), (rows, width)), jnp.broadcast_to(low.astype(F32), (rows, width))], axis=1
    )


def kernel(
    hidden_in, state_in, conv_x_in, conv_bc_in, tokens_in, ref_in, in_z, in_x, in_bc, dt_in, out_t, lm_in,
    conv_wx_in, conv_bx, conv_wbc_in, conv_bbc_in, dt_bias_in, a_log_in, skip_in, norm_in, norm_gain, final_gain,
    state, div_out, logprob_out, zg, xg, bg, dt_out, og,
    dg, lm, refs, hsend, hrecv, gains, psend, precv, gsend, grecv, rsend, rrecv, usend, urecv, lsend, lrecv,
    ssend, srecv, decays, b_parts, x_cols, c_rows, y_acc,
    hidden, conv_x, conv_bc, tokens, in_dt, conv_wx, conv_wbc, conv_bbc, dt_bias, a_log, skip_gain,
    long_rows, short_rows, loc, small, chain_s, chain_r, ag_s, ag_r, d2_s, d2_r,
):
    g = lax.axis_index("group")
    h = lax.axis_index("head")
    k = g // 2
    c = g % 2
    x = k // 2
    zl = k % 2
    sibling = (2 * k + 1 - c, h)

    barrier = pltpu.get_barrier_semaphore()
    pl.semaphore_signal(barrier, inc=1, device_id=sibling, device_id_type=MESH)
    for d in range(1, 8):
        pl.semaphore_signal(barrier, inc=1, device_id=(2 * ((k + d) % 8) + c, h), device_id_type=MESH)
        pl.semaphore_signal(barrier, inc=1, device_id=(g, (h + d) % 8), device_id_type=MESH)

    rows_mine = pl.ds(pl.multiple_of(g * SHARD, SHARD), SHARD)
    lm_rows = pl.ds(pl.multiple_of(c * SHARD, SHARD), SHARD)
    local = [
        pltpu.make_async_copy(source, target, loc.at[at])
        for at, (source, target) in enumerate(
            [
                (in_x, xg.at[rows_mine]), (in_bc, bg.at[rows_mine]), (in_z, zg.at[rows_mine]),
                (out_t, og.at[rows_mine]), (lm_in, lm.at[lm_rows]), (state_in, state), (ref_in, refs),
                (norm_in, long_rows.at[0]), (final_gain, long_rows.at[1]), (conv_bx, short_rows.at[0]),
                (norm_gain, short_rows.at[1]),
            ]
        )
    ]
    first = [
        pltpu.make_async_copy(source, target, small.at[at])
        for at, (source, target) in enumerate(
            [
                (hidden_in, hidden), (dt_in, in_dt), (conv_x_in, conv_x), (conv_bc_in, conv_bc), (tokens_in, tokens),
                (conv_wx_in, conv_wx), (conv_wbc_in, conv_wbc), (conv_bbc_in, conv_bbc), (dt_bias_in, dt_bias),
                (a_log_in, a_log), (skip_in, skip_gain),
            ]
        )
    ]
    for copy in first + local:
        copy.start()
    first[0].wait()
    first[1].wait()

    for j in range(CHIPS):
        hsend[j] = hidden[:, SLICE * j : SLICE * (j + 1)]
    turned = jnp.transpose(jnp.concatenate([in_dt[...].astype(F32), jnp.zeros((128 - HEADS, SHARD), F32)], axis=0))
    dg[rows_mine, :] = turned.astype(BF16)
    local[7].wait()
    local[8].wait()
    for j in range(CHIPS):
        gains[0, j] = long_rows[0:1, SLICE * j : SLICE * (j + 1)]
        gains[1, j] = long_rows[1:2, SLICE * j : SLICE * (j + 1)]
    whole = hidden[...].astype(F32)
    scale_in = lax.rsqrt(jnp.mean(whole * whole, axis=-1, keepdims=True) + EPSILON)

    pl.semaphore_wait(barrier, 15)

    pending = []

    def chain_copy(phase, d, src, dst, device):
        return pltpu.make_async_remote_copy(
            src_ref=src, dst_ref=dst, send_sem=chain_s.at[phase, d], recv_sem=chain_r.at[phase, d],
            device_id=device, device_id_type=MESH,
        )

    def to_chips(phase, send_slot, recv):
        for d in range(1, 8):
            j = (k + d) % 8
            copy = chain_copy(phase, d, send_slot(j), recv.at[k], (2 * j + c, h))
            copy.start()
            pending.append(copy)

    def from_chips(phase, recv):
        for d in range(1, 8):
            j = (k + 8 - d) % 8
            chain_copy(phase, d, recv.at[j], recv.at[j], (2 * j + c, h)).wait_recv()

    def to_heads(phase, send_slot, recv):
        for d in range(1, 8):
            j = (h + d) % 8
            copy = chain_copy(phase, d, send_slot(j), recv.at[h], (g, j))
            copy.start()
            pending.append(copy)

    def from_heads(phase, recv):
        for d in range(1, 8):
            j = (h + 8 - d) % 8
            chain_copy(phase, d, recv.at[j], recv.at[j], (g, j)).wait_recv()

    buffers = {"x": xg, "z": zg, "o": og, "b": bg, "d": dg}

    def region(piece, dx, dz, core):
        name, first, rows, _ = PIECES[piece]
        at = ((((x + dx) % 4) * 2 + (zl + dz) % 2) * 2 + core) * SHARD + first
        return buffers[name].at[pl.ds(pl.multiple_of(at, 16), rows)]

    count = [0]

    def ici(piece, dx, dz, way):
        move = {"+": 1, "-": 3, "z": 0}[way]
        rx, rz = (dx - move) % 4, (dz + (way == "z")) % 2
        chip = ((x + move) % 4) * 2 + (zl + (way == "z")) % 2
        block = region(piece, dx, dz, c)
        copy = pltpu.make_async_remote_copy(
            src_ref=block, dst_ref=block, send_sem=ag_s.at[count[0]], recv_sem=ag_r.at[ORDER[piece], rx, rz],
            device_id=(2 * chip + c, h), device_id_type=MESH,
        )
        count[0] += 1
        copy.start()
        pending.append(copy)

    def on_chip(piece, dx, dz):
        block = region(piece, dx, dz, c)
        copy = pltpu.make_async_remote_copy(
            src_ref=block, dst_ref=block, send_sem=d2_s.at[ORDER[piece], dx, dz], recv_sem=d2_r.at[ORDER[piece], dx, dz],
            device_id=sibling, device_id_type=MESH,
        )
        copy.start()
        pending.append(copy)

    waited = set()

    def arrived(piece, dx, dz):
        block = region(piece, dx, dz, c)
        pltpu.make_async_remote_copy(
            src_ref=block, dst_ref=block, send_sem=d2_s.at[ORDER[piece], dx, dz], recv_sem=ag_r.at[ORDER[piece], dx, dz],
            device_id=sibling, device_id_type=MESH,
        ).wait_recv()
        waited.add((piece, dx, dz))
        on_chip(piece, dx, dz)

    chip_waited = set()

    def from_sibling(piece, dx, dz):
        block = region(piece, dx, dz, 1 - c)
        pltpu.make_async_remote_copy(
            src_ref=block, dst_ref=block, send_sem=d2_s.at[ORDER[piece], dx, dz], recv_sem=d2_r.at[ORDER[piece], dx, dz],
            device_id=sibling, device_id_type=MESH,
        ).wait_recv()
        chip_waited.add((piece, dx, dz))

    to_chips(0, lambda j: hsend.at[j], hrecv)
    hrecv[k] = hsend[k]
    local[0].wait()
    on_chip("X", 0, 0)
    local[1].wait()
    on_chip("BC", 0, 0)
    on_chip("DT", 0, 0)
    local[2].wait()
    on_chip("Z", 0, 0)
    ici("X", 0, 0, "+")
    ici("X", 0, 0, "-")
    ici("Z", 0, 0, "z")
    local[3].wait()
    on_chip("OL", 0, 0)
    on_chip("OH", 0, 0)
    local[4].wait()
    lm_copy = pltpu.make_async_remote_copy(
        src_ref=lm.at[lm_rows], dst_ref=lm.at[lm_rows], send_sem=loc.at[12], recv_sem=loc.at[13],
        device_id=sibling, device_id_type=MESH,
    )
    lm_copy.start()
    pending.append(lm_copy)

    from_chips(0, hrecv)
    gain = gains[0, k]
    lhs = (hrecv[...].astype(F32) * gain[None]).astype(BF16).reshape(CHIPS * SEQS, SLICE)
    slice_rows = pl.ds(pl.multiple_of(k * SLICE, SLICE), SLICE)

    def partial(weights, at, width):
        product = jnp.dot(lhs, weights[slice_rows, :], preferred_element_type=F32)
        psend[:, :, at : at + width] = product.astype(BF16).reshape(CHIPS, SEQS, width)

    from_sibling("X", 0, 0)
    partial(xg, 0, 640)
    from_sibling("BC", 0, 0)
    partial(bg, 640, 256)
    from_sibling("DT", 0, 0)
    partial(dg, 896, 128)
    to_chips(1, lambda j: psend.at[j, :, pl.ds(0, 1024)], precv.at[:, :, pl.ds(0, 1024)])
    from_sibling("Z", 0, 0)
    partial(zg, 1024, 640)
    to_chips(2, lambda j: psend.at[j, :, pl.ds(1024, 640)], precv.at[:, :, pl.ds(1024, 640)])
    precv[k] = psend[k]
    arrived("Z", 0, 1)
    ici("Z", 0, 0, "+")
    ici("Z", 0, 0, "-")
    ici("X", 0, 0, "z")

    for copy in first[2:] + local[9:]:
        copy.wait()
    from_chips(1, precv.at[:, :, pl.ds(0, 1024)])
    summed = jnp.sum(precv[:, :, 0:1024].astype(F32), axis=0) * scale_in
    x_new = summed[:, 0:640]
    bc_new = summed[:, 640:896]
    step_raw = summed[:, 896 : 896 + HEADS]
    acc = x_new * conv_wx[3:4, :] + short_rows[0:1, :]
    acc_bc = bc_new * conv_wbc[3:4, :] + conv_bbc[...]
    for tap in range(3):
        acc = acc + conv_x[tap].astype(F32) * conv_wx[tap : tap + 1, :]
        acc_bc = acc_bc + conv_bc[tap].astype(F32) * conv_wbc[tap : tap + 1, :]
    x_conv = silu(acc)
    bc_conv = silu(acc_bc)
    b_vals = bc_conv[:, :N]
    c_vals = bc_conv[:, N:]
    biased = step_raw + dt_bias[...]
    step = jnp.maximum(biased, 0.0) + jnp.log1p(jnp.exp(-jnp.abs(biased)))
    decays[:, 0:HEADS] = jnp.exp(-step * jnp.exp(a_log[...]))
    inflow = per_head(step) * x_conv
    in_high = inflow.astype(BF16).astype(F32)
    in_low = inflow - in_high
    stacked = jnp.concatenate([in_high, in_low, in_high, jnp.zeros_like(in_high)], axis=0)
    x_cols[...] = jnp.transpose(jnp.concatenate([stacked, jnp.zeros_like(stacked)], axis=0)).astype(BF16)
    b_high = b_vals.astype(BF16).astype(F32)
    b_low = b_vals - b_high
    b_parts[...] = jnp.concatenate([b_high, b_high, b_low, jnp.zeros((5 * SEQS, N), F32)], axis=0)
    c_high = c_vals.astype(BF16)
    c_low = (c_vals - c_high.astype(F32)).astype(BF16)
    c_rows[...] = jnp.concatenate([c_high, c_low], axis=0)
    y_acc[...] = jnp.zeros_like(y_acc)
    local[5].wait()

    def one_sequence(s, _):
        row = lax.broadcasted_iota(jnp.int32, (8 * SEQS, N), 0)
        picked_b = jnp.where(row % SEQS == s, b_parts[...], 0.0).astype(BF16)
        added = jnp.dot(x_cols[...], picked_b, preferred_element_type=F32)
        decay_row = decays[pl.ds(s, 1), :]
        for head in range(HEADS):
            rows = slice(head * P_SIZE, (head + 1) * P_SIZE)
            factor = jnp.broadcast_to(decay_row[:, head : head + 1], (P_SIZE, N))
            state[s, rows] = state[s, rows] * factor + added[rows]
        seen = lax.dot_general(
            c_rows[...], state[s].astype(BF16), (((1,), (1,)), ((), ())), preferred_element_type=F32
        )
        seen = seen[0:SEQS] + seen[SEQS:]
        which = lax.broadcasted_iota(jnp.int32, (SEQS, DI), 0)
        y_acc[...] += jnp.where(which == s, seen, 0.0)
        return 0

    lax.fori_loop(0, SEQS, one_sequence, 0)
    from_chips(2, precv.at[:, :, pl.ds(1024, 640)])
    gate = jnp.sum(precv[:, :, 1024:1664].astype(F32), axis=0) * scale_in
    ssm_out = y_acc[...] + per_head(skip_gain[...]) * x_conv
    gated = ssm_out * silu(gate)
    squares = jnp.sum(gated * gated, axis=-1, keepdims=True)
    gsend[:, 0:640] = (gated * short_rows[1:2, :]).astype(BF16)
    gsend[:, 640:768] = two_parts(squares, 64).astype(BF16)

    to_chips(3, lambda j: gsend, grecv)
    grecv[k] = gsend[...]
    arrived("X", 3, 0)
    ici("X", 3, 0, "+")
    ici("X", 3, 0, "z")
    arrived("X", 1, 0)
    ici("X", 1, 0, "z")
    ici("Z", 0, 1, "+")
    ici("Z", 0, 1, "-")
    ici("OL", 0, 0, "+")
    ici("OL", 0, 0, "-")

    from_sibling("OL", 0, 0)
    from_sibling("OH", 0, 0)
    from_chips(3, grecv)
    mixed = lax.dot_general(
        grecv[:, :, 0:640].reshape(CHIPS * SEQS, 640), og[slice_rows, :], (((1,), (1,)), ((), ())),
        preferred_element_type=F32,
    )
    parts = grecv[:, :, 640:768].astype(F32)
    sq = (parts[:, :, 0:1] + parts[:, :, 64:65])
    rsend[:, :, 0:SLICE] = mixed.reshape(CHIPS, SEQS, SLICE)
    rsend[:, :, 384:512] = jnp.broadcast_to(sq, (CHIPS, SEQS, 128))
    to_heads(4, lambda j: rsend.at[j], rrecv)
    rrecv[h] = rsend[h]
    ici("BC", 0, 0, "z")
    ici("OH", 0, 0, "z")
    ici("DT", 0, 0, "z")
    ici("OL", 0, 0, "z")
    from_heads(4, rrecv)
    total = jnp.sum(rrecv[...], axis=0)
    scale_gate = lax.rsqrt(total[:, 384:385] / (8.0 * DI) + EPSILON)
    stream = hrecv[h].astype(F32) + total[:, 0:SLICE] * scale_gate
    usend[:, 0:SLICE] = (stream * gains[1, k]).astype(BF16)
    usend[:, 384:512] = two_parts(jnp.sum(stream * stream, axis=-1, keepdims=True), 64).astype(BF16)

    to_heads(5, lambda j: usend, urecv)
    urecv[h] = usend[...]

    local[6].wait()
    pltpu.make_async_remote_copy(
        src_ref=lm.at[pl.ds(pl.multiple_of((1 - c) * SHARD, SHARD), SHARD)],
        dst_ref=lm.at[pl.ds(pl.multiple_of((1 - c) * SHARD, SHARD), SHARD)], send_sem=loc.at[12], recv_sem=loc.at[13],
        device_id=sibling, device_id_type=MESH,
    ).wait_recv()
    from_heads(5, urecv)
    final = urecv[:, :, 0:SLICE].reshape(CHIPS * SEQS, SLICE)

    def some_logits(block, _):
        at = pl.ds(pl.multiple_of(block * 640, 640), 640)
        product = jnp.dot(final, lm[:, at], preferred_element_type=F32)
        lsend[:, :, at] = product.astype(BF16).reshape(CHIPS, SEQS, 640)
        return 0

    lax.fori_loop(0, VL // 640, some_logits, 0)
    lsend[:, :, VL : VL + 128] = urecv[:, :, 384:512]
    to_chips(6, lambda j: lsend.at[j], lrecv)
    lrecv[k] = lsend[k]

    for way in "+-":
        ici("BC", 0, 0, way)
        ici("OH", 0, 0, way)
        ici("DT", 0, 0, way)
    arrived("X", 2, 0)
    ici("X", 2, 0, "z")
    arrived("Z", 3, 0)
    ici("Z", 3, 0, "+")
    arrived("Z", 1, 1)
    ici("Z", 1, 1, "-")
    arrived("OL", 1, 0)
    ici("OL", 1, 0, "-")
    ici("OL", 1, 0, "z")
    arrived("OL", 3, 0)
    ici("OL", 3, 0, "z")
    arrived("BC", 0, 1)
    arrived("OH", 0, 1)
    for way in "+-":
        ici("BC", 0, 1, way)
        ici("OH", 0, 1, way)

    reference = refs[...].astype(F32)
    ref_max = jnp.max(reference, axis=-1, keepdims=True)
    weight = jnp.exp(reference - ref_max)
    ref_sum = jnp.sum(weight, axis=-1, keepdims=True)

    arrived("DT", 1, 0)
    ici("DT", 1, 0, "-")
    ici("DT", 1, 0, "z")
    arrived("DT", 3, 0)
    ici("DT", 3, 0, "z")
    from_chips(6, lrecv)
    logits = jnp.sum(lrecv[:, :, 0:VL].astype(F32), axis=0)
    tail = jnp.sum(lrecv[:, :, VL : VL + 128].astype(F32), axis=0)
    logits = logits * lax.rsqrt((tail[:, 0:1] + tail[:, 64:65]) / D + EPSILON)
    roll_max = jnp.max(logits, axis=-1, keepdims=True)
    roll_sum = jnp.sum(jnp.exp(logits - roll_max), axis=-1, keepdims=True)
    cross = jnp.sum(weight * (reference - logits), axis=-1, keepdims=True)
    token = as_column(tokens[...].astype(F32)).astype(jnp.int32)
    column = lax.broadcasted_iota(jnp.int32, (SEQS, VL), 1) + h * VL
    picked = jnp.sum(jnp.where(column == token, logits, 0.0), axis=-1, keepdims=True)
    lane = lax.broadcasted_iota(jnp.int32, (SEQS, 128), 1)
    packed = jnp.zeros((SEQS, 128), F32)
    for at, value in enumerate((roll_max, roll_sum, ref_max, ref_sum, cross, picked)):
        packed = jnp.where(lane == at, jnp.broadcast_to(value, (SEQS, 128)), packed)
    ssend[...] = packed

    to_heads(7, lambda j: ssend, srecv)
    srecv[h] = ssend[...]

    arrived("BC", 3, 0)
    ici("BC", 3, 0, "+")
    arrived("OH", 3, 0)
    ici("OH", 3, 0, "+")
    arrived("BC", 1, 1)
    ici("BC", 1, 1, "-")
    arrived("OH", 1, 1)
    ici("OH", 1, 1, "-")
    arrived("OL", 2, 0)
    ici("OL", 2, 0, "z")
    arrived("DT", 2, 0)
    ici("DT", 2, 0, "z")

    from_heads(7, srecv)
    every = srecv[...]
    m_all, s_all, rm_all, rs_all, x_all, p_all = (every[:, :, at : at + 1] for at in range(6))
    roll_top = jnp.max(m_all, axis=0)
    roll_total = jnp.sum(s_all * jnp.exp(m_all - roll_top[None]), axis=0)
    ref_top = jnp.max(rm_all, axis=0)
    ref_scale = jnp.exp(rm_all - ref_top[None])
    ref_total = jnp.sum(rs_all * ref_scale, axis=0)
    cross_total = jnp.sum(x_all * ref_scale, axis=0)
    lse_roll = roll_top + jnp.log(roll_total)
    lse_ref = ref_top + jnp.log(ref_total)
    divergence = cross_total / ref_total - lse_ref + lse_roll
    logprob = jnp.sum(p_all, axis=0) - lse_roll
    div_out[...] = as_row(divergence)[:, 0:SEQS]
    logprob_out[...] = as_row(logprob)[:, 0:SEQS]

    for piece in PIECES:
        for dz in range(2):
            for dx in range(4):
                if (dx, dz) != (0, 0) and (piece, dx, dz) not in waited:
                    arrived(piece, dx, dz)
    for piece in PIECES:
        for dz in range(2):
            for dx in range(4):
                if (piece, dx, dz) not in chip_waited:
                    from_sibling(piece, dx, dz)
    for block in range(2):
        turned = jnp.transpose(dg[block * 1280 : (block + 1) * 1280, :].astype(F32))
        dt_out[:, block * 1280 : (block + 1) * 1280] = turned[0:HEADS].astype(BF16)
    for copy in pending:
        copy.wait_send()


def write_out(*refs):
    count = len(refs) // 2
    copies = [pltpu.make_async_copy(refs[at], refs[count + at], refs[-1].at[at]) for at in range(count)]
    for copy in copies:
        copy.start()
    for copy in copies:
        copy.wait()


ANY = pl.BlockSpec(memory_space=pl.ANY)
VMEM = pl.BlockSpec(memory_space=pltpu.VMEM)
SENDS = 64


def shards(
    hidden_in, ssm_state, conv_x_state, conv_bc_state, token_ids, ref_logits, in_z, in_x, in_bc, in_dt, out_t,
    lm_head, conv_wx, conv_bx, conv_wbc, conv_bbc, dt_bias, a_log, skip_gain, norm_in, norm_gain, final_gain,
):
    row = lambda v: v.reshape(1, -1)
    results = (
        ((SEQS, DI, N), F32), ((1, SEQS), F32), ((1, SEQS), F32), ((D, DI), BF16), ((D, DI), BF16), ((D, 256), BF16),
        ((HEADS, D), BF16), ((D, DI), BF16),
    )
    held = pl.pallas_call(
        kernel,
        out_shape=tuple(pltpu.VMEM(shape, dtype) for shape, dtype in results),
        in_specs=[pl.BlockSpec(memory_space=pltpu.HBM)] * 22,
        out_specs=(VMEM,) * len(results),
        scratch_shapes=[
            pltpu.VMEM((D, 128), BF16),
            pltpu.VMEM((SLICE, VL), BF16),
            pltpu.VMEM((SEQS, VL), BF16),
            pltpu.VMEM((CHIPS, SEQS, SLICE), BF16),
            pltpu.VMEM((CHIPS, SEQS, SLICE), BF16),
            pltpu.VMEM((2, CHIPS, 1, SLICE), F32),
            pltpu.VMEM((CHIPS, SEQS, 1664), BF16),
            pltpu.VMEM((CHIPS, SEQS, 1664), BF16),
            pltpu.VMEM((SEQS, 768), BF16),
            pltpu.VMEM((CHIPS, SEQS, 768), BF16),
            pltpu.VMEM((CHIPS, SEQS, 512), F32),
            pltpu.VMEM((CHIPS, SEQS, 512), F32),
            pltpu.VMEM((SEQS, 512), BF16),
            pltpu.VMEM((CHIPS, SEQS, 512), BF16),
            pltpu.VMEM((CHIPS, SEQS, VL + 128), BF16),
            pltpu.VMEM((CHIPS, SEQS, VL + 128), BF16),
            pltpu.VMEM((SEQS, 128), F32),
            pltpu.VMEM((CHIPS, SEQS, 128), F32),
            pltpu.VMEM((SEQS, 128), F32),
            pltpu.VMEM((8 * SEQS, N), F32),
            pltpu.VMEM((DI, 8 * SEQS), BF16),
            pltpu.VMEM((2 * SEQS, N), BF16),
            pltpu.VMEM((SEQS, DI), F32),
            pltpu.VMEM((SEQS, D), BF16),
            pltpu.VMEM((3, SEQS, DI), BF16),
            pltpu.VMEM((3, SEQS, 256), BF16),
            pltpu.VMEM((1, SEQS), jnp.int32),
            pltpu.VMEM((HEADS, SHARD), BF16),
            pltpu.VMEM((4, DI), F32),
            pltpu.VMEM((4, 256), F32),
            pltpu.VMEM((1, 256), F32),
            pltpu.VMEM((1, HEADS), F32),
            pltpu.VMEM((1, HEADS), F32),
            pltpu.VMEM((1, HEADS), F32),
            pltpu.VMEM((2, D), F32),
            pltpu.VMEM((2, DI), F32),
            pltpu.SemaphoreType.DMA((14,)),
            pltpu.SemaphoreType.DMA((11,)),
            pltpu.SemaphoreType.DMA((8, 8)),
            pltpu.SemaphoreType.DMA((8, 8)),
            pltpu.SemaphoreType.DMA((SENDS,)),
            pltpu.SemaphoreType.DMA((6, 4, 2)),
            pltpu.SemaphoreType.DMA((6, 4, 2)),
            pltpu.SemaphoreType.DMA((6, 4, 2)),
        ],
        compiler_params=pltpu.CompilerParams(
            collective_id=0, has_side_effects=True, vmem_limit_bytes=32 * 1024 * 1024
        ),
    )(*[pltpu.with_memory_space_constraint(array, pltpu.HBM) for array in (
        hidden_in, ssm_state.reshape(SEQS, DI, N), conv_x_state.transpose(1, 0, 2), conv_bc_state.transpose(1, 0, 2),
        row(token_ids), ref_logits, in_z, in_x, in_bc, in_dt.T, out_t, lm_head.T,
        conv_wx, conv_bx, conv_wbc, row(conv_bbc), row(dt_bias), row(a_log), row(skip_gain), norm_in,
        norm_gain, final_gain,
    )])
    held = [pltpu.with_memory_space_constraint(array, pltpu.VMEM) for array in held]
    state, divergence, logprob, roll_z, roll_x, roll_bc, dt_rows, roll_out = pl.pallas_call(
        write_out,
        out_shape=tuple(jax.ShapeDtypeStruct(shape, dtype) for shape, dtype in results),
        in_specs=[VMEM] * len(results),
        out_specs=(ANY,) * len(results),
        scratch_shapes=[pltpu.SemaphoreType.DMA((len(results),))],
        compiler_params=pltpu.CompilerParams(vmem_limit_bytes=1024 * 1024),
    )(*held)
    return (
        state.reshape(ssm_state.shape), divergence.reshape(SEQS), logprob.reshape(SEQS), roll_z, roll_x, roll_bc,
        dt_rows.T, roll_out,
    )


def solution(mesh):
    spread = P("group", "head")
    return jax.shard_map(
        shards,
        mesh=mesh,
        in_specs=(
            P("group", None), P("group", "head", None, None), P("group", None, "head"), P("group", None, None),
            P("group"), spread, spread, spread, P("group", None), spread, spread, P("head", "group"),
            P(None, "head"), P("head"), P(), P(), P("head"), P("head"), P("head"), P(), P("head"), P(),
        ),
        out_specs=(
            P("group", "head", None, None), P("group"), P("group"), P(None, "head"), P(None, "head"), P(),
            P(None, "head"), P(None, "head"),
        ),
        check_vma=False,
    )
```

```python
import functools

import jax
import jax.numpy as jnp
from jax import lax
from jax.experimental import pallas as pl
from jax.experimental.pallas import tpu as pltpu
from jax.sharding import PartitionSpec as P

MESH = pl.DeviceIdType.MESH
EPSILON = 1e-05
SEQS, D, DI, HEADS, P_SIZE, N = 16, 2560, 640, 10, 64, 128
SHARD = 160
SLICE = 320
CHIPS = 8
VL = 3200
F32 = jnp.float32
BF16 = jnp.bfloat16

PIECES = {
    "X": ("x", 0, 160),
    "OL": ("o", 0, 80),
    "DT": ("d", 0, 160),
    "Z": ("z", 0, 160),
    "BC": ("b", 0, 160),
    "OH": ("o", 80, 80),
}
ORDER = {name: at for at, name in enumerate(PIECES)}
ARRAYS = "xobdz"


def silu(v):
    return v / (1.0 + jnp.exp(-v))


def per_head(values):
    rows = values.shape[0]
    lane = lax.broadcasted_iota(jnp.int32, (rows, 128), 1)
    parts = []
    for pair in range(HEADS // 2):
        left = jnp.broadcast_to(values[:, 2 * pair : 2 * pair + 1], (rows, 128))
        right = jnp.broadcast_to(values[:, 2 * pair + 1 : 2 * pair + 2], (rows, 128))
        parts.append(jnp.where(lane < P_SIZE, left, right))
    return jnp.concatenate(parts, axis=1)


def as_column(row):
    r = lax.broadcasted_iota(jnp.int32, (SEQS, SEQS), 0)
    c = lax.broadcasted_iota(jnp.int32, (SEQS, SEQS), 1)
    return jnp.sum(jnp.where(r == c, jnp.broadcast_to(row, (SEQS, SEQS)), 0.0), axis=1, keepdims=True)


def as_row(column):
    r = lax.broadcasted_iota(jnp.int32, (SEQS, 128), 0)
    c = lax.broadcasted_iota(jnp.int32, (SEQS, 128), 1)
    return jnp.sum(jnp.where(r == c, jnp.broadcast_to(column, (SEQS, 128)), 0.0), axis=0, keepdims=True)


def two_parts(values, width):
    high = values.astype(BF16).astype(F32)
    rows = values.shape[0]
    lane = lax.broadcasted_iota(jnp.int32, (rows, 2 * width), 1)
    return jnp.where(
        lane < width, jnp.broadcast_to(high, (rows, 2 * width)), jnp.broadcast_to(values - high, (rows, 2 * width))
    ).astype(BF16)


def kernel(
    hidden_in, state_in, conv_x_in, conv_bc_in, tokens_in, ref_in, in_z, in_x, in_bc, dt_in, out_t, lm_in,
    conv_wx_in, conv_bx, conv_wbc_in, conv_bbc_in, dt_bias_in, a_log_in, skip_in, norm_in, norm_gain, final_gain,
    state, div_out, logprob_out, zg, xg, bg, dt_out, og,
    dg, lm, refs, hsend, hrecv, gains, psend, precv, gsend, grecv, rsend, rrecv, usend, urecv, lsend, lrecv,
    ssend, srecv, decays, b_rows, x_cols, c_rows, y_acc,
    hidden, conv_x, conv_bc, tokens, in_dt, conv_wx, conv_wbc, conv_bbc, dt_bias, a_log, skip_gain,
    long_rows, short_rows, small, loc, chain_s, chain_r, ag_s, ag_r, d2_s, d2_own, d2_r,
):
    g = lax.axis_index("group")
    h = lax.axis_index("head")
    k = g // 2
    c = g % 2
    x = k // 2
    zl = k % 2
    sibling = (2 * k + 1 - c, h)

    barrier = pltpu.get_barrier_semaphore()
    for d in range(1, 8):
        pl.semaphore_signal(barrier, inc=1, device_id=(g, (h + d) % 8), device_id_type=MESH)
        pl.semaphore_signal(barrier, inc=1, device_id=(2 * ((k + d) % 8) + c, h), device_id_type=MESH)
    pl.semaphore_signal(barrier, inc=1, device_id=sibling, device_id_type=MESH)

    rows_mine = pl.ds(pl.multiple_of(g * SHARD, SHARD), SHARD)
    lm_mine = pl.ds(pl.multiple_of(c * SHARD, SHARD), SHARD)
    lm_other = pl.ds(pl.multiple_of((1 - c) * SHARD, SHARD), SHARD)
    first = [
        pltpu.make_async_copy(source, target, small.at[at])
        for at, (source, target) in enumerate(
            [
                (hidden_in, hidden), (norm_in, long_rows.at[0]), (dt_in, in_dt), (final_gain, long_rows.at[1]),
                (conv_x_in, conv_x), (conv_bc_in, conv_bc), (tokens_in, tokens), (conv_wx_in, conv_wx),
                (conv_wbc_in, conv_wbc), (conv_bbc_in, conv_bbc), (dt_bias_in, dt_bias), (a_log_in, a_log),
                (skip_in, skip_gain), (conv_bx, short_rows.at[0]), (norm_gain, short_rows.at[1]),
            ]
        )
    ]
    local = [
        pltpu.make_async_copy(source, target, loc.at[at])
        for at, (source, target) in enumerate(
            [
                (in_x, xg.at[rows_mine]), (in_bc, bg.at[rows_mine]), (in_z, zg.at[rows_mine]),
                (out_t, og.at[rows_mine]), (lm_in, lm.at[lm_mine]), (state_in, state), (ref_in, refs),
            ]
        )
    ]
    for copy in first + local:
        copy.start()
    first[0].wait()

    for j in range(CHIPS):
        hsend[j] = hidden[:, SLICE * j : SLICE * (j + 1)]

    pl.semaphore_wait(barrier, 15)

    def chain_copy(phase, src, dst, device):
        return pltpu.make_async_remote_copy(
            src_ref=src, dst_ref=dst, send_sem=chain_s.at[phase], recv_sem=chain_r.at[phase],
            device_id=device, device_id_type=MESH,
        )

    pending = []

    def to_chips(phase, send_slot, recv):
        for d in range(1, 8):
            j = (k + d) % 8
            chain_copy(phase, send_slot(j), recv.at[k], (2 * j + c, h)).start()
        pending.append(chain_copy(phase, recv.at[pl.ds(0, 7)], recv.at[pl.ds(0, 7)], sibling))

    def to_heads(phase, send_slot, recv):
        for d in range(1, 8):
            j = (h + d) % 8
            chain_copy(phase, send_slot(j), recv.at[h], (g, j)).start()
        pending.append(chain_copy(phase, recv.at[pl.ds(0, 7)], recv.at[pl.ds(0, 7)], sibling))

    def received(phase, recv):
        chain_copy(phase, recv.at[pl.ds(0, 7)], recv.at[pl.ds(0, 7)], sibling).wait_recv()

    buffers = {"x": xg, "z": zg, "o": og, "b": bg, "d": dg}

    def region(piece, dx, dz, core):
        name, begin, rows = PIECES[piece]
        at = ((((x + dx) % 4) * 2 + (zl + dz) % 2) * 2 + core) * SHARD + begin
        return buffers[name].at[pl.ds(pl.multiple_of(at, 16), rows)]

    def ici(piece, dx, dz, ways):
        for way in ways:
            move = {"+": 1, "-": 3, "z": 0}[way]
            rx, rz = (dx - move) % 4, (dz + (way == "z")) % 2
            chip = ((x + move) % 4) * 2 + (zl + (way == "z")) % 2
            block = region(piece, dx, dz, c)
            pltpu.make_async_remote_copy(
                src_ref=block, dst_ref=block, send_sem=ag_s.at[ARRAYS.index(PIECES[piece][0])],
                recv_sem=ag_r.at[ORDER[piece], 4 * rz + rx - 1], device_id=(2 * chip + c, h), device_id_type=MESH,
            ).start()

    def on_chip(block, name, sem):
        pltpu.make_async_remote_copy(
            src_ref=block, dst_ref=block, send_sem=d2_s.at[ARRAYS.index(name)], recv_sem=sem,
            device_id=sibling, device_id_type=MESH,
        ).start()

    def share_own(name):
        on_chip(buffers[name].at[rows_mine], name, d2_own.at[ARRAYS.index(name)])

    def sibling_own(name):
        rows = buffers[name].at[pl.ds(pl.multiple_of((2 * k + 1 - c) * SHARD, SHARD), SHARD)]
        pltpu.make_async_remote_copy(
            src_ref=rows, dst_ref=rows, send_sem=d2_s.at[ARRAYS.index(name)], recv_sem=d2_own.at[ARRAYS.index(name)],
            device_id=sibling, device_id_type=MESH,
        ).wait_recv()

    waited = set()

    def arrived(piece, dx, dz):
        block = region(piece, dx, dz, c)
        name = PIECES[piece][0]
        pltpu.make_async_remote_copy(
            src_ref=block, dst_ref=block, send_sem=d2_s.at[ARRAYS.index(name)],
            recv_sem=ag_r.at[ORDER[piece], 4 * dz + dx - 1], device_id=sibling, device_id_type=MESH,
        ).wait_recv()
        waited.add((piece, dx, dz))
        on_chip(block, name, d2_r.at[ARRAYS.index(name)])

    to_chips(0, lambda j: hsend.at[j], hrecv)
    local[0].wait()
    share_own("x")
    local[1].wait()
    share_own("b")
    local[2].wait()
    share_own("z")
    ici("X", 0, 0, "+-")
    ici("Z", 0, 0, "z")
    hrecv[k] = hsend[k]
    for copy in first[1:]:
        copy.wait()
    turned = jnp.transpose(jnp.concatenate([in_dt[...].astype(F32), jnp.zeros((128 - HEADS, SHARD), F32)], axis=0))
    dg[rows_mine, :] = turned.astype(BF16)
    for j in range(CHIPS):
        gains[0, j] = long_rows[0:1, SLICE * j : SLICE * (j + 1)]
        gains[1, j] = long_rows[1:2, SLICE * j : SLICE * (j + 1)]
    whole = hidden[...].astype(F32)
    scale_in = lax.rsqrt(jnp.mean(whole * whole, axis=-1, keepdims=True) + EPSILON)
    share_own("d")
    local[3].wait()
    local[4].wait()

    received(0, hrecv)
    gain = gains[0, k]
    lhs = (hrecv[...].astype(F32) * gain[None]).astype(BF16).reshape(CHIPS * SEQS, SLICE)
    slice_rows = pl.ds(pl.multiple_of(k * SLICE, SLICE), SLICE)

    def partial(weights, at, width):
        product = jnp.dot(lhs, weights[slice_rows, :], preferred_element_type=F32)
        psend[:, :, at : at + width] = product.astype(BF16).reshape(CHIPS, SEQS, width)

    sibling_own("x")
    partial(xg, 0, 640)
    sibling_own("b")
    partial(bg, 640, 256)
    sibling_own("d")
    partial(dg, 896, 128)
    to_chips(1, lambda j: psend.at[j, :, pl.ds(0, 1024)], precv.at[:, :, pl.ds(0, 1024)])
    sibling_own("z")
    partial(zg, 1024, 640)
    to_chips(2, lambda j: psend.at[j, :, pl.ds(1024, 640)], precv.at[:, :, pl.ds(1024, 640)])
    precv[k] = psend[k]
    arrived("Z", 0, 1)
    ici("Z", 0, 0, "+-")
    ici("OL", 0, 0, "+-")
    ici("X", 0, 0, "z")
    ici("BC", 0, 0, "z")
    share_own("o")
    lm_copy = pltpu.make_async_remote_copy(
        src_ref=lm.at[lm_mine], dst_ref=lm.at[lm_mine], send_sem=loc.at[7], recv_sem=loc.at[8],
        device_id=sibling, device_id_type=MESH,
    )
    lm_copy.start()

    received(1, precv.at[:, :, pl.ds(0, 1024)])
    summed = jnp.sum(precv[:, :, 0:1024].astype(F32), axis=0) * scale_in
    x_new = summed[:, 0:640]
    bc_new = summed[:, 640:896]
    step_raw = summed[:, 896 : 896 + HEADS]
    acc = x_new * conv_wx[3:4, :] + short_rows[0:1, :]
    acc_bc = bc_new * conv_wbc[3:4, :] + conv_bbc[...]
    for tap in range(3):
        acc = acc + conv_x[tap].astype(F32) * conv_wx[tap : tap + 1, :]
        acc_bc = acc_bc + conv_bc[tap].astype(F32) * conv_wbc[tap : tap + 1, :]
    x_conv = silu(acc)
    bc_conv = silu(acc_bc)
    b_rows[...] = bc_conv[:, :N]
    c_vals = bc_conv[:, N:]
    biased = step_raw + dt_bias[...]
    step = jnp.maximum(biased, 0.0) + jnp.log1p(jnp.exp(-jnp.abs(biased)))
    decay = jnp.exp(-step * jnp.exp(a_log[...]))
    square = jnp.concatenate(
        [jnp.concatenate([decay, jnp.zeros((SEQS, 128 - HEADS), F32)], axis=1), jnp.zeros((112, 128), F32)], axis=0
    )
    decays[...] = jnp.transpose(square)[0:SEQS]
    inflow = per_head(step) * x_conv
    x_cols[...] = jnp.transpose(jnp.concatenate([inflow, jnp.zeros((112, DI), F32)], axis=0))
    c_high = c_vals.astype(BF16)
    c_low = (c_vals - c_high.astype(F32)).astype(BF16)
    c_rows[...] = jnp.concatenate([c_high, c_low], axis=0)
    local[5].wait()

    def two_heads(pair, _):
        rows = pl.ds(pl.multiple_of(pair * 128, 128), 128)
        columns = x_cols[rows, :]
        left = decays[pl.ds(2 * pair, 1), :]
        right = decays[pl.ds(2 * pair + 1, 1), :]
        both = c_rows[...]
        row = lax.broadcasted_iota(jnp.int32, (SEQS, N), 0)
        total = jnp.zeros((SEQS, N), F32)
        for s in range(SEQS):
            factor = jnp.concatenate(
                [
                    jnp.broadcast_to(left[:, s : s + 1], (P_SIZE, N)),
                    jnp.broadcast_to(right[:, s : s + 1], (P_SIZE, N)),
                ],
                axis=0,
            )
            column = jnp.broadcast_to(columns[:, s : s + 1], (2 * P_SIZE, N))
            new = state[s, rows, :] * factor + column * b_rows[s : s + 1, :]
            state[s, rows, :] = new
            seen = lax.dot_general(both, new.astype(BF16), (((1,), (1,)), ((), ())), preferred_element_type=F32)
            total = total + jnp.where(row == s, seen[0:SEQS] + seen[SEQS:], 0.0)
        y_acc[:, rows] = total
        return 0

    lax.fori_loop(0, HEADS // 2, two_heads, 0)
    received(2, precv.at[:, :, pl.ds(1024, 640)])
    gate = jnp.sum(precv[:, :, 1024:1664].astype(F32), axis=0) * scale_in
    ssm_out = y_acc[...] + per_head(skip_gain[...]) * x_conv
    gated = ssm_out * silu(gate)
    squares = jnp.sum(gated * gated, axis=-1, keepdims=True)
    gsend[:, 0:640] = (gated * short_rows[1:2, :]).astype(BF16)
    gsend[:, 640:768] = two_parts(squares, 64)

    to_chips(3, lambda j: gsend, grecv)
    grecv[k] = gsend[...]
    arrived("X", 3, 0)
    arrived("X", 1, 0)
    ici("X", 3, 0, "z")
    ici("X", 3, 0, "+")
    ici("Z", 0, 1, "+-")
    ici("BC", 0, 0, "+-")
    ici("DT", 0, 0, "+-")
    ici("OH", 0, 0, "z")
    ici("DT", 0, 0, "z")

    sibling_own("o")
    received(3, grecv)
    mixed = lax.dot_general(
        grecv[:, :, 0:640].reshape(CHIPS * SEQS, 640), og[slice_rows, :], (((1,), (1,)), ((), ())),
        preferred_element_type=F32,
    )
    parts = grecv[:, :, 640:768].astype(F32)
    sq = (parts[:, :, 0:1] + parts[:, :, 64:65]).reshape(CHIPS * SEQS, 1)
    rsend[:, :, 0:SLICE] = mixed.astype(BF16).reshape(CHIPS, SEQS, SLICE)
    rsend[:, :, SLICE:384] = two_parts(sq, 32).reshape(CHIPS, SEQS, 64)
    to_heads(4, lambda j: rsend.at[j], rrecv)
    rrecv[h] = rsend[h]
    ici("OH", 0, 0, "+-")
    arrived("Z", 3, 0)
    ici("Z", 3, 0, "+")
    ici("X", 1, 0, "z")
    received(4, rrecv)
    total = jnp.sum(rrecv[...].astype(F32), axis=0)
    scale_gate = lax.rsqrt((total[:, SLICE : SLICE + 1] + total[:, SLICE + 32 : SLICE + 33]) / (8.0 * DI) + EPSILON)
    stream = hrecv[h].astype(F32) + total[:, 0:SLICE] * scale_gate
    usend[:, 0:SLICE] = (stream * gains[1, k]).astype(BF16)
    usend[:, SLICE:384] = two_parts(jnp.sum(stream * stream, axis=-1, keepdims=True), 32)

    to_heads(5, lambda j: usend, urecv)
    urecv[h] = usend[...]
    arrived("Z", 1, 1)
    ici("Z", 1, 1, "-")
    arrived("OL", 1, 0)
    ici("OL", 1, 0, "-")

    local[6].wait()
    pltpu.make_async_remote_copy(
        src_ref=lm.at[lm_other], dst_ref=lm.at[lm_other], send_sem=loc.at[7], recv_sem=loc.at[8],
        device_id=sibling, device_id_type=MESH,
    ).wait_recv()
    received(5, urecv)
    final = urecv[:, :, 0:SLICE].reshape(CHIPS * SEQS, SLICE)

    def some_logits(block, _):
        at = pl.ds(pl.multiple_of(block * 640, 640), 640)
        product = jnp.dot(final, lm[:, at], preferred_element_type=F32)
        lsend[:, :, at] = product.astype(BF16).reshape(CHIPS, SEQS, 640)
        return 0

    cut = 1920
    lax.fori_loop(0, cut // 640, some_logits, 0)
    to_chips(6, lambda j: lsend.at[j, :, pl.ds(0, cut)], lrecv.at[:, :, pl.ds(0, cut)])
    lax.fori_loop(cut // 640, VL // 640, some_logits, 0)
    lsend[:, :, VL : VL + 64] = urecv[:, :, SLICE:384]
    lsend[:, :, VL + 64 : VL + 128] = urecv[:, :, SLICE:384]
    to_chips(8, lambda j: lsend.at[j, :, pl.ds(cut, VL + 128 - cut)], lrecv.at[:, :, pl.ds(cut, VL + 128 - cut)])
    lrecv[k] = lsend[k]

    ici("OL", 0, 0, "z")
    arrived("X", 2, 0)
    ici("X", 2, 0, "z")
    arrived("OL", 3, 0)
    ici("OL", 1, 0, "z")
    ici("OL", 3, 0, "z")
    arrived("BC", 0, 1)
    ici("BC", 0, 1, "+-")
    arrived("OH", 0, 1)
    ici("OH", 0, 1, "+-")
    arrived("DT", 0, 1)
    ici("DT", 0, 1, "+-")
    arrived("DT", 1, 0)
    ici("DT", 1, 0, "-")
    arrived("BC", 3, 0)
    ici("BC", 3, 0, "+")
    arrived("OH", 3, 0)
    ici("OH", 3, 0, "+")

    reference = refs[...].astype(F32)
    ref_max = jnp.max(reference, axis=-1, keepdims=True)
    weight = jnp.exp(reference - ref_max)
    ref_sum = jnp.sum(weight, axis=-1, keepdims=True)
    token = as_column(tokens[...].astype(F32)).astype(jnp.int32)

    received(6, lrecv.at[:, :, pl.ds(0, cut)])
    received(8, lrecv.at[:, :, pl.ds(cut, VL + 128 - cut)])
    logits = jnp.sum(lrecv[:, :, 0:VL].astype(F32), axis=0)
    tail = jnp.sum(lrecv[:, :, VL : VL + 128].astype(F32), axis=0)
    logits = logits * lax.rsqrt((tail[:, 0:1] + tail[:, 32:33]) / D + EPSILON)
    roll_max = jnp.max(logits, axis=-1, keepdims=True)
    roll_sum = jnp.sum(jnp.exp(logits - roll_max), axis=-1, keepdims=True)
    cross = jnp.sum(weight * (reference - logits), axis=-1, keepdims=True)
    column = lax.broadcasted_iota(jnp.int32, (SEQS, VL), 1) + h * VL
    picked = jnp.sum(jnp.where(column == token, logits, 0.0), axis=-1, keepdims=True)
    lane = lax.broadcasted_iota(jnp.int32, (SEQS, 128), 1)
    packed = jnp.zeros((SEQS, 128), F32)
    for at, value in enumerate((roll_max, roll_sum, ref_max, ref_sum, cross, picked)):
        packed = jnp.where(lane == at, jnp.broadcast_to(value, (SEQS, 128)), packed)
    ssend[...] = packed

    to_heads(7, lambda j: ssend, srecv)
    srecv[h] = ssend[...]

    arrived("BC", 1, 1)
    ici("BC", 1, 1, "-")
    arrived("OH", 1, 1)
    ici("OH", 1, 1, "-")
    arrived("DT", 1, 1)
    ici("DT", 1, 1, "-")
    arrived("OL", 2, 0)
    ici("OL", 2, 0, "z")

    received(7, srecv)
    every = srecv[...]
    m_all, s_all, rm_all, rs_all, x_all, p_all = (every[:, :, at : at + 1] for at in range(6))
    roll_top = jnp.max(m_all, axis=0)
    roll_total = jnp.sum(s_all * jnp.exp(m_all - roll_top[None]), axis=0)
    ref_top = jnp.max(rm_all, axis=0)
    ref_scale = jnp.exp(rm_all - ref_top[None])
    ref_total = jnp.sum(rs_all * ref_scale, axis=0)
    cross_total = jnp.sum(x_all * ref_scale, axis=0)
    lse_roll = roll_top + jnp.log(roll_total)
    lse_ref = ref_top + jnp.log(ref_total)
    divergence = cross_total / ref_total - lse_ref + lse_roll
    logprob = jnp.sum(p_all, axis=0) - lse_roll
    div_out[...] = as_row(divergence)[:, 0:SEQS]
    logprob_out[...] = as_row(logprob)[:, 0:SEQS]

    for piece in PIECES:
        for dz in range(2):
            for dx in range(4):
                if (dx, dz) != (0, 0) and (piece, dx, dz) not in waited:
                    arrived(piece, dx, dz)
    seven, eight = pl.ds(0, 7 * SHARD), pl.ds(0, 8 * SHARD)
    for at, name in enumerate(ARRAYS):
        whole = buffers[name].at[seven]
        pltpu.make_async_remote_copy(
            src_ref=whole, dst_ref=whole, send_sem=ag_s.at[at], recv_sem=d2_r.at[at], device_id=sibling,
            device_id_type=MESH,
        ).wait()
    for block in range(2):
        turned = jnp.transpose(dg[block * 1280 : (block + 1) * 1280, :].astype(F32))
        dt_out[:, block * 1280 : (block + 1) * 1280] = turned[0:HEADS].astype(BF16)
    for at, name in enumerate(ARRAYS):
        whole = buffers[name].at[eight]
        pltpu.make_async_remote_copy(
            src_ref=whole, dst_ref=whole, send_sem=d2_s.at[at], recv_sem=d2_r.at[at], device_id=sibling,
            device_id_type=MESH,
        ).wait_send()
    lm_copy.wait_send()
    for copy in pending:
        copy.wait_send()


def write_out(*refs):
    count = len(refs) // 2
    copies = [pltpu.make_async_copy(refs[at], refs[count + at], refs[-1].at[at]) for at in range(count)]
    for copy in copies:
        copy.start()
    for copy in copies:
        copy.wait()


ANY = pl.BlockSpec(memory_space=pl.ANY)
VMEM = pl.BlockSpec(memory_space=pltpu.VMEM)


def shards(
    hidden_in, ssm_state, conv_x_state, conv_bc_state, token_ids, ref_logits, in_z, in_x, in_bc, in_dt, out_t,
    lm_head, conv_wx, conv_bx, conv_wbc, conv_bbc, dt_bias, a_log, skip_gain, norm_in, norm_gain, final_gain,
):
    row = lambda v: v.reshape(1, -1)
    results = (
        ((SEQS, DI, N), F32), ((1, SEQS), F32), ((1, SEQS), F32), ((D, DI), BF16), ((D, DI), BF16), ((D, 256), BF16),
        ((HEADS, D), BF16), ((D, DI), BF16),
    )
    held = pl.pallas_call(
        kernel,
        out_shape=tuple(pltpu.VMEM(shape, dtype) for shape, dtype in results),
        in_specs=[pl.BlockSpec(memory_space=pltpu.HBM)] * 22,
        out_specs=(VMEM,) * len(results),
        scratch_shapes=[
            pltpu.VMEM((D, 128), BF16),
            pltpu.VMEM((SLICE, VL), BF16),
            pltpu.VMEM((SEQS, VL), BF16),
            pltpu.VMEM((CHIPS, SEQS, SLICE), BF16),
            pltpu.VMEM((CHIPS, SEQS, SLICE), BF16),
            pltpu.VMEM((2, CHIPS, 1, SLICE), F32),
            pltpu.VMEM((CHIPS, SEQS, 1664), BF16),
            pltpu.VMEM((CHIPS, SEQS, 1664), BF16),
            pltpu.VMEM((SEQS, 768), BF16),
            pltpu.VMEM((CHIPS, SEQS, 768), BF16),
            pltpu.VMEM((CHIPS, SEQS, 384), BF16),
            pltpu.VMEM((CHIPS, SEQS, 384), BF16),
            pltpu.VMEM((SEQS, 384), BF16),
            pltpu.VMEM((CHIPS, SEQS, 384), BF16),
            pltpu.VMEM((CHIPS, SEQS, VL + 128), BF16),
            pltpu.VMEM((CHIPS, SEQS, VL + 128), BF16),
            pltpu.VMEM((SEQS, 128), F32),
            pltpu.VMEM((CHIPS, SEQS, 128), F32),
            pltpu.VMEM((SEQS, 128), F32),
            pltpu.VMEM((SEQS, N), F32),
            pltpu.VMEM((DI, 128), F32),
            pltpu.VMEM((2 * SEQS, N), BF16),
            pltpu.VMEM((SEQS, DI), F32),
            pltpu.VMEM((SEQS, D), BF16),
            pltpu.VMEM((3, SEQS, DI), BF16),
            pltpu.VMEM((3, SEQS, 256), BF16),
            pltpu.VMEM((1, SEQS), jnp.int32),
            pltpu.VMEM((HEADS, SHARD), BF16),
            pltpu.VMEM((4, DI), F32),
            pltpu.VMEM((4, 256), F32),
            pltpu.VMEM((1, 256), F32),
            pltpu.VMEM((1, HEADS), F32),
            pltpu.VMEM((1, HEADS), F32),
            pltpu.VMEM((1, HEADS), F32),
            pltpu.VMEM((2, D), F32),
            pltpu.VMEM((2, DI), F32),
            pltpu.SemaphoreType.DMA((15,)),
            pltpu.SemaphoreType.DMA((9,)),
            pltpu.SemaphoreType.DMA((9,)),
            pltpu.SemaphoreType.DMA((9,)),
            pltpu.SemaphoreType.DMA((5,)),
            pltpu.SemaphoreType.DMA((6, 7)),
            pltpu.SemaphoreType.DMA((5,)),
            pltpu.SemaphoreType.DMA((5,)),
            pltpu.SemaphoreType.DMA((5,)),
        ],
        compiler_params=pltpu.CompilerParams(
            collective_id=0, has_side_effects=True, vmem_limit_bytes=32 * 1024 * 1024
        ),
    )(*[pltpu.with_memory_space_constraint(array, pltpu.HBM) for array in (
        hidden_in, ssm_state.reshape(SEQS, DI, N), conv_x_state.transpose(1, 0, 2), conv_bc_state.transpose(1, 0, 2),
        row(token_ids), ref_logits, in_z, in_x, in_bc, in_dt.T, out_t, lm_head.T,
        conv_wx, conv_bx, conv_wbc, row(conv_bbc), row(dt_bias), row(a_log), row(skip_gain), norm_in,
        norm_gain, final_gain,
    )])
    held = [pltpu.with_memory_space_constraint(array, pltpu.VMEM) for array in held]
    state, divergence, logprob, roll_z, roll_x, roll_bc, dt_rows, roll_out = pl.pallas_call(
        write_out,
        out_shape=tuple(jax.ShapeDtypeStruct(shape, dtype) for shape, dtype in results),
        in_specs=[VMEM] * len(results),
        out_specs=(ANY,) * len(results),
        scratch_shapes=[pltpu.SemaphoreType.DMA((len(results),))],
        compiler_params=pltpu.CompilerParams(vmem_limit_bytes=1024 * 1024),
    )(*held)
    return (
        state.reshape(ssm_state.shape), divergence.reshape(SEQS), logprob.reshape(SEQS), roll_z, roll_x, roll_bc,
        dt_rows.T, roll_out,
    )


def solution(mesh):
    spread = P("group", "head")
    return jax.shard_map(
        shards,
        mesh=mesh,
        in_specs=(
            P("group", None), P("group", "head", None, None), P("group", None, "head"), P("group", None, None),
            P("group"), spread, spread, spread, P("group", None), spread, spread, P("head", "group"),
            P(None, "head"), P("head"), P(), P(), P("head"), P("head"), P("head"), P(), P("head"), P(),
        ),
        out_specs=(
            P("group", "head", None, None), P("group"), P("group"), P(None, "head"), P(None, "head"), P(),
            P(None, "head"), P(None, "head"),
        ),
        check_vma=False,
    )
```

```python
import functools

import jax
import jax.numpy as jnp
from jax import lax
from jax.experimental import pallas as pl
from jax.experimental.pallas import tpu as pltpu
from jax.sharding import PartitionSpec as P

MESH = pl.DeviceIdType.MESH
EPSILON = 1e-05
SEQS, D, DI, HEADS, P_SIZE, N = 16, 2560, 640, 10, 64, 128
SHARD = 160
SLICE = 320
CHIPS = 8
VL = 3200
F32 = jnp.float32
BF16 = jnp.bfloat16

PIECES = {
    "X": ("x", 0, 160),
    "OL": ("o", 0, 64),
    "DT": ("d", 0, 160),
    "Z": ("z", 0, 160),
    "BC": ("b", 0, 160),
    "OH": ("o", 64, 96),
}
ORDER = {name: at for at, name in enumerate(PIECES)}
ARRAYS = "xobdz"


def silu(v):
    return v / (1.0 + jnp.exp(-v))


def per_head(values):
    rows = values.shape[0]
    lane = lax.broadcasted_iota(jnp.int32, (rows, 128), 1)
    parts = []
    for pair in range(HEADS // 2):
        left = jnp.broadcast_to(values[:, 2 * pair : 2 * pair + 1], (rows, 128))
        right = jnp.broadcast_to(values[:, 2 * pair + 1 : 2 * pair + 2], (rows, 128))
        parts.append(jnp.where(lane < P_SIZE, left, right))
    return jnp.concatenate(parts, axis=1)


def as_column(row):
    r = lax.broadcasted_iota(jnp.int32, (SEQS, SEQS), 0)
    c = lax.broadcasted_iota(jnp.int32, (SEQS, SEQS), 1)
    return jnp.sum(jnp.where(r == c, jnp.broadcast_to(row, (SEQS, SEQS)), 0.0), axis=1, keepdims=True)


def as_row(column):
    r = lax.broadcasted_iota(jnp.int32, (SEQS, 128), 0)
    c = lax.broadcasted_iota(jnp.int32, (SEQS, 128), 1)
    return jnp.sum(jnp.where(r == c, jnp.broadcast_to(column, (SEQS, 128)), 0.0), axis=0, keepdims=True)


def two_parts(values, width):
    high = values.astype(BF16).astype(F32)
    rows = values.shape[0]
    lane = lax.broadcasted_iota(jnp.int32, (rows, 2 * width), 1)
    return jnp.where(
        lane < width, jnp.broadcast_to(high, (rows, 2 * width)), jnp.broadcast_to(values - high, (rows, 2 * width))
    ).astype(BF16)


def kernel(
    hidden_in, state_in, conv_x_in, conv_bc_in, tokens_in, ref_in, in_z, in_x, in_bc, dt_in, out_t, lm_in,
    conv_wx_in, conv_bx, conv_wbc_in, conv_bbc_in, dt_bias_in, a_log_in, skip_in, norm_in, norm_gain, final_gain,
    state, div_out, logprob_out, zg, xg, bg, dt_out, og,
    dts, lm, refs, hsend, hrecv, gains, psend, precv, gsend, grecv, rsend, rrecv, usend, urecv, lsend, lrecv,
    ssend, srecv, decays, b_rows, x_cols, c_rows, y_acc,
    hidden, conv_x, conv_bc, tokens, conv_wx, conv_wbc, conv_bbc, dt_bias, a_log, skip_gain,
    long_rows, short_rows, small, loc, chain_s, chain_r, ag_s, ag_r, d2_s, d2_own, d2_r, y_sems,
):
    g = lax.axis_index("group")
    h = lax.axis_index("head")
    k = g // 2
    c = g % 2
    x = k // 2
    zl = k % 2
    y = h // 2
    sibling = (2 * k + 1 - c, h)

    barrier = pltpu.get_barrier_semaphore()
    for d in range(1, 8):
        pl.semaphore_signal(barrier, inc=1, device_id=(g, (h + d) % 8), device_id_type=MESH)
        pl.semaphore_signal(barrier, inc=1, device_id=(2 * ((k + d) % 8) + c, h), device_id_type=MESH)
    pl.semaphore_signal(barrier, inc=1, device_id=sibling, device_id_type=MESH)

    rows_mine = pl.ds(pl.multiple_of(g * SHARD, SHARD), SHARD)
    lm_mine = pl.ds(pl.multiple_of(c * SHARD, SHARD), SHARD)
    lm_other = pl.ds(pl.multiple_of((1 - c) * SHARD, SHARD), SHARD)
    first = [
        pltpu.make_async_copy(source, target, small.at[at])
        for at, (source, target) in enumerate(
            [
                (hidden_in, hidden), (dt_in, dts.at[g]), (norm_in, long_rows.at[0]), (final_gain, long_rows.at[1]),
                (conv_x_in, conv_x), (conv_bc_in, conv_bc), (tokens_in, tokens), (conv_wx_in, conv_wx),
                (conv_wbc_in, conv_wbc), (conv_bbc_in, conv_bbc), (dt_bias_in, dt_bias), (a_log_in, a_log),
                (skip_in, skip_gain), (conv_bx, short_rows.at[0]), (norm_gain, short_rows.at[1]),
            ]
        )
    ]
    local = [
        pltpu.make_async_copy(source, target, loc.at[at])
        for at, (source, target) in enumerate(
            [
                (in_x, xg.at[rows_mine]), (in_bc, bg.at[rows_mine]), (in_z, zg.at[rows_mine]),
                (out_t, og.at[rows_mine]), (lm_in, lm.at[lm_mine]), (state_in, state), (ref_in, refs),
            ]
        )
    ]
    for copy in first + local:
        copy.start()
    first[0].wait()

    for j in range(CHIPS):
        hsend[j] = hidden[:, SLICE * j : SLICE * (j + 1)]

    pl.semaphore_wait(barrier, 15)

    def chain_copy(phase, src, dst, device):
        return pltpu.make_async_remote_copy(
            src_ref=src, dst_ref=dst, send_sem=chain_s.at[phase], recv_sem=chain_r.at[phase],
            device_id=device, device_id_type=MESH,
        )

    pending = []

    def to_chips(phase, send_slot, recv):
        for d in range(1, 8):
            j = (k + d) % 8
            chain_copy(phase, send_slot(j), recv.at[k], (2 * j + c, h)).start()
        pending.append(chain_copy(phase, recv.at[pl.ds(0, 7)], recv.at[pl.ds(0, 7)], sibling))

    def to_heads(phase, send_slot, recv):
        for d in range(1, 8):
            j = (h + d) % 8
            chain_copy(phase, send_slot(j), recv.at[h], (g, j)).start()
        pending.append(chain_copy(phase, recv.at[pl.ds(0, 7)], recv.at[pl.ds(0, 7)], sibling))

    def received(phase, recv):
        chain_copy(phase, recv.at[pl.ds(0, 7)], recv.at[pl.ds(0, 7)], sibling).wait_recv()

    buffers = {"x": xg, "z": zg, "o": og, "b": bg, "d": dts}

    def quarter(device):
        at = pl.multiple_of(device * SHARD + 80 * (y // 2), 16)
        return bg.at[pl.ds(at, 80), pl.ds(pl.multiple_of(128 * (y % 2), 128), 128)]

    def region(piece, dx, dz, core):
        name, begin, rows = PIECES[piece]
        at = (((x + dx) % 4) * 2 + (zl + dz) % 2) * 2 + core
        if name == "d":
            return dts.at[at]
        if name == "b":
            return quarter(at)
        at = at * SHARD + begin
        return buffers[name].at[pl.ds(pl.multiple_of(at, 16), rows)]

    def ici(piece, dx, dz, ways):
        for way in ways:
            move = {"+": 1, "-": 3, "z": 0}[way]
            rx, rz = (dx - move) % 4, (dz + (way == "z")) % 2
            chip = ((x + move) % 4) * 2 + (zl + (way == "z")) % 2
            block = region(piece, dx, dz, c)
            pltpu.make_async_remote_copy(
                src_ref=block, dst_ref=block, send_sem=ag_s.at[ARRAYS.index(PIECES[piece][0])],
                recv_sem=ag_r.at[ORDER[piece], 4 * rz + rx - 1], device_id=(2 * chip + c, h), device_id_type=MESH,
            ).start()

    def on_chip(block, name, sem):
        pltpu.make_async_remote_copy(
            src_ref=block, dst_ref=block, send_sem=d2_s.at[ARRAYS.index(name)], recv_sem=sem,
            device_id=sibling, device_id_type=MESH,
        ).start()

    def shard_of(name, device):
        if name == "d":
            return dts.at[device]
        return buffers[name].at[pl.ds(pl.multiple_of(device * SHARD, SHARD), SHARD)]

    def along_y():
        return pltpu.make_async_remote_copy(
            src_ref=bg.at[pl.ds(0, 840)], dst_ref=bg.at[pl.ds(0, 840)], send_sem=y_sems.at[0], recv_sem=y_sems.at[1],
            device_id=sibling, device_id_type=MESH,
        )

    def several(name, shards):
        return buffers[name].at[pl.ds(0, shards if name == "d" else shards * SHARD)]

    def share_own(name):
        on_chip(shard_of(name, g), name, d2_own.at[ARRAYS.index(name)])

    def sibling_own(name):
        rows = shard_of(name, 2 * k + 1 - c)
        pltpu.make_async_remote_copy(
            src_ref=rows, dst_ref=rows, send_sem=d2_s.at[ARRAYS.index(name)], recv_sem=d2_own.at[ARRAYS.index(name)],
            device_id=sibling, device_id_type=MESH,
        ).wait_recv()

    waited = set()

    def arrived(piece, dx, dz):
        block = region(piece, dx, dz, c)
        name = PIECES[piece][0]
        pltpu.make_async_remote_copy(
            src_ref=block, dst_ref=block, send_sem=d2_s.at[ARRAYS.index(name)],
            recv_sem=ag_r.at[ORDER[piece], 4 * dz + dx - 1], device_id=sibling, device_id_type=MESH,
        ).wait_recv()
        waited.add((piece, dx, dz))
        if name == "b":
            for move in range(1, 4):
                pltpu.make_async_remote_copy(
                    src_ref=block, dst_ref=block, send_sem=y_sems.at[0], recv_sem=y_sems.at[1],
                    device_id=(g, (h + 2 * move) % 8), device_id_type=MESH,
                ).start()
            return
        on_chip(block, name, d2_r.at[ARRAYS.index(name)])

    to_chips(0, lambda j: hsend.at[j], hrecv)
    local[0].wait()
    share_own("x")
    local[1].wait()
    share_own("b")
    local[2].wait()
    share_own("z")
    first[1].wait()
    share_own("d")
    ici("X", 0, 0, "+-")
    ici("Z", 0, 0, "z")
    hrecv[k] = hsend[k]
    for copy in first[2:]:
        copy.wait()
    for j in range(CHIPS):
        gains[0, j] = long_rows[0:1, SLICE * j : SLICE * (j + 1)]
        gains[1, j] = long_rows[1:2, SLICE * j : SLICE * (j + 1)]
    whole = hidden[...].astype(F32)
    scale_in = lax.rsqrt(jnp.mean(whole * whole, axis=-1, keepdims=True) + EPSILON)
    local[3].wait()
    local[4].wait()

    received(0, hrecv)
    gain = gains[0, k]
    lhs = (hrecv[...].astype(F32) * gain[None]).astype(BF16).reshape(CHIPS * SEQS, SLICE)
    slice_rows = pl.ds(pl.multiple_of(k * SLICE, SLICE), SLICE)

    def turned(device):
        rows = jnp.concatenate([dts[device].astype(F32), jnp.zeros((128 - HEADS, SHARD), F32)], axis=0)
        return jnp.transpose(rows).astype(BF16)

    def partial(weights, at, width):
        product = jnp.dot(lhs, weights, preferred_element_type=F32)
        psend[:, :, at : at + width] = product.astype(BF16).reshape(CHIPS, SEQS, width)

    sibling_own("x")
    partial(xg[slice_rows, :], 0, 640)
    sibling_own("b")
    partial(bg[slice_rows, :], 640, 256)
    sibling_own("d")
    partial(jnp.concatenate([turned(2 * k), turned(2 * k + 1)], axis=0), 896, 128)
    to_chips(1, lambda j: psend.at[j, :, pl.ds(0, 1024)], precv.at[:, :, pl.ds(0, 1024)])
    sibling_own("z")
    partial(zg[slice_rows, :], 1024, 640)
    to_chips(2, lambda j: psend.at[j, :, pl.ds(1024, 640)], precv.at[:, :, pl.ds(1024, 640)])
    precv[k] = psend[k]
    arrived("Z", 0, 1)
    ici("Z", 0, 0, "+-")
    ici("OL", 0, 0, "+-")
    ici("X", 0, 0, "z")
    ici("BC", 0, 0, "z")
    ici("DT", 0, 0, "z")
    share_own("o")
    lm_copy = pltpu.make_async_remote_copy(
        src_ref=lm.at[lm_mine], dst_ref=lm.at[lm_mine], send_sem=loc.at[7], recv_sem=loc.at[8],
        device_id=sibling, device_id_type=MESH,
    )
    lm_copy.start()

    received(1, precv.at[:, :, pl.ds(0, 1024)])
    summed = jnp.sum(precv[:, :, 0:1024].astype(F32), axis=0) * scale_in
    x_new = summed[:, 0:640]
    bc_new = summed[:, 640:896]
    step_raw = summed[:, 896 : 896 + HEADS]
    acc = x_new * conv_wx[3:4, :] + short_rows[0:1, :]
    acc_bc = bc_new * conv_wbc[3:4, :] + conv_bbc[...]
    for tap in range(3):
        acc = acc + conv_x[tap].astype(F32) * conv_wx[tap : tap + 1, :]
        acc_bc = acc_bc + conv_bc[tap].astype(F32) * conv_wbc[tap : tap + 1, :]
    x_conv = silu(acc)
    bc_conv = silu(acc_bc)
    b_rows[...] = bc_conv[:, :N]
    c_vals = bc_conv[:, N:]
    biased = step_raw + dt_bias[...]
    step = jnp.maximum(biased, 0.0) + jnp.log1p(jnp.exp(-jnp.abs(biased)))
    decay = jnp.exp(-step * jnp.exp(a_log[...]))
    square = jnp.concatenate(
        [jnp.concatenate([decay, jnp.zeros((SEQS, 128 - HEADS), F32)], axis=1), jnp.zeros((112, 128), F32)], axis=0
    )
    decays[...] = jnp.transpose(square)[0:SEQS]
    inflow = per_head(step) * x_conv
    x_cols[...] = jnp.transpose(jnp.concatenate([inflow, jnp.zeros((112, DI), F32)], axis=0))
    c_high = c_vals.astype(BF16)
    c_low = (c_vals - c_high.astype(F32)).astype(BF16)
    c_rows[...] = jnp.concatenate([c_high, c_low], axis=0)
    local[5].wait()

    def two_heads(pair, _):
        rows = pl.ds(pl.multiple_of(pair * 128, 128), 128)
        columns = x_cols[rows, :]
        left = decays[pl.ds(2 * pair, 1), :]
        right = decays[pl.ds(2 * pair + 1, 1), :]
        both = c_rows[...]
        row = lax.broadcasted_iota(jnp.int32, (SEQS, N), 0)
        total = jnp.zeros((SEQS, N), F32)
        for s in range(SEQS):
            factor = jnp.concatenate(
                [
                    jnp.broadcast_to(left[:, s : s + 1], (P_SIZE, N)),
                    jnp.broadcast_to(right[:, s : s + 1], (P_SIZE, N)),
                ],
                axis=0,
            )
            column = jnp.broadcast_to(columns[:, s : s + 1], (2 * P_SIZE, N))
            new = state[s, rows, :] * factor + column * b_rows[s : s + 1, :]
            state[s, rows, :] = new
            seen = lax.dot_general(both, new.astype(BF16), (((1,), (1,)), ((), ())), preferred_element_type=F32)
            total = total + jnp.where(row == s, seen[0:SEQS] + seen[SEQS:], 0.0)
        y_acc[:, rows] = total
        return 0

    lax.fori_loop(0, HEADS // 2, two_heads, 0)
    received(2, precv.at[:, :, pl.ds(1024, 640)])
    gate = jnp.sum(precv[:, :, 1024:1664].astype(F32), axis=0) * scale_in
    ssm_out = y_acc[...] + per_head(skip_gain[...]) * x_conv
    gated = ssm_out * silu(gate)
    squares = jnp.sum(gated * gated, axis=-1, keepdims=True)
    gsend[:, 0:640] = (gated * short_rows[1:2, :]).astype(BF16)
    gsend[:, 640:768] = two_parts(squares, 64)

    to_chips(3, lambda j: gsend, grecv)
    grecv[k] = gsend[...]
    arrived("X", 3, 0)
    ici("X", 3, 0, "z+")
    ici("DT", 0, 0, "+-")
    ici("BC", 0, 0, "+-")
    ici("Z", 0, 1, "+-")
    ici("OH", 0, 0, "z")
    arrived("X", 1, 0)

    sibling_own("o")
    received(3, grecv)
    mixed = lax.dot_general(
        grecv[:, :, 0:640].reshape(CHIPS * SEQS, 640), og[slice_rows, :], (((1,), (1,)), ((), ())),
        preferred_element_type=F32,
    )
    parts = grecv[:, :, 640:768].astype(F32)
    sq = (parts[:, :, 0:1] + parts[:, :, 64:65]).reshape(CHIPS * SEQS, 1)
    rsend[:, :, 0:SLICE] = mixed.astype(BF16).reshape(CHIPS, SEQS, SLICE)
    rsend[:, :, SLICE:384] = two_parts(sq, 32).reshape(CHIPS, SEQS, 64)
    to_heads(4, lambda j: rsend.at[j], rrecv)
    rrecv[h] = rsend[h]
    arrived("DT", 0, 1)
    ici("DT", 0, 1, "+-")
    arrived("BC", 0, 1)
    ici("BC", 0, 1, "+-")
    ici("OH", 0, 0, "+-")
    ici("X", 1, 0, "z")
    arrived("Z", 3, 0)
    ici("Z", 3, 0, "+")
    arrived("Z", 1, 0)
    arrived("Z", 1, 1)
    ici("Z", 1, 1, "-")
    received(4, rrecv)
    total = jnp.sum(rrecv[...].astype(F32), axis=0)
    scale_gate = lax.rsqrt((total[:, SLICE : SLICE + 1] + total[:, SLICE + 32 : SLICE + 33]) / (8.0 * DI) + EPSILON)
    stream = hrecv[h].astype(F32) + total[:, 0:SLICE] * scale_gate
    usend[:, 0:SLICE] = (stream * gains[1, k]).astype(BF16)
    usend[:, SLICE:384] = two_parts(jnp.sum(stream * stream, axis=-1, keepdims=True), 32)

    to_heads(5, lambda j: usend, urecv)
    urecv[h] = usend[...]
    arrived("DT", 1, 0)
    ici("DT", 1, 0, "-")
    arrived("DT", 1, 1)
    ici("DT", 1, 1, "-")
    arrived("BC", 3, 0)
    ici("BC", 3, 0, "+")
    arrived("BC", 1, 1)
    ici("BC", 1, 1, "-")
    arrived("OL", 1, 0)
    ici("OL", 1, 0, "-")
    ici("OL", 0, 0, "z")
    arrived("OL", 3, 0)
    arrived("X", 0, 1)
    arrived("X", 3, 1)
    arrived("BC", 1, 0)
    arrived("BC", 3, 1)
    arrived("DT", 3, 0)
    arrived("DT", 3, 1)

    local[6].wait()
    pltpu.make_async_remote_copy(
        src_ref=lm.at[lm_other], dst_ref=lm.at[lm_other], send_sem=loc.at[7], recv_sem=loc.at[8],
        device_id=sibling, device_id_type=MESH,
    ).wait_recv()
    received(5, urecv)
    final = urecv[:, :, 0:SLICE].reshape(CHIPS * SEQS, SLICE)

    def some_logits(block, _):
        at = pl.ds(pl.multiple_of(block * 640, 640), 640)
        product = jnp.dot(final, lm[:, at], preferred_element_type=F32)
        lsend[:, :, at] = product.astype(BF16).reshape(CHIPS, SEQS, 640)
        return 0

    cut = 1920
    lax.fori_loop(0, cut // 640, some_logits, 0)
    to_chips(6, lambda j: lsend.at[j, :, pl.ds(0, cut)], lrecv.at[:, :, pl.ds(0, cut)])
    lax.fori_loop(cut // 640, VL // 640, some_logits, 0)
    lsend[:, :, VL : VL + 64] = urecv[:, :, SLICE:384]
    lsend[:, :, VL + 64 : VL + 128] = urecv[:, :, SLICE:384]
    to_chips(8, lambda j: lsend.at[j, :, pl.ds(cut, VL + 128 - cut)], lrecv.at[:, :, pl.ds(cut, VL + 128 - cut)])
    lrecv[k] = lsend[k]

    arrived("OH", 0, 1)
    ici("OH", 0, 1, "+-")
    arrived("X", 2, 0)
    ici("X", 2, 0, "z")
    ici("OL", 1, 0, "z")
    ici("OL", 3, 0, "z")
    arrived("OH", 3, 0)
    ici("OH", 3, 0, "+")
    arrived("OL", 2, 0)
    ici("OL", 2, 0, "z")
    arrived("BC", 2, 0)
    arrived("BC", 2, 1)
    arrived("X", 1, 1)
    arrived("Z", 3, 1)
    arrived("OH", 1, 0)
    arrived("DT", 2, 0)
    arrived("DT", 2, 1)
    arrived("Z", 2, 0)
    arrived("Z", 2, 1)

    reference = refs[...].astype(F32)
    ref_max = jnp.max(reference, axis=-1, keepdims=True)
    weight = jnp.exp(reference - ref_max)
    ref_sum = jnp.sum(weight, axis=-1, keepdims=True)
    token = as_column(tokens[...].astype(F32)).astype(jnp.int32)

    received(6, lrecv.at[:, :, pl.ds(0, cut)])
    received(8, lrecv.at[:, :, pl.ds(cut, VL + 128 - cut)])
    logits = jnp.sum(lrecv[:, :, 0:VL].astype(F32), axis=0)
    tail = jnp.sum(lrecv[:, :, VL : VL + 128].astype(F32), axis=0)
    logits = logits * lax.rsqrt((tail[:, 0:1] + tail[:, 32:33]) / D + EPSILON)
    roll_max = jnp.max(logits, axis=-1, keepdims=True)
    roll_sum = jnp.sum(jnp.exp(logits - roll_max), axis=-1, keepdims=True)
    cross = jnp.sum(weight * (reference - logits), axis=-1, keepdims=True)
    column = lax.broadcasted_iota(jnp.int32, (SEQS, VL), 1) + h * VL
    picked = jnp.sum(jnp.where(column == token, logits, 0.0), axis=-1, keepdims=True)
    lane = lax.broadcasted_iota(jnp.int32, (SEQS, 128), 1)
    packed = jnp.zeros((SEQS, 128), F32)
    for at, value in enumerate((roll_max, roll_sum, ref_max, ref_sum, cross, picked)):
        packed = jnp.where(lane == at, jnp.broadcast_to(value, (SEQS, 128)), packed)
    ssend[...] = packed

    to_heads(7, lambda j: ssend, srecv)
    srecv[h] = ssend[...]

    along_y().wait_recv()
    for dz in range(2):
        for dx in range(4):
            if (dx, dz) != (0, 0):
                block = shard_of("b", ((((x + dx) % 4) * 2 + (zl + dz) % 2) * 2 + c))
                on_chip(block, "b", d2_r.at[ARRAYS.index("b")])
    arrived("OH", 1, 1)
    ici("OH", 1, 1, "-")
    arrived("OL", 0, 1)
    arrived("X", 2, 1)
    arrived("OH", 3, 1)

    received(7, srecv)
    every = srecv[...]
    m_all, s_all, rm_all, rs_all, x_all, p_all = (every[:, :, at : at + 1] for at in range(6))
    roll_top = jnp.max(m_all, axis=0)
    roll_total = jnp.sum(s_all * jnp.exp(m_all - roll_top[None]), axis=0)
    ref_top = jnp.max(rm_all, axis=0)
    ref_scale = jnp.exp(rm_all - ref_top[None])
    ref_total = jnp.sum(rs_all * ref_scale, axis=0)
    cross_total = jnp.sum(x_all * ref_scale, axis=0)
    lse_roll = roll_top + jnp.log(roll_total)
    lse_ref = ref_top + jnp.log(ref_total)
    divergence = cross_total / ref_total - lse_ref + lse_roll
    logprob = jnp.sum(p_all, axis=0) - lse_roll
    div_out[...] = as_row(divergence)[:, 0:SEQS]
    logprob_out[...] = as_row(logprob)[:, 0:SEQS]

    for piece in PIECES:
        for dz in range(2):
            for dx in range(4):
                if (dx, dz) != (0, 0) and (piece, dx, dz) not in waited:
                    arrived(piece, dx, dz)
    for at, name in enumerate(ARRAYS):
        pltpu.make_async_remote_copy(
            src_ref=bg.at[pl.ds(0, 280)] if name == "b" else several(name, 7), dst_ref=several(name, 7),
            send_sem=ag_s.at[at], recv_sem=d2_r.at[at], device_id=sibling, device_id_type=MESH,
        ).wait()
    dt_out[...] = jnp.concatenate([dts[device].astype(F32) for device in range(2 * CHIPS)], axis=1).astype(BF16)
    for at, name in enumerate(ARRAYS):
        pltpu.make_async_remote_copy(
            src_ref=several(name, 8), dst_ref=several(name, 8), send_sem=d2_s.at[at], recv_sem=d2_r.at[at],
            device_id=sibling, device_id_type=MESH,
        ).wait_send()
    lm_copy.wait_send()
    along_y().wait_send()
    for copy in pending:
        copy.wait_send()


def write_out(*refs):
    count = len(refs) // 2
    copies = [pltpu.make_async_copy(refs[at], refs[count + at], refs[-1].at[at]) for at in range(count)]
    for copy in copies:
        copy.start()
    for copy in copies:
        copy.wait()


ANY = pl.BlockSpec(memory_space=pl.ANY)
VMEM = pl.BlockSpec(memory_space=pltpu.VMEM)


def shards(
    hidden_in, ssm_state, conv_x_state, conv_bc_state, token_ids, ref_logits, in_z, in_x, in_bc, in_dt, out_t,
    lm_head, conv_wx, conv_bx, conv_wbc, conv_bbc, dt_bias, a_log, skip_gain, norm_in, norm_gain, final_gain,
):
    row = lambda v: v.reshape(1, -1)
    results = (
        ((SEQS, DI, N), F32), ((1, SEQS), F32), ((1, SEQS), F32), ((D, DI), BF16), ((D, DI), BF16), ((D, 256), BF16),
        ((HEADS, D), BF16), ((D, DI), BF16),
    )
    held = pl.pallas_call(
        kernel,
        out_shape=tuple(pltpu.VMEM(shape, dtype) for shape, dtype in results),
        in_specs=[pl.BlockSpec(memory_space=pltpu.HBM)] * 22,
        out_specs=(VMEM,) * len(results),
        scratch_shapes=[
            pltpu.VMEM((2 * CHIPS, HEADS, SHARD), BF16),
            pltpu.VMEM((SLICE, VL), BF16),
            pltpu.VMEM((SEQS, VL), BF16),
            pltpu.VMEM((CHIPS, SEQS, SLICE), BF16),
            pltpu.VMEM((CHIPS, SEQS, SLICE), BF16),
            pltpu.VMEM((2, CHIPS, 1, SLICE), F32),
            pltpu.VMEM((CHIPS, SEQS, 1664), BF16),
            pltpu.VMEM((CHIPS, SEQS, 1664), BF16),
            pltpu.VMEM((SEQS, 768), BF16),
            pltpu.VMEM((CHIPS, SEQS, 768), BF16),
            pltpu.VMEM((CHIPS, SEQS, 384), BF16),
            pltpu.VMEM((CHIPS, SEQS, 384), BF16),
            pltpu.VMEM((SEQS, 384), BF16),
            pltpu.VMEM((CHIPS, SEQS, 384), BF16),
            pltpu.VMEM((CHIPS, SEQS, VL + 128), BF16),
            pltpu.VMEM((CHIPS, SEQS, VL + 128), BF16),
            pltpu.VMEM((SEQS, 128), F32),
            pltpu.VMEM((CHIPS, SEQS, 128), F32),
            pltpu.VMEM((SEQS, 128), F32),
            pltpu.VMEM((SEQS, N), F32),
            pltpu.VMEM((DI, 128), F32),
            pltpu.VMEM((2 * SEQS, N), BF16),
            pltpu.VMEM((SEQS, DI), F32),
            pltpu.VMEM((SEQS, D), BF16),
            pltpu.VMEM((3, SEQS, DI), BF16),
            pltpu.VMEM((3, SEQS, 256), BF16),
            pltpu.VMEM((1, SEQS), jnp.int32),
            pltpu.VMEM((4, DI), F32),
            pltpu.VMEM((4, 256), F32),
            pltpu.VMEM((1, 256), F32),
            pltpu.VMEM((1, HEADS), F32),
            pltpu.VMEM((1, HEADS), F32),
            pltpu.VMEM((1, HEADS), F32),
            pltpu.VMEM((2, D), F32),
            pltpu.VMEM((2, DI), F32),
            pltpu.SemaphoreType.DMA((15,)),
            pltpu.SemaphoreType.DMA((9,)),
            pltpu.SemaphoreType.DMA((9,)),
            pltpu.SemaphoreType.DMA((9,)),
            pltpu.SemaphoreType.DMA((5,)),
            pltpu.SemaphoreType.DMA((6, 7)),
            pltpu.SemaphoreType.DMA((5,)),
            pltpu.SemaphoreType.DMA((5,)),
            pltpu.SemaphoreType.DMA((5,)),
            pltpu.SemaphoreType.DMA((2,)),
        ],
        compiler_params=pltpu.CompilerParams(
            collective_id=0, has_side_effects=True, vmem_limit_bytes=32 * 1024 * 1024
        ),
    )(*[pltpu.with_memory_space_constraint(array, pltpu.HBM) for array in (
        hidden_in, ssm_state.reshape(SEQS, DI, N), conv_x_state.transpose(1, 0, 2), conv_bc_state.transpose(1, 0, 2),
        row(token_ids), ref_logits, in_z, in_x, in_bc, in_dt.T, out_t, lm_head.T,
        conv_wx, conv_bx, conv_wbc, row(conv_bbc), row(dt_bias), row(a_log), row(skip_gain), norm_in,
        norm_gain, final_gain,
    )])
    held = [pltpu.with_memory_space_constraint(array, pltpu.VMEM) for array in held]
    state, divergence, logprob, roll_z, roll_x, roll_bc, dt_rows, roll_out = pl.pallas_call(
        write_out,
        out_shape=tuple(jax.ShapeDtypeStruct(shape, dtype) for shape, dtype in results),
        in_specs=[VMEM] * len(results),
        out_specs=(ANY,) * len(results),
        scratch_shapes=[pltpu.SemaphoreType.DMA((len(results),))],
        compiler_params=pltpu.CompilerParams(vmem_limit_bytes=1024 * 1024),
    )(*held)
    return (
        state.reshape(ssm_state.shape), divergence.reshape(SEQS), logprob.reshape(SEQS), roll_z, roll_x, roll_bc,
        dt_rows.T, roll_out,
    )


def solution(mesh):
    spread = P("group", "head")
    return jax.shard_map(
        shards,
        mesh=mesh,
        in_specs=(
            P("group", None), P("group", "head", None, None), P("group", None, "head"), P("group", None, None),
            P("group"), spread, spread, spread, P("group", None), spread, spread, P("head", "group"),
            P(None, "head"), P("head"), P(), P(), P("head"), P("head"), P("head"), P(), P("head"), P(),
        ),
        out_specs=(
            P("group", "head", None, None), P("group"), P("group"), P(None, "head"), P(None, "head"), P(),
            P(None, "head"), P(None, "head"),
        ),
        check_vma=False,
    )
```

```python
import functools

import jax
import jax.numpy as jnp
from jax import lax
from jax.experimental import pallas as pl
from jax.experimental.pallas import tpu as pltpu
from jax.sharding import PartitionSpec as P

MESH = pl.DeviceIdType.MESH
EPSILON = 1e-05
SEQS, D, DI, HEADS, P_SIZE, N = 16, 2560, 640, 10, 64, 128
SHARD = 160
SLICE = 320
CHIPS = 8
VL = 3200
CUT = 1920
REST = VL + 128 - CUT
F32 = jnp.float32
BF16 = jnp.bfloat16

PIECES = {
    "X": ("x", 0, 160),
    "OL": ("o", 0, 32),
    "DT": ("d", 0, 160),
    "Z": ("z", 0, 160),
    "BC": ("b", 0, 160),
    "OH": ("o", 32, 128),
}
ORDER = {name: at for at, name in enumerate(PIECES)}
ARRAYS = "xobdz"


def silu(v):
    return v / (1.0 + jnp.exp(-v))


def per_head(values):
    rows = values.shape[0]
    lane = lax.broadcasted_iota(jnp.int32, (rows, 128), 1)
    parts = []
    for pair in range(HEADS // 2):
        left = jnp.broadcast_to(values[:, 2 * pair : 2 * pair + 1], (rows, 128))
        right = jnp.broadcast_to(values[:, 2 * pair + 1 : 2 * pair + 2], (rows, 128))
        parts.append(jnp.where(lane < P_SIZE, left, right))
    return jnp.concatenate(parts, axis=1)


def as_column(row):
    r = lax.broadcasted_iota(jnp.int32, (SEQS, SEQS), 0)
    c = lax.broadcasted_iota(jnp.int32, (SEQS, SEQS), 1)
    return jnp.sum(jnp.where(r == c, jnp.broadcast_to(row, (SEQS, SEQS)), 0.0), axis=1, keepdims=True)


def as_row(column):
    r = lax.broadcasted_iota(jnp.int32, (SEQS, 128), 0)
    c = lax.broadcasted_iota(jnp.int32, (SEQS, 128), 1)
    return jnp.sum(jnp.where(r == c, jnp.broadcast_to(column, (SEQS, 128)), 0.0), axis=0, keepdims=True)


def two_parts(values, width):
    high = values.astype(BF16).astype(F32)
    rows = values.shape[0]
    lane = lax.broadcasted_iota(jnp.int32, (rows, 2 * width), 1)
    return jnp.where(
        lane < width, jnp.broadcast_to(high, (rows, 2 * width)), jnp.broadcast_to(values - high, (rows, 2 * width))
    ).astype(BF16)


def kernel(
    hidden_in, state_in, conv_x_in, conv_bc_in, tokens_in, ref_in, in_z, in_x, in_bc, dt_in, out_t, lm_in,
    conv_wx_in, conv_bx, conv_wbc_in, conv_bbc_in, dt_bias_in, a_log_in, skip_in, norm_in, norm_gain, final_gain,
    state, div_out, logprob_out, zg, xg, bg, dt_out, og,
    dts, lm, refs, hsend, hrecv, gains, psend, precv, gsend, grecv, rsend, rrecv, usend, urecv, lsend, zrecv, zsum, total_z, xrecv, xsum, total_x,
    ssend, srecv, decays, b_rows, x_cols, c_rows, y_acc,
    hidden, conv_x, conv_bc, tokens, conv_wx, conv_wbc, conv_bbc, dt_bias, a_log, skip_gain,
    long_rows, short_rows, small, loc, chain_s, chain_r, ag_s, ag_r, d2_s, d2_own, d2_r, y_sems, sum_s, sum_r,
):
    g = lax.axis_index("group")
    h = lax.axis_index("head")
    k = g // 2
    c = g % 2
    x = k // 2
    zl = k % 2
    y = h // 2
    sibling = (2 * k + 1 - c, h)

    barrier = pltpu.get_barrier_semaphore()
    for d in range(1, 8):
        pl.semaphore_signal(barrier, inc=1, device_id=(g, (h + d) % 8), device_id_type=MESH)
        pl.semaphore_signal(barrier, inc=1, device_id=(2 * ((k + d) % 8) + c, h), device_id_type=MESH)
    pl.semaphore_signal(barrier, inc=1, device_id=sibling, device_id_type=MESH)

    rows_mine = pl.ds(pl.multiple_of(g * SHARD, SHARD), SHARD)
    lm_mine = pl.ds(pl.multiple_of(c * SHARD, SHARD), SHARD)
    lm_other = pl.ds(pl.multiple_of((1 - c) * SHARD, SHARD), SHARD)
    first = [
        pltpu.make_async_copy(source, target, small.at[at])
        for at, (source, target) in enumerate(
            [
                (hidden_in, hidden), (dt_in, dts.at[g]), (norm_in, long_rows.at[0]), (final_gain, long_rows.at[1]),
                (conv_x_in, conv_x), (conv_bc_in, conv_bc), (tokens_in, tokens), (conv_wx_in, conv_wx),
                (conv_wbc_in, conv_wbc), (conv_bbc_in, conv_bbc), (dt_bias_in, dt_bias), (a_log_in, a_log),
                (skip_in, skip_gain), (conv_bx, short_rows.at[0]), (norm_gain, short_rows.at[1]),
            ]
        )
    ]
    local = [
        pltpu.make_async_copy(source, target, loc.at[at])
        for at, (source, target) in enumerate(
            [
                (in_x, xg.at[rows_mine]), (in_bc, bg.at[rows_mine]), (in_z, zg.at[rows_mine]),
                (out_t, og.at[rows_mine]), (lm_in, lm.at[lm_mine]), (state_in, state), (ref_in, refs),
            ]
        )
    ]
    for copy in first + local:
        copy.start()
    first[0].wait()

    for j in range(CHIPS):
        hsend[j] = hidden[:, SLICE * j : SLICE * (j + 1)]

    pl.semaphore_wait(barrier, 15)

    def chain_copy(phase, src, dst, device):
        return pltpu.make_async_remote_copy(
            src_ref=src, dst_ref=dst, send_sem=chain_s.at[phase], recv_sem=chain_r.at[phase],
            device_id=device, device_id_type=MESH,
        )

    pending = []

    def to_chips(phase, send_slot, recv):
        for d in range(1, 8):
            j = (k + d) % 8
            chain_copy(phase, send_slot(j), recv.at[k], (2 * j + c, h)).start()
        pending.append(chain_copy(phase, recv.at[pl.ds(0, 7)], recv.at[pl.ds(0, 7)], sibling))

    def to_heads(phase, send_slot, recv):
        for d in range(1, 8):
            j = (h + d) % 8
            chain_copy(phase, send_slot(j), recv.at[h], (g, j)).start()
        pending.append(chain_copy(phase, recv.at[pl.ds(0, 7)], recv.at[pl.ds(0, 7)], sibling))

    def received(phase, recv):
        chain_copy(phase, recv.at[pl.ds(0, 7)], recv.at[pl.ds(0, 7)], sibling).wait_recv()

    buffers = {"x": xg, "z": zg, "o": og, "b": bg, "d": dts}

    def quarter(device):
        at = pl.multiple_of(device * SHARD + 80 * (y // 2), 16)
        return bg.at[pl.ds(at, 80), pl.ds(pl.multiple_of(128 * (y % 2), 128), 128)]

    def region(piece, dx, dz, core):
        name, begin, rows = PIECES[piece]
        at = (((x + dx) % 4) * 2 + (zl + dz) % 2) * 2 + core
        if name == "d":
            return dts.at[at]
        if name == "b":
            return quarter(at)
        at = at * SHARD + begin
        return buffers[name].at[pl.ds(pl.multiple_of(at, 16), rows)]

    def ici(piece, dx, dz, ways):
        for way in ways:
            move = {"+": 1, "-": 3, "z": 0}[way]
            rx, rz = (dx - move) % 4, (dz + (way == "z")) % 2
            chip = ((x + move) % 4) * 2 + (zl + (way == "z")) % 2
            block = region(piece, dx, dz, c)
            pltpu.make_async_remote_copy(
                src_ref=block, dst_ref=block, send_sem=ag_s.at[ARRAYS.index(PIECES[piece][0])],
                recv_sem=ag_r.at[ORDER[piece], 4 * rz + rx - 1], device_id=(2 * chip + c, h), device_id_type=MESH,
            ).start()

    def on_chip(block, name, sem):
        pltpu.make_async_remote_copy(
            src_ref=block, dst_ref=block, send_sem=d2_s.at[ARRAYS.index(name)], recv_sem=sem,
            device_id=sibling, device_id_type=MESH,
        ).start()

    def shard_of(name, device):
        if name == "d":
            return dts.at[device]
        return buffers[name].at[pl.ds(pl.multiple_of(device * SHARD, SHARD), SHARD)]

    def along_y():
        return pltpu.make_async_remote_copy(
            src_ref=bg.at[pl.ds(0, 840)], dst_ref=bg.at[pl.ds(0, 840)], send_sem=y_sems.at[0], recv_sem=y_sems.at[1],
            device_id=sibling, device_id_type=MESH,
        )

    def several(name, shards):
        return buffers[name].at[pl.ds(0, shards if name == "d" else shards * SHARD)]

    def share_own(name):
        on_chip(shard_of(name, g), name, d2_own.at[ARRAYS.index(name)])

    def sibling_own(name):
        rows = shard_of(name, 2 * k + 1 - c)
        pltpu.make_async_remote_copy(
            src_ref=rows, dst_ref=rows, send_sem=d2_s.at[ARRAYS.index(name)], recv_sem=d2_own.at[ARRAYS.index(name)],
            device_id=sibling, device_id_type=MESH,
        ).wait_recv()

    waited = set()

    def arrived(piece, dx, dz):
        block = region(piece, dx, dz, c)
        name = PIECES[piece][0]
        pltpu.make_async_remote_copy(
            src_ref=block, dst_ref=block, send_sem=d2_s.at[ARRAYS.index(name)],
            recv_sem=ag_r.at[ORDER[piece], 4 * dz + dx - 1], device_id=sibling, device_id_type=MESH,
        ).wait_recv()
        waited.add((piece, dx, dz))
        if name == "b":
            for move in range(1, 4):
                pltpu.make_async_remote_copy(
                    src_ref=block, dst_ref=block, send_sem=y_sems.at[0], recv_sem=y_sems.at[1],
                    device_id=(g, (h + 2 * move) % 8), device_id_type=MESH,
                ).start()
            return
        on_chip(block, name, d2_r.at[ARRAYS.index(name)])

    to_chips(0, lambda j: hsend.at[j], hrecv)
    local[0].wait()
    share_own("x")
    local[1].wait()
    share_own("b")
    local[2].wait()
    share_own("z")
    first[1].wait()
    share_own("d")
    ici("X", 0, 0, "+-")
    ici("Z", 0, 0, "z")
    hrecv[k] = hsend[k]
    for copy in first[2:]:
        copy.wait()
    for j in range(CHIPS):
        gains[0, j] = long_rows[0:1, SLICE * j : SLICE * (j + 1)]
        gains[1, j] = long_rows[1:2, SLICE * j : SLICE * (j + 1)]
    whole = hidden[...].astype(F32)
    scale_in = lax.rsqrt(jnp.mean(whole * whole, axis=-1, keepdims=True) + EPSILON)
    local[3].wait()
    local[4].wait()

    received(0, hrecv)
    gain = gains[0, k]
    lhs = (hrecv[...].astype(F32) * gain[None]).astype(BF16).reshape(CHIPS * SEQS, SLICE)
    slice_rows = pl.ds(pl.multiple_of(k * SLICE, SLICE), SLICE)

    def turned(device):
        rows = jnp.concatenate([dts[device].astype(F32), jnp.zeros((128 - HEADS, SHARD), F32)], axis=0)
        return jnp.transpose(rows).astype(BF16)

    def partial(weights, at, width):
        product = jnp.dot(lhs, weights, preferred_element_type=F32)
        psend[:, :, at : at + width] = product.astype(BF16).reshape(CHIPS, SEQS, width)

    sibling_own("x")
    partial(xg[slice_rows, :], 0, 640)
    sibling_own("b")
    partial(bg[slice_rows, :], 640, 256)
    sibling_own("d")
    partial(jnp.concatenate([turned(2 * k), turned(2 * k + 1)], axis=0), 896, 128)
    to_chips(1, lambda j: psend.at[j, :, pl.ds(0, 1024)], precv.at[:, :, pl.ds(0, 1024)])
    sibling_own("z")
    partial(zg[slice_rows, :], 1024, 640)
    to_chips(2, lambda j: psend.at[j, :, pl.ds(1024, 640)], precv.at[:, :, pl.ds(1024, 640)])
    precv[k] = psend[k]
    arrived("Z", 0, 1)
    ici("Z", 0, 0, "+-")
    ici("OL", 0, 0, "+-")
    ici("X", 0, 0, "z")
    ici("BC", 0, 0, "z")
    ici("DT", 0, 0, "z")
    share_own("o")
    lm_copy = pltpu.make_async_remote_copy(
        src_ref=lm.at[lm_mine], dst_ref=lm.at[lm_mine], send_sem=loc.at[7], recv_sem=loc.at[8],
        device_id=sibling, device_id_type=MESH,
    )
    lm_copy.start()

    received(1, precv.at[:, :, pl.ds(0, 1024)])
    summed = jnp.sum(precv[:, :, 0:1024].astype(F32), axis=0) * scale_in
    x_new = summed[:, 0:640]
    bc_new = summed[:, 640:896]
    step_raw = summed[:, 896 : 896 + HEADS]
    acc = x_new * conv_wx[3:4, :] + short_rows[0:1, :]
    acc_bc = bc_new * conv_wbc[3:4, :] + conv_bbc[...]
    for tap in range(3):
        acc = acc + conv_x[tap].astype(F32) * conv_wx[tap : tap + 1, :]
        acc_bc = acc_bc + conv_bc[tap].astype(F32) * conv_wbc[tap : tap + 1, :]
    x_conv = silu(acc)
    bc_conv = silu(acc_bc)
    b_rows[...] = bc_conv[:, :N]
    c_vals = bc_conv[:, N:]
    biased = step_raw + dt_bias[...]
    step = jnp.maximum(biased, 0.0) + jnp.log1p(jnp.exp(-jnp.abs(biased)))
    decay = jnp.exp(-step * jnp.exp(a_log[...]))
    square = jnp.concatenate(
        [jnp.concatenate([decay, jnp.zeros((SEQS, 128 - HEADS), F32)], axis=1), jnp.zeros((112, 128), F32)], axis=0
    )
    decays[...] = jnp.transpose(square)[0:SEQS]
    inflow = per_head(step) * x_conv
    x_cols[...] = jnp.transpose(jnp.concatenate([inflow, jnp.zeros((112, DI), F32)], axis=0))
    c_high = c_vals.astype(BF16)
    c_low = (c_vals - c_high.astype(F32)).astype(BF16)
    c_rows[...] = jnp.concatenate([c_high, c_low], axis=0)
    local[5].wait()

    def two_heads(pair, _):
        rows = pl.ds(pl.multiple_of(pair * 128, 128), 128)
        columns = x_cols[rows, :]
        left = decays[pl.ds(2 * pair, 1), :]
        right = decays[pl.ds(2 * pair + 1, 1), :]
        both = c_rows[...]
        row = lax.broadcasted_iota(jnp.int32, (SEQS, N), 0)
        total = jnp.zeros((SEQS, N), F32)
        for s in range(SEQS):
            factor = jnp.concatenate(
                [
                    jnp.broadcast_to(left[:, s : s + 1], (P_SIZE, N)),
                    jnp.broadcast_to(right[:, s : s + 1], (P_SIZE, N)),
                ],
                axis=0,
            )
            column = jnp.broadcast_to(columns[:, s : s + 1], (2 * P_SIZE, N))
            new = state[s, rows, :] * factor + column * b_rows[s : s + 1, :]
            state[s, rows, :] = new
            seen = lax.dot_general(both, new.astype(BF16), (((1,), (1,)), ((), ())), preferred_element_type=F32)
            total = total + jnp.where(row == s, seen[0:SEQS] + seen[SEQS:], 0.0)
        y_acc[:, rows] = total
        return 0

    lax.fori_loop(0, HEADS // 2, two_heads, 0)
    received(2, precv.at[:, :, pl.ds(1024, 640)])
    gate = jnp.sum(precv[:, :, 1024:1664].astype(F32), axis=0) * scale_in
    ssm_out = y_acc[...] + per_head(skip_gain[...]) * x_conv
    gated = ssm_out * silu(gate)
    squares = jnp.sum(gated * gated, axis=-1, keepdims=True)
    gsend[:, 0:640] = (gated * short_rows[1:2, :]).astype(BF16)
    gsend[:, 640:768] = two_parts(squares, 64)

    to_chips(3, lambda j: gsend, grecv)
    grecv[k] = gsend[...]
    arrived("X", 3, 0)
    ici("X", 3, 0, "z+")
    ici("DT", 0, 0, "+-")
    ici("BC", 0, 0, "+-")
    ici("Z", 0, 1, "+-")
    ici("OH", 0, 0, "z")
    arrived("X", 1, 0)

    sibling_own("o")
    received(3, grecv)
    mixed = lax.dot_general(
        grecv[:, :, 0:640].reshape(CHIPS * SEQS, 640), og[slice_rows, :], (((1,), (1,)), ((), ())),
        preferred_element_type=F32,
    )
    parts = grecv[:, :, 640:768].astype(F32)
    sq = (parts[:, :, 0:1] + parts[:, :, 64:65]).reshape(CHIPS * SEQS, 1)
    rsend[:, :, 0:SLICE] = mixed.astype(BF16).reshape(CHIPS, SEQS, SLICE)
    rsend[:, :, SLICE:384] = two_parts(sq, 32).reshape(CHIPS, SEQS, 64)
    to_heads(4, lambda j: rsend.at[j], rrecv)
    rrecv[h] = rsend[h]
    arrived("DT", 0, 1)
    ici("DT", 0, 1, "+-")
    arrived("BC", 0, 1)
    ici("BC", 0, 1, "+-")
    ici("OH", 0, 0, "+-")
    ici("X", 1, 0, "z")
    arrived("Z", 3, 0)
    ici("Z", 3, 0, "+")
    arrived("Z", 1, 0)
    arrived("Z", 1, 1)
    ici("Z", 1, 1, "-")
    received(4, rrecv)
    total = jnp.sum(rrecv[...].astype(F32), axis=0)
    scale_gate = lax.rsqrt((total[:, SLICE : SLICE + 1] + total[:, SLICE + 32 : SLICE + 33]) / (8.0 * DI) + EPSILON)
    stream = hrecv[h].astype(F32) + total[:, 0:SLICE] * scale_gate
    usend[:, 0:SLICE] = (stream * gains[1, k]).astype(BF16)
    usend[:, SLICE:384] = two_parts(jnp.sum(stream * stream, axis=-1, keepdims=True), 32)

    to_heads(5, lambda j: usend, urecv)
    urecv[h] = usend[...]
    arrived("DT", 1, 0)
    ici("DT", 1, 0, "-")
    arrived("DT", 1, 1)
    ici("DT", 1, 1, "-")
    arrived("BC", 3, 0)
    ici("BC", 3, 0, "+")
    arrived("BC", 1, 1)
    ici("BC", 1, 1, "-")
    arrived("OL", 1, 0)
    ici("OL", 1, 0, "-")
    ici("OL", 0, 0, "z")
    arrived("OL", 3, 0)
    arrived("X", 0, 1)
    arrived("X", 3, 1)
    arrived("BC", 1, 0)
    arrived("BC", 3, 1)
    arrived("DT", 3, 0)
    arrived("DT", 3, 1)

    local[6].wait()
    pltpu.make_async_remote_copy(
        src_ref=lm.at[lm_other], dst_ref=lm.at[lm_other], send_sem=loc.at[7], recv_sem=loc.at[8],
        device_id=sibling, device_id_type=MESH,
    ).wait_recv()
    received(5, urecv)
    final = urecv[:, :, 0:SLICE].reshape(CHIPS * SEQS, SLICE)

    def some_logits(at, width):
        product = jnp.dot(final, lm[:, at : at + width], preferred_element_type=F32)
        product = product.astype(BF16).reshape(4, 2, SEQS, width)
        for z in range(2):
            lsend[z, :, :, at : at + width] = product[:, z]

    def sum_copy(at, src, dst, device):
        return pltpu.make_async_remote_copy(
            src_ref=src, dst_ref=dst, send_sem=sum_s.at[at], recv_sem=sum_r.at[at], device_id=device,
            device_id_type=MESH,
        )

    partner = (2 * (2 * x + 1 - zl) + c, h)
    across = []
    for part in range(3):
        columns = pl.ds(640 * part, 640)
        some_logits(640 * part, 640)
        copy = sum_copy(part, lsend.at[1 - zl, :, :, columns], zrecv.at[:, :, columns], partner)
        copy.start()
        across.append(copy)
        if part == 0:
            for at in range(CUT, VL, 640):
                some_logits(at, 640)
            for z in range(2):
                for position in range(4):
                    lsend[z, position, :, VL : VL + 64] = urecv[2 * position + z, :, SLICE:384]
                    lsend[z, position, :, VL + 64 : VL + 128] = urecv[2 * position + z, :, SLICE:384]
            for move in (1, 3, 2):
                other = (x + move) % 4
                sum_copy(3, lsend.at[:, other, :, pl.ds(CUT, REST)], xrecv.at[x], (2 * (2 * other + zl) + c, h)).start()

    reference = refs[...].astype(F32)
    ref_max = jnp.max(reference, axis=-1, keepdims=True)
    weight = jnp.exp(reference - ref_max)
    ref_sum = jnp.sum(weight, axis=-1, keepdims=True)
    token = as_column(tokens[...].astype(F32)).astype(jnp.int32)


    def pair_sums(part):
        columns = slice(640 * part, 640 * part + 640)
        across[part].wait_recv()
        summed = lsend[zl, :, :, columns].astype(F32) + zrecv[:, :, columns].astype(F32)
        zsum[:, :, columns] = summed.astype(BF16)
        for move in (2, 1, 3):
            other = (x + move) % 4
            sum_copy(
                4 + part, zsum.at[other, :, pl.ds(640 * part, 640)], total_z.at[x, :, pl.ds(640 * part, 640)],
                (2 * (2 * other + zl) + c, h),
            ).start()
        total_z[x, :, columns] = zsum[x, :, columns]

    pair_sums(0)
    pair_sums(1)
    three = xrecv.at[pl.ds(0, 3)]
    xrecv[x] = lsend[:, x, :, CUT : CUT + REST]
    sum_copy(3, three, three, partner).wait_recv()
    xsum[...] = jnp.sum(xrecv[:, 1 - zl].astype(F32), axis=0).astype(BF16)
    along_z = sum_copy(7, xsum, total_x, partner)
    along_z.start()
    mine = jnp.sum(xrecv[:, zl].astype(F32), axis=0)
    pair_sums(2)

    arrived("OH", 0, 1)
    ici("OH", 0, 1, "+-")
    arrived("X", 2, 0)
    ici("X", 2, 0, "z")
    ici("OL", 1, 0, "z")
    ici("OL", 3, 0, "z")
    arrived("OH", 3, 0)
    ici("OH", 3, 0, "+")
    arrived("OL", 2, 0)
    ici("OL", 2, 0, "z")
    arrived("BC", 2, 0)
    arrived("BC", 2, 1)
    arrived("X", 1, 1)
    arrived("Z", 3, 1)
    arrived("OH", 1, 0)
    arrived("DT", 2, 0)
    arrived("DT", 2, 1)
    arrived("Z", 2, 0)
    arrived("Z", 2, 1)


    for part in range(3):
        block = total_z.at[pl.ds(0, 3), :, pl.ds(640 * part, 640)]
        sum_copy(4 + part, block, block, partner).wait_recv()
    along_z.wait_recv()
    rest = mine + total_x[...].astype(F32)
    logits = jnp.concatenate([jnp.sum(total_z[...].astype(F32), axis=0), rest[:, 0 : VL - CUT]], axis=1)
    tail = rest[:, VL - CUT :]
    logits = logits * lax.rsqrt((tail[:, 0:1] + tail[:, 32:33]) / D + EPSILON)
    roll_max = jnp.max(logits, axis=-1, keepdims=True)
    roll_sum = jnp.sum(jnp.exp(logits - roll_max), axis=-1, keepdims=True)
    cross = jnp.sum(weight * (reference - logits), axis=-1, keepdims=True)
    column = lax.broadcasted_iota(jnp.int32, (SEQS, VL), 1) + h * VL
    picked = jnp.sum(jnp.where(column == token, logits, 0.0), axis=-1, keepdims=True)
    lane = lax.broadcasted_iota(jnp.int32, (SEQS, 128), 1)
    packed = jnp.zeros((SEQS, 128), F32)
    for at, value in enumerate((roll_max, roll_sum, ref_max, ref_sum, cross, picked)):
        packed = jnp.where(lane == at, jnp.broadcast_to(value, (SEQS, 128)), packed)
    ssend[...] = packed

    to_heads(7, lambda j: ssend, srecv)
    srecv[h] = ssend[...]

    along_y().wait_recv()
    for dz in range(2):
        for dx in range(4):
            if (dx, dz) != (0, 0):
                block = shard_of("b", ((((x + dx) % 4) * 2 + (zl + dz) % 2) * 2 + c))
                on_chip(block, "b", d2_r.at[ARRAYS.index("b")])
    arrived("OH", 1, 1)
    ici("OH", 1, 1, "-")
    arrived("OL", 0, 1)
    arrived("X", 2, 1)
    arrived("OH", 3, 1)

    received(7, srecv)
    every = srecv[...]
    m_all, s_all, rm_all, rs_all, x_all, p_all = (every[:, :, at : at + 1] for at in range(6))
    roll_top = jnp.max(m_all, axis=0)
    roll_total = jnp.sum(s_all * jnp.exp(m_all - roll_top[None]), axis=0)
    ref_top = jnp.max(rm_all, axis=0)
    ref_scale = jnp.exp(rm_all - ref_top[None])
    ref_total = jnp.sum(rs_all * ref_scale, axis=0)
    cross_total = jnp.sum(x_all * ref_scale, axis=0)
    lse_roll = roll_top + jnp.log(roll_total)
    lse_ref = ref_top + jnp.log(ref_total)
    divergence = cross_total / ref_total - lse_ref + lse_roll
    logprob = jnp.sum(p_all, axis=0) - lse_roll
    div_out[...] = as_row(divergence)[:, 0:SEQS]
    logprob_out[...] = as_row(logprob)[:, 0:SEQS]

    for piece in PIECES:
        for dz in range(2):
            for dx in range(4):
                if (dx, dz) != (0, 0) and (piece, dx, dz) not in waited:
                    arrived(piece, dx, dz)
    for at, name in enumerate(ARRAYS):
        pltpu.make_async_remote_copy(
            src_ref=bg.at[pl.ds(0, 280)] if name == "b" else several(name, 7), dst_ref=several(name, 7),
            send_sem=ag_s.at[at], recv_sem=d2_r.at[at], device_id=sibling, device_id_type=MESH,
        ).wait()
    dt_out[...] = jnp.concatenate([dts[device].astype(F32) for device in range(2 * CHIPS)], axis=1).astype(BF16)
    for at, name in enumerate(ARRAYS):
        pltpu.make_async_remote_copy(
            src_ref=several(name, 8), dst_ref=several(name, 8), send_sem=d2_s.at[at], recv_sem=d2_r.at[at],
            device_id=sibling, device_id_type=MESH,
        ).wait_send()
    lm_copy.wait_send()
    for copy in across:
        copy.wait_send()
    along_z.wait_send()
    sum_copy(3, three, three, partner).wait_send()
    for part in range(3):
        block = total_z.at[pl.ds(0, 3), :, pl.ds(640 * part, 640)]
        sum_copy(4 + part, block, block, partner).wait_send()
    along_y().wait_send()
    for copy in pending:
        copy.wait_send()


def write_out(*refs):
    count = len(refs) // 2
    copies = [pltpu.make_async_copy(refs[at], refs[count + at], refs[-1].at[at]) for at in range(count)]
    for copy in copies:
        copy.start()
    for copy in copies:
        copy.wait()


ANY = pl.BlockSpec(memory_space=pl.ANY)
VMEM = pl.BlockSpec(memory_space=pltpu.VMEM)


def shards(
    hidden_in, ssm_state, conv_x_state, conv_bc_state, token_ids, ref_logits, in_z, in_x, in_bc, in_dt, out_t,
    lm_head, conv_wx, conv_bx, conv_wbc, conv_bbc, dt_bias, a_log, skip_gain, norm_in, norm_gain, final_gain,
):
    row = lambda v: v.reshape(1, -1)
    results = (
        ((SEQS, DI, N), F32), ((1, SEQS), F32), ((1, SEQS), F32), ((D, DI), BF16), ((D, DI), BF16), ((D, 256), BF16),
        ((HEADS, D), BF16), ((D, DI), BF16),
    )
    held = pl.pallas_call(
        kernel,
        out_shape=tuple(pltpu.VMEM(shape, dtype) for shape, dtype in results),
        in_specs=[pl.BlockSpec(memory_space=pltpu.HBM)] * 22,
        out_specs=(VMEM,) * len(results),
        scratch_shapes=[
            pltpu.VMEM((2 * CHIPS, HEADS, SHARD), BF16),
            pltpu.VMEM((SLICE, VL), BF16),
            pltpu.VMEM((SEQS, VL), BF16),
            pltpu.VMEM((CHIPS, SEQS, SLICE), BF16),
            pltpu.VMEM((CHIPS, SEQS, SLICE), BF16),
            pltpu.VMEM((2, CHIPS, 1, SLICE), F32),
            pltpu.VMEM((CHIPS, SEQS, 1664), BF16),
            pltpu.VMEM((CHIPS, SEQS, 1664), BF16),
            pltpu.VMEM((SEQS, 768), BF16),
            pltpu.VMEM((CHIPS, SEQS, 768), BF16),
            pltpu.VMEM((CHIPS, SEQS, 384), BF16),
            pltpu.VMEM((CHIPS, SEQS, 384), BF16),
            pltpu.VMEM((SEQS, 384), BF16),
            pltpu.VMEM((CHIPS, SEQS, 384), BF16),
            pltpu.VMEM((2, 4, SEQS, VL + 128), BF16),
            pltpu.VMEM((4, SEQS, CUT), BF16),
            pltpu.VMEM((4, SEQS, CUT), BF16),
            pltpu.VMEM((4, SEQS, CUT), BF16),
            pltpu.VMEM((4, 2, SEQS, REST), BF16),
            pltpu.VMEM((SEQS, REST), BF16),
            pltpu.VMEM((SEQS, REST), BF16),
            pltpu.VMEM((SEQS, 128), F32),
            pltpu.VMEM((CHIPS, SEQS, 128), F32),
            pltpu.VMEM((SEQS, 128), F32),
            pltpu.VMEM((SEQS, N), F32),
            pltpu.VMEM((DI, 128), F32),
            pltpu.VMEM((2 * SEQS, N), BF16),
            pltpu.VMEM((SEQS, DI), F32),
            pltpu.VMEM((SEQS, D), BF16),
            pltpu.VMEM((3, SEQS, DI), BF16),
            pltpu.VMEM((3, SEQS, 256), BF16),
            pltpu.VMEM((1, SEQS), jnp.int32),
            pltpu.VMEM((4, DI), F32),
            pltpu.VMEM((4, 256), F32),
            pltpu.VMEM((1, 256), F32),
            pltpu.VMEM((1, HEADS), F32),
            pltpu.VMEM((1, HEADS), F32),
            pltpu.VMEM((1, HEADS), F32),
            pltpu.VMEM((2, D), F32),
            pltpu.VMEM((2, DI), F32),
            pltpu.SemaphoreType.DMA((15,)),
            pltpu.SemaphoreType.DMA((9,)),
            pltpu.SemaphoreType.DMA((9,)),
            pltpu.SemaphoreType.DMA((9,)),
            pltpu.SemaphoreType.DMA((5,)),
            pltpu.SemaphoreType.DMA((6, 7)),
            pltpu.SemaphoreType.DMA((5,)),
            pltpu.SemaphoreType.DMA((5,)),
            pltpu.SemaphoreType.DMA((5,)),
            pltpu.SemaphoreType.DMA((2,)),
            pltpu.SemaphoreType.DMA((8,)),
            pltpu.SemaphoreType.DMA((8,)),
        ],
        compiler_params=pltpu.CompilerParams(
            collective_id=0, has_side_effects=True, vmem_limit_bytes=32 * 1024 * 1024
        ),
    )(*[pltpu.with_memory_space_constraint(array, pltpu.HBM) for array in (
        hidden_in, ssm_state.reshape(SEQS, DI, N), conv_x_state.transpose(1, 0, 2), conv_bc_state.transpose(1, 0, 2),
        row(token_ids), ref_logits, in_z, in_x, in_bc, in_dt.T, out_t, lm_head.T,
        conv_wx, conv_bx, conv_wbc, row(conv_bbc), row(dt_bias), row(a_log), row(skip_gain), norm_in,
        norm_gain, final_gain,
    )])
    held = [pltpu.with_memory_space_constraint(array, pltpu.VMEM) for array in held]
    state, divergence, logprob, roll_z, roll_x, roll_bc, dt_rows, roll_out = pl.pallas_call(
        write_out,
        out_shape=tuple(jax.ShapeDtypeStruct(shape, dtype) for shape, dtype in results),
        in_specs=[VMEM] * len(results),
        out_specs=(ANY,) * len(results),
        scratch_shapes=[pltpu.SemaphoreType.DMA((len(results),))],
        compiler_params=pltpu.CompilerParams(vmem_limit_bytes=1024 * 1024),
    )(*held)
    return (
        state.reshape(ssm_state.shape), divergence.reshape(SEQS), logprob.reshape(SEQS), roll_z, roll_x, roll_bc,
        dt_rows.T, roll_out,
    )


def solution(mesh):
    spread = P("group", "head")
    return jax.shard_map(
        shards,
        mesh=mesh,
        in_specs=(
            P("group", None), P("group", "head", None, None), P("group", None, "head"), P("group", None, None),
            P("group"), spread, spread, spread, P("group", None), spread, spread, P("head", "group"),
            P(None, "head"), P("head"), P(), P(), P("head"), P("head"), P("head"), P(), P("head"), P(),
        ),
        out_specs=(
            P("group", "head", None, None), P("group"), P("group"), P(None, "head"), P(None, "head"), P(),
            P(None, "head"), P(None, "head"),
        ),
        check_vma=False,
    )
```

```python
import functools

import jax
import jax.numpy as jnp
from jax import lax
from jax.experimental import pallas as pl
from jax.experimental.pallas import tpu as pltpu
from jax.sharding import PartitionSpec as P

MESH = pl.DeviceIdType.MESH
EPSILON = 1e-05
SEQS, D, DI, HEADS, P_SIZE, N = 16, 2560, 640, 10, 64, 128
SHARD = 160
SLICE = 320
CHIPS = 8
VL = 3200
CUT = 1920
REST = VL + 128 - CUT
F32 = jnp.float32
BF16 = jnp.bfloat16

PIECES = {
    "X": ("x", 0, 160),
    "OL": ("o", 0, 32),
    "DT": ("d", 0, 160),
    "Z": ("z", 0, 160),
    "BC": ("b", 0, 160),
    "OH": ("o", 32, 128),
}
ORDER = {name: at for at, name in enumerate(PIECES)}
ARRAYS = "xobdz"


def silu(v):
    return v / (1.0 + jnp.exp(-v))


def per_head(values):
    rows = values.shape[0]
    lane = lax.broadcasted_iota(jnp.int32, (rows, 128), 1)
    parts = []
    for pair in range(HEADS // 2):
        left = jnp.broadcast_to(values[:, 2 * pair : 2 * pair + 1], (rows, 128))
        right = jnp.broadcast_to(values[:, 2 * pair + 1 : 2 * pair + 2], (rows, 128))
        parts.append(jnp.where(lane < P_SIZE, left, right))
    return jnp.concatenate(parts, axis=1)


def as_column(row):
    r = lax.broadcasted_iota(jnp.int32, (SEQS, SEQS), 0)
    c = lax.broadcasted_iota(jnp.int32, (SEQS, SEQS), 1)
    return jnp.sum(jnp.where(r == c, jnp.broadcast_to(row, (SEQS, SEQS)), 0.0), axis=1, keepdims=True)


def two_parts(values, width):
    high = values.astype(BF16).astype(F32)
    rows = values.shape[0]
    lane = lax.broadcasted_iota(jnp.int32, (rows, 2 * width), 1)
    return jnp.where(
        lane < width, jnp.broadcast_to(high, (rows, 2 * width)), jnp.broadcast_to(values - high, (rows, 2 * width))
    ).astype(BF16)


def kernel(
    hidden_in, state_in, conv_x_in, conv_bc_in, tokens_in, ref_in, in_z, in_x, in_bc, dt_in, out_t, lm_in,
    conv_wx_in, conv_bx, conv_wbc_in, conv_bbc_in, dt_bias_in, a_log_in, skip_in, norm_in, norm_gain, final_gain,
    state, div_out, logprob_out, zg, xg, bg, dt_out, og,
    dts, lm, refs, hsend, hrecv, gains, psend, precv, gsend, grecv, rsend, rrecv, usend, urecv, lsend, zrecv, zsum, total_z, xrecv, xsum, total_x,
    ssend, srecv, decays, b_rows, x_cols, c_rows, y_acc,
    hidden, conv_x, conv_bc, tokens, conv_wx, conv_wbc, conv_bbc, dt_bias, a_log, skip_gain,
    long_rows, short_rows, small, loc, chain_s, chain_r, ag_s, ag_r, d2_s, d2_own, d2_r, y_sems, sum_s, sum_r,
):
    g = lax.axis_index("group")
    h = lax.axis_index("head")
    k = g // 2
    c = g % 2
    x = k // 2
    zl = k % 2
    y = h // 2
    sibling = (2 * k + 1 - c, h)

    barrier = pltpu.get_barrier_semaphore()
    for d in range(1, 8):
        pl.semaphore_signal(barrier, inc=1, device_id=(g, (h + d) % 8), device_id_type=MESH)
        pl.semaphore_signal(barrier, inc=1, device_id=(2 * ((k + d) % 8) + c, h), device_id_type=MESH)
    pl.semaphore_signal(barrier, inc=1, device_id=sibling, device_id_type=MESH)

    rows_mine = pl.ds(pl.multiple_of(g * SHARD, SHARD), SHARD)
    lm_mine = pl.ds(pl.multiple_of(c * SHARD, SHARD), SHARD)
    lm_other = pl.ds(pl.multiple_of((1 - c) * SHARD, SHARD), SHARD)
    first = [
        pltpu.make_async_copy(source, target, small.at[at])
        for at, (source, target) in enumerate(
            [
                (hidden_in, hidden), (dt_in, dts.at[g]), (norm_in, long_rows.at[0]), (final_gain, long_rows.at[1]),
                (conv_x_in, conv_x), (conv_bc_in, conv_bc), (tokens_in, tokens), (conv_wx_in, conv_wx),
                (conv_wbc_in, conv_wbc), (conv_bbc_in, conv_bbc), (dt_bias_in, dt_bias), (a_log_in, a_log),
                (skip_in, skip_gain), (conv_bx, short_rows.at[0]), (norm_gain, short_rows.at[1]),
            ]
        )
    ]
    local = [
        pltpu.make_async_copy(source, target, loc.at[at])
        for at, (source, target) in enumerate(
            [
                (in_x, xg.at[rows_mine]), (in_bc, bg.at[rows_mine]), (in_z, zg.at[rows_mine]),
                (out_t, og.at[rows_mine]), (lm_in, lm.at[lm_mine]), (state_in, state), (ref_in, refs),
            ]
        )
    ]
    for copy in first + local:
        copy.start()
    first[0].wait()

    for j in range(CHIPS):
        hsend[j] = hidden[:, SLICE * j : SLICE * (j + 1)]

    pl.semaphore_wait(barrier, 15)

    def chain_copy(phase, src, dst, device):
        return pltpu.make_async_remote_copy(
            src_ref=src, dst_ref=dst, send_sem=chain_s.at[phase], recv_sem=chain_r.at[phase],
            device_id=device, device_id_type=MESH,
        )

    pending = []

    def to_chips(phase, send_slot, recv):
        for d in range(1, 8):
            j = (k + d) % 8
            chain_copy(phase, send_slot(j), recv.at[k], (2 * j + c, h)).start()
        pending.append(chain_copy(phase, recv.at[pl.ds(0, 7)], recv.at[pl.ds(0, 7)], sibling))

    def to_heads(phase, send_slot, recv):
        for d in range(1, 8):
            j = (h + d) % 8
            chain_copy(phase, send_slot(j), recv.at[h], (g, j)).start()
        pending.append(chain_copy(phase, recv.at[pl.ds(0, 7)], recv.at[pl.ds(0, 7)], sibling))

    def received(phase, recv):
        chain_copy(phase, recv.at[pl.ds(0, 7)], recv.at[pl.ds(0, 7)], sibling).wait_recv()

    buffers = {"x": xg, "z": zg, "o": og, "b": bg, "d": dts}

    def quarter(device):
        at = pl.multiple_of(device * SHARD + 80 * (y // 2), 16)
        return bg.at[pl.ds(at, 80), pl.ds(pl.multiple_of(128 * (y % 2), 128), 128)]

    def region(piece, dx, dz, core):
        name, begin, rows = PIECES[piece]
        at = (((x + dx) % 4) * 2 + (zl + dz) % 2) * 2 + core
        if name == "d":
            return dts.at[at]
        if name == "b":
            return quarter(at)
        at = at * SHARD + begin
        return buffers[name].at[pl.ds(pl.multiple_of(at, 16), rows)]

    def ici(piece, dx, dz, ways):
        for way in ways:
            move = {"+": 1, "-": 3, "z": 0}[way]
            rx, rz = (dx - move) % 4, (dz + (way == "z")) % 2
            chip = ((x + move) % 4) * 2 + (zl + (way == "z")) % 2
            block = region(piece, dx, dz, c)
            pltpu.make_async_remote_copy(
                src_ref=block, dst_ref=block, send_sem=ag_s.at[ARRAYS.index(PIECES[piece][0])],
                recv_sem=ag_r.at[ORDER[piece], 4 * rz + rx - 1], device_id=(2 * chip + c, h), device_id_type=MESH,
            ).start()

    def on_chip(block, name, sem):
        pltpu.make_async_remote_copy(
            src_ref=block, dst_ref=block, send_sem=d2_s.at[ARRAYS.index(name)], recv_sem=sem,
            device_id=sibling, device_id_type=MESH,
        ).start()

    def shard_of(name, device):
        if name == "d":
            return dts.at[device]
        return buffers[name].at[pl.ds(pl.multiple_of(device * SHARD, SHARD), SHARD)]

    def along_y():
        return pltpu.make_async_remote_copy(
            src_ref=bg.at[pl.ds(0, 840)], dst_ref=bg.at[pl.ds(0, 840)], send_sem=y_sems.at[0], recv_sem=y_sems.at[1],
            device_id=sibling, device_id_type=MESH,
        )

    def several(name, shards):
        return buffers[name].at[pl.ds(0, shards if name == "d" else shards * SHARD)]

    def share_own(name):
        on_chip(shard_of(name, g), name, d2_own.at[ARRAYS.index(name)])

    def sibling_own(name):
        rows = shard_of(name, 2 * k + 1 - c)
        pltpu.make_async_remote_copy(
            src_ref=rows, dst_ref=rows, send_sem=d2_s.at[ARRAYS.index(name)], recv_sem=d2_own.at[ARRAYS.index(name)],
            device_id=sibling, device_id_type=MESH,
        ).wait_recv()

    waited = set()

    def arrived(piece, dx, dz):
        block = region(piece, dx, dz, c)
        name = PIECES[piece][0]
        pltpu.make_async_remote_copy(
            src_ref=block, dst_ref=block, send_sem=d2_s.at[ARRAYS.index(name)],
            recv_sem=ag_r.at[ORDER[piece], 4 * dz + dx - 1], device_id=sibling, device_id_type=MESH,
        ).wait_recv()
        waited.add((piece, dx, dz))
        if name == "b":
            for move in range(1, 4):
                pltpu.make_async_remote_copy(
                    src_ref=block, dst_ref=block, send_sem=y_sems.at[0], recv_sem=y_sems.at[1],
                    device_id=(g, (h + 2 * move) % 8), device_id_type=MESH,
                ).start()
            return
        on_chip(block, name, d2_r.at[ARRAYS.index(name)])

    to_chips(0, lambda j: hsend.at[j], hrecv)
    local[0].wait()
    share_own("x")
    local[1].wait()
    share_own("b")
    local[2].wait()
    share_own("z")
    first[1].wait()
    share_own("d")
    ici("X", 0, 0, "+-")
    ici("Z", 0, 0, "z")
    hrecv[k] = hsend[k]
    for copy in first[2:]:
        copy.wait()
    for j in range(CHIPS):
        gains[0, j] = long_rows[0:1, SLICE * j : SLICE * (j + 1)]
        gains[1, j] = long_rows[1:2, SLICE * j : SLICE * (j + 1)]
    whole = hidden[...].astype(F32)
    scale_in = lax.rsqrt(jnp.mean(whole * whole, axis=-1, keepdims=True) + EPSILON)
    local[3].wait()
    local[4].wait()

    received(0, hrecv)
    gain = gains[0, k]
    lhs = (hrecv[...].astype(F32) * gain[None]).astype(BF16).reshape(CHIPS * SEQS, SLICE)
    slice_rows = pl.ds(pl.multiple_of(k * SLICE, SLICE), SLICE)

    def turned(device):
        rows = jnp.concatenate([dts[device].astype(F32), jnp.zeros((128 - HEADS, SHARD), F32)], axis=0)
        return jnp.transpose(rows).astype(BF16)

    def partial(weights, at, width):
        product = jnp.dot(lhs, weights, preferred_element_type=F32)
        psend[:, :, at : at + width] = product.astype(BF16).reshape(CHIPS, SEQS, width)

    sibling_own("x")
    partial(xg[slice_rows, :], 0, 640)
    sibling_own("b")
    partial(bg[slice_rows, :], 640, 256)
    sibling_own("d")
    partial(jnp.concatenate([turned(2 * k), turned(2 * k + 1)], axis=0), 896, 128)
    to_chips(1, lambda j: psend.at[j, :, pl.ds(0, 1024)], precv.at[:, :, pl.ds(0, 1024)])
    sibling_own("z")
    partial(zg[slice_rows, :], 1024, 640)
    to_chips(2, lambda j: psend.at[j, :, pl.ds(1024, 640)], precv.at[:, :, pl.ds(1024, 640)])
    precv[k] = psend[k]
    arrived("Z", 0, 1)
    ici("Z", 0, 0, "+-")
    ici("OL", 0, 0, "+-")
    ici("X", 0, 0, "z")
    ici("BC", 0, 0, "z")
    ici("DT", 0, 0, "z")
    share_own("o")
    lm_copy = pltpu.make_async_remote_copy(
        src_ref=lm.at[lm_mine], dst_ref=lm.at[lm_mine], send_sem=loc.at[7], recv_sem=loc.at[8],
        device_id=sibling, device_id_type=MESH,
    )
    lm_copy.start()

    received(1, precv.at[:, :, pl.ds(0, 1024)])
    summed = jnp.sum(precv[:, :, 0:1024].astype(F32), axis=0) * scale_in
    x_new = summed[:, 0:640]
    bc_new = summed[:, 640:896]
    step_raw = summed[:, 896 : 896 + HEADS]
    acc = x_new * conv_wx[3:4, :] + short_rows[0:1, :]
    acc_bc = bc_new * conv_wbc[3:4, :] + conv_bbc[...]
    for tap in range(3):
        acc = acc + conv_x[tap].astype(F32) * conv_wx[tap : tap + 1, :]
        acc_bc = acc_bc + conv_bc[tap].astype(F32) * conv_wbc[tap : tap + 1, :]
    x_conv = silu(acc)
    bc_conv = silu(acc_bc)
    b_rows[...] = bc_conv[:, :N]
    c_vals = bc_conv[:, N:]
    biased = step_raw + dt_bias[...]
    step = jnp.maximum(biased, 0.0) + jnp.log1p(jnp.exp(-jnp.abs(biased)))
    decay = jnp.exp(-step * jnp.exp(a_log[...]))
    square = jnp.concatenate(
        [jnp.concatenate([decay, jnp.zeros((SEQS, 128 - HEADS), F32)], axis=1), jnp.zeros((112, 128), F32)], axis=0
    )
    decays[...] = jnp.transpose(square)[0:SEQS]
    inflow = per_head(step) * x_conv
    x_cols[...] = jnp.transpose(jnp.concatenate([inflow, jnp.zeros((112, DI), F32)], axis=0))
    c_high = c_vals.astype(BF16)
    c_low = (c_vals - c_high.astype(F32)).astype(BF16)
    c_rows[...] = jnp.concatenate([c_high, c_low], axis=0)
    local[5].wait()

    def two_heads(pair, _):
        rows = pl.ds(pl.multiple_of(pair * 128, 128), 128)
        columns = x_cols[rows, :]
        left = decays[pl.ds(2 * pair, 1), :]
        right = decays[pl.ds(2 * pair + 1, 1), :]
        both = c_rows[...]
        row = lax.broadcasted_iota(jnp.int32, (SEQS, N), 0)
        total = jnp.zeros((SEQS, N), F32)
        for s in range(SEQS):
            factor = jnp.concatenate(
                [
                    jnp.broadcast_to(left[:, s : s + 1], (P_SIZE, N)),
                    jnp.broadcast_to(right[:, s : s + 1], (P_SIZE, N)),
                ],
                axis=0,
            )
            column = jnp.broadcast_to(columns[:, s : s + 1], (2 * P_SIZE, N))
            new = state[s, rows, :] * factor + column * b_rows[s : s + 1, :]
            state[s, rows, :] = new
            seen = lax.dot_general(both, new.astype(BF16), (((1,), (1,)), ((), ())), preferred_element_type=F32)
            total = total + jnp.where(row == s, seen[0:SEQS] + seen[SEQS:], 0.0)
        y_acc[:, rows] = total
        return 0

    lax.fori_loop(0, HEADS // 2, two_heads, 0)
    received(2, precv.at[:, :, pl.ds(1024, 640)])
    gate = jnp.sum(precv[:, :, 1024:1664].astype(F32), axis=0) * scale_in
    ssm_out = y_acc[...] + per_head(skip_gain[...]) * x_conv
    gated = ssm_out * silu(gate)
    squares = jnp.sum(gated * gated, axis=-1, keepdims=True)
    gsend[:, 0:640] = (gated * short_rows[1:2, :]).astype(BF16)
    gsend[:, 640:768] = two_parts(squares, 64)

    to_chips(3, lambda j: gsend, grecv)
    grecv[k] = gsend[...]
    arrived("X", 3, 0)
    ici("X", 3, 0, "z+")
    ici("DT", 0, 0, "+-")
    ici("BC", 0, 0, "+-")
    ici("Z", 0, 1, "+-")
    ici("OH", 0, 0, "z")
    arrived("X", 1, 0)

    sibling_own("o")
    received(3, grecv)
    mixed = lax.dot_general(
        grecv[:, :, 0:640].reshape(CHIPS * SEQS, 640), og[slice_rows, :], (((1,), (1,)), ((), ())),
        preferred_element_type=F32,
    )
    parts = grecv[:, :, 640:768].astype(F32)
    sq = (parts[:, :, 0:1] + parts[:, :, 64:65]).reshape(CHIPS * SEQS, 1)
    rsend[:, :, 0:SLICE] = mixed.astype(BF16).reshape(CHIPS, SEQS, SLICE)
    rsend[:, :, SLICE:384] = two_parts(sq, 32).reshape(CHIPS, SEQS, 64)
    to_heads(4, lambda j: rsend.at[j], rrecv)
    rrecv[h] = rsend[h]
    arrived("DT", 0, 1)
    ici("DT", 0, 1, "+-")
    arrived("BC", 0, 1)
    ici("BC", 0, 1, "+-")
    ici("OH", 0, 0, "+-")
    ici("X", 1, 0, "z")
    arrived("Z", 3, 0)
    ici("Z", 3, 0, "+")
    arrived("Z", 1, 0)
    arrived("Z", 1, 1)
    ici("Z", 1, 1, "-")
    received(4, rrecv)
    total = jnp.sum(rrecv[...].astype(F32), axis=0)
    scale_gate = lax.rsqrt((total[:, SLICE : SLICE + 1] + total[:, SLICE + 32 : SLICE + 33]) / (8.0 * DI) + EPSILON)
    stream = hrecv[h].astype(F32) + total[:, 0:SLICE] * scale_gate
    usend[:, 0:SLICE] = (stream * gains[1, k]).astype(BF16)
    usend[:, SLICE:384] = two_parts(jnp.sum(stream * stream, axis=-1, keepdims=True), 32)

    to_heads(5, lambda j: usend, urecv)
    urecv[h] = usend[...]
    arrived("DT", 1, 0)
    ici("DT", 1, 0, "-")
    arrived("DT", 1, 1)
    ici("DT", 1, 1, "-")
    arrived("BC", 3, 0)
    ici("BC", 3, 0, "+")
    arrived("BC", 1, 1)
    ici("BC", 1, 1, "-")
    arrived("OL", 1, 0)
    ici("OL", 1, 0, "-")
    ici("OL", 0, 0, "z")
    arrived("OH", 0, 1)
    ici("OH", 0, 1, "-")
    arrived("OL", 3, 0)
    arrived("X", 0, 1)
    arrived("X", 3, 1)
    arrived("BC", 1, 0)
    arrived("BC", 3, 1)
    arrived("DT", 3, 0)
    arrived("DT", 3, 1)

    local[6].wait()
    pltpu.make_async_remote_copy(
        src_ref=lm.at[lm_other], dst_ref=lm.at[lm_other], send_sem=loc.at[7], recv_sem=loc.at[8],
        device_id=sibling, device_id_type=MESH,
    ).wait_recv()
    received(5, urecv)
    final = urecv[:, :, 0:SLICE].reshape(CHIPS * SEQS, SLICE)

    def some_logits(at, width):
        product = jnp.dot(final, lm[:, at : at + width], preferred_element_type=F32)
        product = product.astype(BF16).reshape(4, 2, SEQS, width)
        for z in range(2):
            lsend[z, :, :, at : at + width] = product[:, z]

    def sum_copy(at, src, dst, device):
        return pltpu.make_async_remote_copy(
            src_ref=src, dst_ref=dst, send_sem=sum_s.at[at], recv_sem=sum_r.at[at], device_id=device,
            device_id_type=MESH,
        )

    partner = (2 * (2 * x + 1 - zl) + c, h)
    across = []
    for part in range(3):
        columns = pl.ds(640 * part, 640)
        some_logits(640 * part, 640)
        copy = sum_copy(part, lsend.at[1 - zl, :, :, columns], zrecv.at[:, :, columns], partner)
        copy.start()
        across.append(copy)
        if part == 0:
            for at in range(CUT, VL, 640):
                some_logits(at, 640)
            for z in range(2):
                for position in range(4):
                    lsend[z, position, :, VL : VL + 64] = urecv[2 * position + z, :, SLICE:384]
                    lsend[z, position, :, VL + 64 : VL + 128] = urecv[2 * position + z, :, SLICE:384]
            for move in (1, 3, 2):
                other = (x + move) % 4
                sum_copy(3, lsend.at[:, other, :, pl.ds(CUT, REST)], xrecv.at[x], (2 * (2 * other + zl) + c, h)).start()

    reference = refs[...].astype(F32)
    ref_max = jnp.max(reference, axis=-1, keepdims=True)
    weight = jnp.exp(reference - ref_max)
    ref_sum = jnp.sum(weight, axis=-1, keepdims=True)
    token = as_column(tokens[...].astype(F32)).astype(jnp.int32)


    def pair_sums(part):
        columns = slice(640 * part, 640 * part + 640)
        across[part].wait_recv()
        summed = lsend[zl, :, :, columns].astype(F32) + zrecv[:, :, columns].astype(F32)
        zsum[:, :, columns] = summed.astype(BF16)
        for move in (2, 1, 3):
            other = (x + move) % 4
            sum_copy(
                4 + part, zsum.at[other, :, pl.ds(640 * part, 640)], total_z.at[x, :, pl.ds(640 * part, 640)],
                (2 * (2 * other + zl) + c, h),
            ).start()
        total_z[x, :, columns] = zsum[x, :, columns]

    pair_sums(0)
    pair_sums(1)
    three = xrecv.at[pl.ds(0, 3)]
    xrecv[x] = lsend[:, x, :, CUT : CUT + REST]
    sum_copy(3, three, three, partner).wait_recv()
    xsum[...] = jnp.sum(xrecv[:, 1 - zl].astype(F32), axis=0).astype(BF16)
    along_z = sum_copy(7, xsum, total_x, partner)
    along_z.start()
    mine = jnp.sum(xrecv[:, zl].astype(F32), axis=0)
    pair_sums(2)

    ici("OH", 0, 1, "+")
    arrived("OH", 1, 1)
    ici("OH", 1, 1, "-")
    arrived("OH", 3, 0)
    ici("OH", 3, 0, "+")
    arrived("X", 2, 0)
    ici("X", 2, 0, "z")
    ici("OL", 1, 0, "z")
    ici("OL", 3, 0, "z")
    arrived("OL", 2, 0)
    ici("OL", 2, 0, "z")
    arrived("BC", 2, 0)
    arrived("BC", 2, 1)
    arrived("X", 1, 1)
    arrived("Z", 3, 1)
    arrived("OH", 1, 0)
    arrived("DT", 2, 0)
    arrived("DT", 2, 1)
    arrived("Z", 2, 0)
    arrived("Z", 2, 1)


    pltpu.make_async_remote_copy(
        src_ref=several("d", 7), dst_ref=several("d", 7), send_sem=d2_s.at[ARRAYS.index("d")],
        recv_sem=d2_r.at[ARRAYS.index("d")], device_id=sibling, device_id_type=MESH,
    ).wait_recv()
    dt_out[...] = jnp.concatenate([dts[device].astype(F32) for device in range(2 * CHIPS)], axis=1).astype(BF16)
    for part in range(3):
        block = total_z.at[pl.ds(0, 3), :, pl.ds(640 * part, 640)]
        sum_copy(4 + part, block, block, partner).wait_recv()
    along_z.wait_recv()
    rest = mine + total_x[...].astype(F32)
    logits = jnp.concatenate([jnp.sum(total_z[...].astype(F32), axis=0), rest[:, 0 : VL - CUT]], axis=1)
    tail = rest[:, VL - CUT :]
    logits = logits * lax.rsqrt((tail[:, 0:1] + tail[:, 32:33]) / D + EPSILON)
    roll_max = jnp.max(logits, axis=-1, keepdims=True)
    roll_sum = jnp.sum(jnp.exp(logits - roll_max), axis=-1, keepdims=True)
    cross = jnp.sum(weight * (reference - logits), axis=-1, keepdims=True)
    column = lax.broadcasted_iota(jnp.int32, (SEQS, VL), 1) + h * VL
    picked = jnp.sum(jnp.where(column == token, logits, 0.0), axis=-1, keepdims=True)
    lane = lax.broadcasted_iota(jnp.int32, (SEQS, 128), 1)
    packed = jnp.zeros((SEQS, 128), F32)
    for at, value in enumerate((roll_max, roll_sum, ref_max, ref_sum, cross, picked)):
        packed = jnp.where(lane == at, jnp.broadcast_to(value, (SEQS, 128)), packed)
    ssend[...] = jnp.transpose(jnp.concatenate([packed, jnp.zeros((128 - SEQS, 128), F32)], axis=0))[0:8]

    to_heads(7, lambda j: ssend, srecv)
    srecv[h] = ssend[...]

    along_y().wait_recv()
    for dz in range(2):
        for dx in range(4):
            if (dx, dz) != (0, 0):
                block = shard_of("b", ((((x + dx) % 4) * 2 + (zl + dz) % 2) * 2 + c))
                on_chip(block, "b", d2_r.at[ARRAYS.index("b")])
    arrived("OL", 0, 1)
    arrived("X", 2, 1)
    arrived("OH", 3, 1)
    arrived("OL", 3, 1)
    arrived("OL", 1, 1)
    arrived("OH", 2, 0)
    arrived("OH", 2, 1)
    arrived("OL", 2, 1)

    received(7, srecv)
    m_all, s_all, rm_all, rs_all, x_all, p_all = (srecv[:, at, :] for at in range(6))
    roll_top = jnp.max(m_all, axis=0, keepdims=True)
    roll_total = jnp.sum(s_all * jnp.exp(m_all - roll_top), axis=0, keepdims=True)
    ref_top = jnp.max(rm_all, axis=0, keepdims=True)
    ref_scale = jnp.exp(rm_all - ref_top)
    ref_total = jnp.sum(rs_all * ref_scale, axis=0, keepdims=True)
    cross_total = jnp.sum(x_all * ref_scale, axis=0, keepdims=True)
    lse_roll = roll_top + jnp.log(roll_total)
    lse_ref = ref_top + jnp.log(ref_total)
    divergence = cross_total / ref_total - lse_ref + lse_roll
    logprob = jnp.sum(p_all, axis=0, keepdims=True) - lse_roll
    div_out[...] = divergence[:, 0:SEQS]
    logprob_out[...] = logprob[:, 0:SEQS]

    for piece in PIECES:
        for dz in range(2):
            for dx in range(4):
                if (dx, dz) != (0, 0) and (piece, dx, dz) not in waited:
                    arrived(piece, dx, dz)
    for at, name in enumerate(ARRAYS):
        sent = bg.at[pl.ds(0, 280)] if name == "b" else several(name, 7)
        copy = pltpu.make_async_remote_copy(
            src_ref=sent, dst_ref=several(name, 7), send_sem=ag_s.at[at], recv_sem=d2_r.at[at], device_id=sibling,
            device_id_type=MESH,
        )
        copy.wait_send()
        if name != "d":
            copy.wait_recv()
    for at, name in enumerate(ARRAYS):
        pltpu.make_async_remote_copy(
            src_ref=several(name, 8), dst_ref=several(name, 8), send_sem=d2_s.at[at], recv_sem=d2_r.at[at],
            device_id=sibling, device_id_type=MESH,
        ).wait_send()
    lm_copy.wait_send()
    for copy in across:
        copy.wait_send()
    along_z.wait_send()
    sum_copy(3, three, three, partner).wait_send()
    for part in range(3):
        block = total_z.at[pl.ds(0, 3), :, pl.ds(640 * part, 640)]
        sum_copy(4 + part, block, block, partner).wait_send()
    along_y().wait_send()
    for copy in pending:
        copy.wait_send()


def write_out(*refs):
    count = len(refs) // 2
    copies = [pltpu.make_async_copy(refs[at], refs[count + at], refs[-1].at[at]) for at in range(count)]
    for copy in copies:
        copy.start()
    for copy in copies:
        copy.wait()


ANY = pl.BlockSpec(memory_space=pl.ANY)
VMEM = pl.BlockSpec(memory_space=pltpu.VMEM)


def shards(
    hidden_in, ssm_state, conv_x_state, conv_bc_state, token_ids, ref_logits, in_z, in_x, in_bc, in_dt, out_t,
    lm_head, conv_wx, conv_bx, conv_wbc, conv_bbc, dt_bias, a_log, skip_gain, norm_in, norm_gain, final_gain,
):
    row = lambda v: v.reshape(1, -1)
    results = (
        ((SEQS, DI, N), F32), ((1, SEQS), F32), ((1, SEQS), F32), ((D, DI), BF16), ((D, DI), BF16), ((D, 256), BF16),
        ((HEADS, D), BF16), ((D, DI), BF16),
    )
    held = pl.pallas_call(
        kernel,
        out_shape=tuple(pltpu.VMEM(shape, dtype) for shape, dtype in results),
        in_specs=[pl.BlockSpec(memory_space=pltpu.HBM)] * 22,
        out_specs=(VMEM,) * len(results),
        scratch_shapes=[
            pltpu.VMEM((2 * CHIPS, HEADS, SHARD), BF16),
            pltpu.VMEM((SLICE, VL), BF16),
            pltpu.VMEM((SEQS, VL), BF16),
            pltpu.VMEM((CHIPS, SEQS, SLICE), BF16),
            pltpu.VMEM((CHIPS, SEQS, SLICE), BF16),
            pltpu.VMEM((2, CHIPS, 1, SLICE), F32),
            pltpu.VMEM((CHIPS, SEQS, 1664), BF16),
            pltpu.VMEM((CHIPS, SEQS, 1664), BF16),
            pltpu.VMEM((SEQS, 768), BF16),
            pltpu.VMEM((CHIPS, SEQS, 768), BF16),
            pltpu.VMEM((CHIPS, SEQS, 384), BF16),
            pltpu.VMEM((CHIPS, SEQS, 384), BF16),
            pltpu.VMEM((SEQS, 384), BF16),
            pltpu.VMEM((CHIPS, SEQS, 384), BF16),
            pltpu.VMEM((2, 4, SEQS, VL + 128), BF16),
            pltpu.VMEM((4, SEQS, CUT), BF16),
            pltpu.VMEM((4, SEQS, CUT), BF16),
            pltpu.VMEM((4, SEQS, CUT), BF16),
            pltpu.VMEM((4, 2, SEQS, REST), BF16),
            pltpu.VMEM((SEQS, REST), BF16),
            pltpu.VMEM((SEQS, REST), BF16),
            pltpu.VMEM((8, 128), F32),
            pltpu.VMEM((CHIPS, 8, 128), F32),
            pltpu.VMEM((SEQS, 128), F32),
            pltpu.VMEM((SEQS, N), F32),
            pltpu.VMEM((DI, 128), F32),
            pltpu.VMEM((2 * SEQS, N), BF16),
            pltpu.VMEM((SEQS, DI), F32),
            pltpu.VMEM((SEQS, D), BF16),
            pltpu.VMEM((3, SEQS, DI), BF16),
            pltpu.VMEM((3, SEQS, 256), BF16),
            pltpu.VMEM((1, SEQS), jnp.int32),
            pltpu.VMEM((4, DI), F32),
            pltpu.VMEM((4, 256), F32),
            pltpu.VMEM((1, 256), F32),
            pltpu.VMEM((1, HEADS), F32),
            pltpu.VMEM((1, HEADS), F32),
            pltpu.VMEM((1, HEADS), F32),
            pltpu.VMEM((2, D), F32),
            pltpu.VMEM((2, DI), F32),
            pltpu.SemaphoreType.DMA((15,)),
            pltpu.SemaphoreType.DMA((9,)),
            pltpu.SemaphoreType.DMA((9,)),
            pltpu.SemaphoreType.DMA((9,)),
            pltpu.SemaphoreType.DMA((5,)),
            pltpu.SemaphoreType.DMA((6, 7)),
            pltpu.SemaphoreType.DMA((5,)),
            pltpu.SemaphoreType.DMA((5,)),
            pltpu.SemaphoreType.DMA((5,)),
            pltpu.SemaphoreType.DMA((2,)),
            pltpu.SemaphoreType.DMA((8,)),
            pltpu.SemaphoreType.DMA((8,)),
        ],
        compiler_params=pltpu.CompilerParams(
            collective_id=0, has_side_effects=True, vmem_limit_bytes=32 * 1024 * 1024
        ),
    )(*[pltpu.with_memory_space_constraint(array, pltpu.HBM) for array in (
        hidden_in, ssm_state.reshape(SEQS, DI, N), conv_x_state.transpose(1, 0, 2), conv_bc_state.transpose(1, 0, 2),
        row(token_ids), ref_logits, in_z, in_x, in_bc, in_dt.T, out_t, lm_head.T,
        conv_wx, conv_bx, conv_wbc, row(conv_bbc), row(dt_bias), row(a_log), row(skip_gain), norm_in,
        norm_gain, final_gain,
    )])
    held = [pltpu.with_memory_space_constraint(array, pltpu.VMEM) for array in held]
    state, divergence, logprob, roll_z, roll_x, roll_bc, dt_rows, roll_out = pl.pallas_call(
        write_out,
        out_shape=tuple(jax.ShapeDtypeStruct(shape, dtype) for shape, dtype in results),
        in_specs=[VMEM] * len(results),
        out_specs=(ANY,) * len(results),
        scratch_shapes=[pltpu.SemaphoreType.DMA((len(results),))],
        compiler_params=pltpu.CompilerParams(vmem_limit_bytes=1024 * 1024),
    )(*held)
    return (
        state.reshape(ssm_state.shape), divergence.reshape(SEQS), logprob.reshape(SEQS), roll_z, roll_x, roll_bc,
        dt_rows.T, roll_out,
    )


def solution(mesh):
    spread = P("group", "head")
    return jax.shard_map(
        shards,
        mesh=mesh,
        in_specs=(
            P("group", None), P("group", "head", None, None), P("group", None, "head"), P("group", None, None),
            P("group"), spread, spread, spread, P("group", None), spread, spread, P("head", "group"),
            P(None, "head"), P("head"), P(), P(), P("head"), P("head"), P("head"), P(), P("head"), P(),
        ),
        out_specs=(
            P("group", "head", None, None), P("group"), P("group"), P(None, "head"), P(None, "head"), P(),
            P(None, "head"), P(None, "head"),
        ),
        check_vma=False,
    )
```

```python
import functools

import jax
import jax.numpy as jnp
from jax import lax
from jax.experimental import pallas as pl
from jax.experimental.pallas import tpu as pltpu
from jax.sharding import PartitionSpec as P

MESH = pl.DeviceIdType.MESH
EPSILON = 1e-05
SEQS, D, DI, HEADS, P_SIZE, N = 16, 2560, 640, 10, 64, 128
SHARD = 160
SLICE = 320
CHIPS = 8
VL = 3200
CUT = 1920
REST = VL + 128 - CUT
F32 = jnp.float32
BF16 = jnp.bfloat16

PIECES = {
    "X": ("x", 0, 160),
    "OL": ("o", 0, 32),
    "DT": ("d", 0, 160),
    "Z": ("z", 0, 160),
    "BC": ("b", 0, 160),
    "OH": ("o", 32, 128),
}
ORDER = {name: at for at, name in enumerate(PIECES)}
ARRAYS = "xobdz"


def silu(v):
    return v / (1.0 + jnp.exp(-v))


def per_head(values):
    rows = values.shape[0]
    lane = lax.broadcasted_iota(jnp.int32, (rows, 128), 1)
    parts = []
    for pair in range(HEADS // 2):
        left = jnp.broadcast_to(values[:, 2 * pair : 2 * pair + 1], (rows, 128))
        right = jnp.broadcast_to(values[:, 2 * pair + 1 : 2 * pair + 2], (rows, 128))
        parts.append(jnp.where(lane < P_SIZE, left, right))
    return jnp.concatenate(parts, axis=1)


def as_column(row):
    r = lax.broadcasted_iota(jnp.int32, (SEQS, SEQS), 0)
    c = lax.broadcasted_iota(jnp.int32, (SEQS, SEQS), 1)
    return jnp.sum(jnp.where(r == c, jnp.broadcast_to(row, (SEQS, SEQS)), 0.0), axis=1, keepdims=True)


def two_parts(values, width):
    high = values.astype(BF16).astype(F32)
    rows = values.shape[0]
    lane = lax.broadcasted_iota(jnp.int32, (rows, 2 * width), 1)
    return jnp.where(
        lane < width, jnp.broadcast_to(high, (rows, 2 * width)), jnp.broadcast_to(values - high, (rows, 2 * width))
    ).astype(BF16)


def kernel(
    hidden_in, state_in, conv_x_in, conv_bc_in, tokens_in, ref_in, in_z, in_x, in_bc, dt_in, out_t, lm_in,
    conv_wx_in, conv_bx, conv_wbc_in, conv_bbc_in, dt_bias_in, a_log_in, skip_in, norm_in, norm_gain, final_gain,
    state, div_out, logprob_out, zg, xg, bg, dt_out, og,
    dts, lm, refs, hsend, hrecv, gains, psend, precv, gsend, grecv, rsend, rrecv, usend, urecv, lsend, zrecv, zsum, total_z, xrecv, xsum, total_x,
    ssend, srecv, decays, b_rows, x_cols, c_rows, y_acc,
    hidden, conv_x, conv_bc, tokens, conv_wx, conv_wbc, conv_bbc, dt_bias, a_log, skip_gain,
    long_rows, short_rows, small, loc, chain_s, chain_r, ag_s, ag_r, d2_s, d2_own, d2_r, y_sems, sum_s, sum_r,
):
    g = lax.axis_index("group")
    h = lax.axis_index("head")
    k = g // 2
    c = g % 2
    x = k // 2
    zl = k % 2
    y = h // 2
    sibling = (2 * k + 1 - c, h)

    barrier = pltpu.get_barrier_semaphore()
    for d in range(1, 8):
        pl.semaphore_signal(barrier, inc=1, device_id=(g, (h + d) % 8), device_id_type=MESH)
        pl.semaphore_signal(barrier, inc=1, device_id=(2 * ((k + d) % 8) + c, h), device_id_type=MESH)
    pl.semaphore_signal(barrier, inc=1, device_id=sibling, device_id_type=MESH)

    rows_mine = pl.ds(pl.multiple_of(g * SHARD, SHARD), SHARD)
    lm_mine = pl.ds(pl.multiple_of(c * SHARD, SHARD), SHARD)
    lm_other = pl.ds(pl.multiple_of((1 - c) * SHARD, SHARD), SHARD)
    first = [
        pltpu.make_async_copy(source, target, small.at[at])
        for at, (source, target) in enumerate(
            [
                (hidden_in, hidden), (dt_in, dts.at[g]), (norm_in, long_rows.at[0]), (final_gain, long_rows.at[1]),
                (conv_x_in, conv_x), (conv_bc_in, conv_bc), (tokens_in, tokens), (conv_wx_in, conv_wx),
                (conv_wbc_in, conv_wbc), (conv_bbc_in, conv_bbc), (dt_bias_in, dt_bias), (a_log_in, a_log),
                (skip_in, skip_gain), (conv_bx, short_rows.at[0]), (norm_gain, short_rows.at[1]),
            ]
        )
    ]
    local = [
        pltpu.make_async_copy(source, target, loc.at[at])
        for at, (source, target) in enumerate(
            [
                (in_x, xg.at[rows_mine]), (in_bc, bg.at[rows_mine]), (in_z, zg.at[rows_mine]),
                (out_t, og.at[rows_mine]), (lm_in, lm.at[lm_mine]), (state_in, state), (ref_in, refs),
            ]
        )
    ]
    for copy in first + local:
        copy.start()
    first[0].wait()

    for j in range(CHIPS):
        hsend[j] = hidden[:, SLICE * j : SLICE * (j + 1)]

    pl.semaphore_wait(barrier, 15)

    def chain_copy(phase, src, dst, device):
        return pltpu.make_async_remote_copy(
            src_ref=src, dst_ref=dst, send_sem=chain_s.at[phase], recv_sem=chain_r.at[phase],
            device_id=device, device_id_type=MESH,
        )

    pending = []

    def to_chips(phase, send_slot, recv):
        for d in range(1, 8):
            j = (k + d) % 8
            chain_copy(phase, send_slot(j), recv.at[k], (2 * j + c, h)).start()
        pending.append(chain_copy(phase, recv.at[pl.ds(0, 7)], recv.at[pl.ds(0, 7)], sibling))

    def to_heads(phase, send_slot, recv):
        for d in range(1, 8):
            j = (h + d) % 8
            chain_copy(phase, send_slot(j), recv.at[h], (g, j)).start()
        pending.append(chain_copy(phase, recv.at[pl.ds(0, 7)], recv.at[pl.ds(0, 7)], sibling))

    def received(phase, recv):
        chain_copy(phase, recv.at[pl.ds(0, 7)], recv.at[pl.ds(0, 7)], sibling).wait_recv()

    buffers = {"x": xg, "z": zg, "o": og, "b": bg, "d": dts}

    def quarter(device):
        at = pl.multiple_of(device * SHARD + 80 * (y // 2), 16)
        return bg.at[pl.ds(at, 80), pl.ds(pl.multiple_of(128 * (y % 2), 128), 128)]

    def region(piece, dx, dz, core):
        name, begin, rows = PIECES[piece]
        at = (((x + dx) % 4) * 2 + (zl + dz) % 2) * 2 + core
        if name == "d":
            return dts.at[at]
        if name == "b":
            return quarter(at)
        at = at * SHARD + begin
        return buffers[name].at[pl.ds(pl.multiple_of(at, 16), rows)]

    def ici(piece, dx, dz, ways):
        for way in ways:
            move = {"+": 1, "-": 3, "z": 0}[way]
            rx, rz = (dx - move) % 4, (dz + (way == "z")) % 2
            chip = ((x + move) % 4) * 2 + (zl + (way == "z")) % 2
            block = region(piece, dx, dz, c)
            pltpu.make_async_remote_copy(
                src_ref=block, dst_ref=block, send_sem=ag_s.at[ARRAYS.index(PIECES[piece][0])],
                recv_sem=ag_r.at[ORDER[piece], 4 * rz + rx - 1], device_id=(2 * chip + c, h), device_id_type=MESH,
            ).start()

    def on_chip(block, name, sem):
        pltpu.make_async_remote_copy(
            src_ref=block, dst_ref=block, send_sem=d2_s.at[ARRAYS.index(name)], recv_sem=sem,
            device_id=sibling, device_id_type=MESH,
        ).start()

    def shard_of(name, device):
        if name == "d":
            return dts.at[device]
        return buffers[name].at[pl.ds(pl.multiple_of(device * SHARD, SHARD), SHARD)]

    def along_y():
        return pltpu.make_async_remote_copy(
            src_ref=bg.at[pl.ds(0, 840)], dst_ref=bg.at[pl.ds(0, 840)], send_sem=y_sems.at[0], recv_sem=y_sems.at[1],
            device_id=sibling, device_id_type=MESH,
        )

    def several(name, shards):
        return buffers[name].at[pl.ds(0, shards if name == "d" else shards * SHARD)]

    def share_own(name):
        on_chip(shard_of(name, g), name, d2_own.at[ARRAYS.index(name)])

    def sibling_own(name):
        rows = shard_of(name, 2 * k + 1 - c)
        pltpu.make_async_remote_copy(
            src_ref=rows, dst_ref=rows, send_sem=d2_s.at[ARRAYS.index(name)], recv_sem=d2_own.at[ARRAYS.index(name)],
            device_id=sibling, device_id_type=MESH,
        ).wait_recv()

    waited = set()

    def arrived(piece, dx, dz):
        block = region(piece, dx, dz, c)
        name = PIECES[piece][0]
        pltpu.make_async_remote_copy(
            src_ref=block, dst_ref=block, send_sem=d2_s.at[ARRAYS.index(name)],
            recv_sem=ag_r.at[ORDER[piece], 4 * dz + dx - 1], device_id=sibling, device_id_type=MESH,
        ).wait_recv()
        waited.add((piece, dx, dz))
        if name == "b":
            for move in range(1, 4):
                pltpu.make_async_remote_copy(
                    src_ref=block, dst_ref=block, send_sem=y_sems.at[0], recv_sem=y_sems.at[1],
                    device_id=(g, (h + 2 * move) % 8), device_id_type=MESH,
                ).start()
            return
        on_chip(block, name, d2_r.at[ARRAYS.index(name)])

    to_chips(0, lambda j: hsend.at[j], hrecv)
    local[0].wait()
    share_own("x")
    local[1].wait()
    share_own("b")
    local[2].wait()
    share_own("z")
    first[1].wait()
    share_own("d")
    ici("X", 0, 0, "+-")
    ici("Z", 0, 0, "z")
    hrecv[k] = hsend[k]
    for copy in first[2:]:
        copy.wait()
    for j in range(CHIPS):
        gains[0, j] = long_rows[0:1, SLICE * j : SLICE * (j + 1)]
        gains[1, j] = long_rows[1:2, SLICE * j : SLICE * (j + 1)]
    whole = hidden[...].astype(F32)
    scale_in = lax.rsqrt(jnp.mean(whole * whole, axis=-1, keepdims=True) + EPSILON)
    local[3].wait()
    local[4].wait()

    received(0, hrecv)
    gain = gains[0, k]
    lhs = (hrecv[...].astype(F32) * gain[None]).astype(BF16).reshape(CHIPS * SEQS, SLICE)
    slice_rows = pl.ds(pl.multiple_of(k * SLICE, SLICE), SLICE)

    def turned(device):
        rows = jnp.concatenate([dts[device].astype(F32), jnp.zeros((128 - HEADS, SHARD), F32)], axis=0)
        return jnp.transpose(rows).astype(BF16)

    def partial(weights, at, width):
        product = jnp.dot(lhs, weights, preferred_element_type=F32)
        psend[:, :, at : at + width] = product.astype(BF16).reshape(CHIPS, SEQS, width)

    sibling_own("x")
    partial(xg[slice_rows, :], 0, 640)
    sibling_own("b")
    partial(bg[slice_rows, :], 640, 256)
    sibling_own("d")
    partial(jnp.concatenate([turned(2 * k), turned(2 * k + 1)], axis=0), 896, 128)
    to_chips(1, lambda j: psend.at[j, :, pl.ds(0, 1024)], precv.at[:, :, pl.ds(0, 1024)])
    sibling_own("z")
    partial(zg[slice_rows, :], 1024, 640)
    to_chips(2, lambda j: psend.at[j, :, pl.ds(1024, 640)], precv.at[:, :, pl.ds(1024, 640)])
    precv[k] = psend[k]
    arrived("Z", 0, 1)
    ici("Z", 0, 0, "+-")
    ici("OL", 0, 0, "+-")
    ici("X", 0, 0, "z")
    ici("BC", 0, 0, "z")
    ici("DT", 0, 0, "z")
    share_own("o")
    lm_copy = pltpu.make_async_remote_copy(
        src_ref=lm.at[lm_mine], dst_ref=lm.at[lm_mine], send_sem=loc.at[7], recv_sem=loc.at[8],
        device_id=sibling, device_id_type=MESH,
    )
    lm_copy.start()

    received(1, precv.at[:, :, pl.ds(0, 1024)])
    summed = jnp.sum(precv[:, :, 0:1024].astype(F32), axis=0) * scale_in
    x_new = summed[:, 0:640]
    bc_new = summed[:, 640:896]
    step_raw = summed[:, 896 : 896 + HEADS]
    acc = x_new * conv_wx[3:4, :] + short_rows[0:1, :]
    acc_bc = bc_new * conv_wbc[3:4, :] + conv_bbc[...]
    for tap in range(3):
        acc = acc + conv_x[tap].astype(F32) * conv_wx[tap : tap + 1, :]
        acc_bc = acc_bc + conv_bc[tap].astype(F32) * conv_wbc[tap : tap + 1, :]
    x_conv = silu(acc)
    bc_conv = silu(acc_bc)
    b_rows[...] = bc_conv[:, :N]
    c_vals = bc_conv[:, N:]
    biased = step_raw + dt_bias[...]
    step = jnp.maximum(biased, 0.0) + jnp.log1p(jnp.exp(-jnp.abs(biased)))
    decay = jnp.exp(-step * jnp.exp(a_log[...]))
    square = jnp.concatenate(
        [jnp.concatenate([decay, jnp.zeros((SEQS, 128 - HEADS), F32)], axis=1), jnp.zeros((112, 128), F32)], axis=0
    )
    decays[...] = jnp.transpose(square)[0:SEQS]
    inflow = per_head(step) * x_conv
    x_cols[...] = jnp.transpose(jnp.concatenate([inflow, jnp.zeros((112, DI), F32)], axis=0))
    c_high = c_vals.astype(BF16)
    c_low = (c_vals - c_high.astype(F32)).astype(BF16)
    c_rows[...] = jnp.concatenate([c_high, c_low], axis=0)
    local[5].wait()

    def two_heads(pair, _):
        rows = pl.ds(pl.multiple_of(pair * 128, 128), 128)
        columns = x_cols[rows, :]
        left = decays[pl.ds(2 * pair, 1), :]
        right = decays[pl.ds(2 * pair + 1, 1), :]
        both = c_rows[...]
        row = lax.broadcasted_iota(jnp.int32, (SEQS, N), 0)
        total = jnp.zeros((SEQS, N), F32)
        for s in range(SEQS):
            factor = jnp.concatenate(
                [
                    jnp.broadcast_to(left[:, s : s + 1], (P_SIZE, N)),
                    jnp.broadcast_to(right[:, s : s + 1], (P_SIZE, N)),
                ],
                axis=0,
            )
            column = jnp.broadcast_to(columns[:, s : s + 1], (2 * P_SIZE, N))
            new = state[s, rows, :] * factor + column * b_rows[s : s + 1, :]
            state[s, rows, :] = new
            seen = lax.dot_general(both, new.astype(BF16), (((1,), (1,)), ((), ())), preferred_element_type=F32)
            total = total + jnp.where(row == s, seen[0:SEQS] + seen[SEQS:], 0.0)
        y_acc[:, rows] = total
        return 0

    lax.fori_loop(0, HEADS // 2, two_heads, 0)
    received(2, precv.at[:, :, pl.ds(1024, 640)])
    gate = jnp.sum(precv[:, :, 1024:1664].astype(F32), axis=0) * scale_in
    ssm_out = y_acc[...] + per_head(skip_gain[...]) * x_conv
    gated = ssm_out * silu(gate)
    gsend[...] = gated.astype(BF16)

    to_chips(3, lambda j: gsend, grecv)
    grecv[k] = gsend[...]
    arrived("X", 3, 0)
    ici("X", 3, 0, "z+")
    ici("DT", 0, 0, "+-")
    ici("BC", 0, 0, "+-")
    ici("Z", 0, 1, "+-")
    ici("OH", 0, 0, "z")
    arrived("X", 1, 0)

    sibling_own("o")
    received(3, grecv)
    values = grecv[...].astype(F32).reshape(CHIPS * SEQS, DI)
    mixed = lax.dot_general(
        (values * short_rows[1:2, :]).astype(BF16), og[slice_rows, :], (((1,), (1,)), ((), ())),
        preferred_element_type=F32,
    )
    sq = jnp.sum(values * values, axis=-1, keepdims=True)
    rsend[:, :, 0:SLICE] = mixed.astype(BF16).reshape(CHIPS, SEQS, SLICE)
    rsend[:, :, SLICE:384] = two_parts(sq, 32).reshape(CHIPS, SEQS, 64)
    to_heads(4, lambda j: rsend.at[j], rrecv)
    rrecv[h] = rsend[h]
    arrived("DT", 0, 1)
    ici("DT", 0, 1, "+-")
    arrived("BC", 0, 1)
    ici("BC", 0, 1, "+-")
    ici("OH", 0, 0, "+-")
    ici("X", 1, 0, "z")
    arrived("Z", 3, 0)
    ici("Z", 3, 0, "+")
    arrived("Z", 1, 0)
    arrived("Z", 1, 1)
    ici("Z", 1, 1, "-")
    received(4, rrecv)
    total = jnp.sum(rrecv[...].astype(F32), axis=0)
    scale_gate = lax.rsqrt((total[:, SLICE : SLICE + 1] + total[:, SLICE + 32 : SLICE + 33]) / (8.0 * DI) + EPSILON)
    stream = hrecv[h].astype(F32) + total[:, 0:SLICE] * scale_gate
    usend[:, 0:SLICE] = (stream * gains[1, k]).astype(BF16)
    usend[:, SLICE:384] = two_parts(jnp.sum(stream * stream, axis=-1, keepdims=True), 32)

    to_heads(5, lambda j: usend, urecv)
    urecv[h] = usend[...]
    arrived("DT", 1, 0)
    ici("DT", 1, 0, "-")
    arrived("DT", 1, 1)
    ici("DT", 1, 1, "-")
    arrived("BC", 3, 0)
    ici("BC", 3, 0, "+")
    arrived("BC", 1, 1)
    ici("BC", 1, 1, "-")
    arrived("OL", 1, 0)
    ici("OL", 1, 0, "-")
    ici("OL", 0, 0, "z")
    arrived("OH", 0, 1)
    ici("OH", 0, 1, "-")
    arrived("OL", 3, 0)
    arrived("X", 0, 1)
    arrived("X", 3, 1)
    arrived("BC", 1, 0)
    arrived("BC", 3, 1)
    arrived("DT", 3, 0)
    arrived("DT", 3, 1)

    local[6].wait()
    pltpu.make_async_remote_copy(
        src_ref=lm.at[lm_other], dst_ref=lm.at[lm_other], send_sem=loc.at[7], recv_sem=loc.at[8],
        device_id=sibling, device_id_type=MESH,
    ).wait_recv()
    received(5, urecv)
    final = urecv[:, :, 0:SLICE].reshape(CHIPS * SEQS, SLICE)

    def some_logits(at, width):
        product = jnp.dot(final, lm[:, at : at + width], preferred_element_type=F32)
        product = product.astype(BF16).reshape(4, 2, SEQS, width)
        for z in range(2):
            lsend[z, :, :, at : at + width] = product[:, z]

    def sum_copy(at, src, dst, device):
        return pltpu.make_async_remote_copy(
            src_ref=src, dst_ref=dst, send_sem=sum_s.at[at], recv_sem=sum_r.at[at], device_id=device,
            device_id_type=MESH,
        )

    partner = (2 * (2 * x + 1 - zl) + c, h)
    across = []
    for part in range(3):
        columns = pl.ds(640 * part, 640)
        some_logits(640 * part, 640)
        copy = sum_copy(part, lsend.at[1 - zl, :, :, columns], zrecv.at[:, :, columns], partner)
        copy.start()
        across.append(copy)
        if part == 0:
            for at in range(CUT, VL, 640):
                some_logits(at, 640)
            for z in range(2):
                for position in range(4):
                    lsend[z, position, :, VL : VL + 64] = urecv[2 * position + z, :, SLICE:384]
                    lsend[z, position, :, VL + 64 : VL + 128] = urecv[2 * position + z, :, SLICE:384]
            for move in (1, 3, 2):
                other = (x + move) % 4
                sum_copy(3, lsend.at[:, other, :, pl.ds(CUT, REST)], xrecv.at[x], (2 * (2 * other + zl) + c, h)).start()

    reference = refs[...].astype(F32)
    ref_max = jnp.max(reference, axis=-1, keepdims=True)
    weight = jnp.exp(reference - ref_max)
    ref_sum = jnp.sum(weight, axis=-1, keepdims=True)
    token = as_column(tokens[...].astype(F32)).astype(jnp.int32)


    def pair_sums(part):
        columns = slice(640 * part, 640 * part + 640)
        across[part].wait_recv()
        summed = lsend[zl, :, :, columns].astype(F32) + zrecv[:, :, columns].astype(F32)
        zsum[:, :, columns] = summed.astype(BF16)
        for move in (2, 1, 3):
            other = (x + move) % 4
            sum_copy(
                4 + part, zsum.at[other, :, pl.ds(640 * part, 640)], total_z.at[x, :, pl.ds(640 * part, 640)],
                (2 * (2 * other + zl) + c, h),
            ).start()
        total_z[x, :, columns] = zsum[x, :, columns]

    pair_sums(0)
    pair_sums(1)
    three = xrecv.at[pl.ds(0, 3)]
    xrecv[x] = lsend[:, x, :, CUT : CUT + REST]
    sum_copy(3, three, three, partner).wait_recv()
    xsum[...] = jnp.sum(xrecv[:, 1 - zl].astype(F32), axis=0).astype(BF16)
    along_z = sum_copy(7, xsum, total_x, partner)
    along_z.start()
    mine = jnp.sum(xrecv[:, zl].astype(F32), axis=0)
    pair_sums(2)

    ici("OH", 0, 1, "+")
    arrived("OH", 1, 1)
    ici("OH", 1, 1, "-")
    arrived("OH", 3, 0)
    ici("OH", 3, 0, "+")
    arrived("X", 2, 0)
    ici("X", 2, 0, "z")
    ici("OL", 1, 0, "z")
    ici("OL", 3, 0, "z")
    arrived("OL", 2, 0)
    ici("OL", 2, 0, "z")
    arrived("BC", 2, 0)
    arrived("BC", 2, 1)
    arrived("X", 1, 1)
    arrived("Z", 3, 1)
    arrived("OH", 1, 0)
    arrived("DT", 2, 0)
    arrived("DT", 2, 1)
    arrived("Z", 2, 0)
    arrived("Z", 2, 1)


    pltpu.make_async_remote_copy(
        src_ref=several("d", 7), dst_ref=several("d", 7), send_sem=d2_s.at[ARRAYS.index("d")],
        recv_sem=d2_r.at[ARRAYS.index("d")], device_id=sibling, device_id_type=MESH,
    ).wait_recv()
    dt_out[...] = jnp.concatenate([dts[device].astype(F32) for device in range(2 * CHIPS)], axis=1).astype(BF16)
    for part in range(3):
        block = total_z.at[pl.ds(0, 3), :, pl.ds(640 * part, 640)]
        sum_copy(4 + part, block, block, partner).wait_recv()
    along_z.wait_recv()
    rest = mine + total_x[...].astype(F32)
    logits = jnp.concatenate([jnp.sum(total_z[...].astype(F32), axis=0), rest[:, 0 : VL - CUT]], axis=1)
    tail = rest[:, VL - CUT :]
    logits = logits * lax.rsqrt((tail[:, 0:1] + tail[:, 32:33]) / D + EPSILON)
    roll_max = jnp.max(logits, axis=-1, keepdims=True)
    roll_sum = jnp.sum(jnp.exp(logits - roll_max), axis=-1, keepdims=True)
    cross = jnp.sum(weight * (reference - logits), axis=-1, keepdims=True)
    column = lax.broadcasted_iota(jnp.int32, (SEQS, VL), 1) + h * VL
    picked = jnp.sum(jnp.where(column == token, logits, 0.0), axis=-1, keepdims=True)
    lane = lax.broadcasted_iota(jnp.int32, (SEQS, 128), 1)
    packed = jnp.zeros((SEQS, 128), F32)
    for at, value in enumerate((roll_max, roll_sum, ref_max, ref_sum, cross, picked)):
        packed = jnp.where(lane == at, jnp.broadcast_to(value, (SEQS, 128)), packed)
    ssend[...] = jnp.transpose(jnp.concatenate([packed, jnp.zeros((128 - SEQS, 128), F32)], axis=0))[0:8]

    to_heads(7, lambda j: ssend, srecv)
    srecv[h] = ssend[...]

    along_y().wait_recv()
    for dz in range(2):
        for dx in range(4):
            if (dx, dz) != (0, 0):
                block = shard_of("b", ((((x + dx) % 4) * 2 + (zl + dz) % 2) * 2 + c))
                on_chip(block, "b", d2_r.at[ARRAYS.index("b")])
    arrived("OL", 0, 1)
    arrived("X", 2, 1)
    arrived("OH", 3, 1)
    arrived("OL", 3, 1)
    arrived("OL", 1, 1)
    arrived("OH", 2, 0)
    arrived("OH", 2, 1)
    arrived("OL", 2, 1)

    received(7, srecv)
    m_all, s_all, rm_all, rs_all, x_all, p_all = (srecv[:, at, :] for at in range(6))
    roll_top = jnp.max(m_all, axis=0, keepdims=True)
    roll_total = jnp.sum(s_all * jnp.exp(m_all - roll_top), axis=0, keepdims=True)
    ref_top = jnp.max(rm_all, axis=0, keepdims=True)
    ref_scale = jnp.exp(rm_all - ref_top)
    ref_total = jnp.sum(rs_all * ref_scale, axis=0, keepdims=True)
    cross_total = jnp.sum(x_all * ref_scale, axis=0, keepdims=True)
    lse_roll = roll_top + jnp.log(roll_total)
    lse_ref = ref_top + jnp.log(ref_total)
    divergence = cross_total / ref_total - lse_ref + lse_roll
    logprob = jnp.sum(p_all, axis=0, keepdims=True) - lse_roll
    div_out[...] = divergence[:, 0:SEQS]
    logprob_out[...] = logprob[:, 0:SEQS]

    for piece in PIECES:
        for dz in range(2):
            for dx in range(4):
                if (dx, dz) != (0, 0) and (piece, dx, dz) not in waited:
                    arrived(piece, dx, dz)
    for at, name in enumerate(ARRAYS):
        sent = bg.at[pl.ds(0, 280)] if name == "b" else several(name, 7)
        copy = pltpu.make_async_remote_copy(
            src_ref=sent, dst_ref=several(name, 7), send_sem=ag_s.at[at], recv_sem=d2_r.at[at], device_id=sibling,
            device_id_type=MESH,
        )
        copy.wait_send()
        if name != "d":
            copy.wait_recv()
    for at, name in enumerate(ARRAYS):
        pltpu.make_async_remote_copy(
            src_ref=several(name, 8), dst_ref=several(name, 8), send_sem=d2_s.at[at], recv_sem=d2_r.at[at],
            device_id=sibling, device_id_type=MESH,
        ).wait_send()
    lm_copy.wait_send()
    for copy in across:
        copy.wait_send()
    along_z.wait_send()
    sum_copy(3, three, three, partner).wait_send()
    for part in range(3):
        block = total_z.at[pl.ds(0, 3), :, pl.ds(640 * part, 640)]
        sum_copy(4 + part, block, block, partner).wait_send()
    along_y().wait_send()
    for copy in pending:
        copy.wait_send()


def write_out(*refs):
    count = len(refs) // 2
    copies = [pltpu.make_async_copy(refs[at], refs[count + at], refs[-1].at[at]) for at in range(count)]
    for copy in copies:
        copy.start()
    for copy in copies:
        copy.wait()


ANY = pl.BlockSpec(memory_space=pl.ANY)
VMEM = pl.BlockSpec(memory_space=pltpu.VMEM)


def shards(
    hidden_in, ssm_state, conv_x_state, conv_bc_state, token_ids, ref_logits, in_z, in_x, in_bc, in_dt, out_t,
    lm_head, conv_wx, conv_bx, conv_wbc, conv_bbc, dt_bias, a_log, skip_gain, norm_in, norm_gain, final_gain,
):
    row = lambda v: v.reshape(1, -1)
    results = (
        ((SEQS, DI, N), F32), ((1, SEQS), F32), ((1, SEQS), F32), ((D, DI), BF16), ((D, DI), BF16), ((D, 256), BF16),
        ((HEADS, D), BF16), ((D, DI), BF16),
    )
    held = pl.pallas_call(
        kernel,
        out_shape=tuple(pltpu.VMEM(shape, dtype) for shape, dtype in results),
        in_specs=[pl.BlockSpec(memory_space=pltpu.HBM)] * 22,
        out_specs=(VMEM,) * len(results),
        scratch_shapes=[
            pltpu.VMEM((2 * CHIPS, HEADS, SHARD), BF16),
            pltpu.VMEM((SLICE, VL), BF16),
            pltpu.VMEM((SEQS, VL), BF16),
            pltpu.VMEM((CHIPS, SEQS, SLICE), BF16),
            pltpu.VMEM((CHIPS, SEQS, SLICE), BF16),
            pltpu.VMEM((2, CHIPS, 1, SLICE), F32),
            pltpu.VMEM((CHIPS, SEQS, 1664), BF16),
            pltpu.VMEM((CHIPS, SEQS, 1664), BF16),
            pltpu.VMEM((SEQS, DI), BF16),
            pltpu.VMEM((CHIPS, SEQS, DI), BF16),
            pltpu.VMEM((CHIPS, SEQS, 384), BF16),
            pltpu.VMEM((CHIPS, SEQS, 384), BF16),
            pltpu.VMEM((SEQS, 384), BF16),
            pltpu.VMEM((CHIPS, SEQS, 384), BF16),
            pltpu.VMEM((2, 4, SEQS, VL + 128), BF16),
            pltpu.VMEM((4, SEQS, CUT), BF16),
            pltpu.VMEM((4, SEQS, CUT), BF16),
            pltpu.VMEM((4, SEQS, CUT), BF16),
            pltpu.VMEM((4, 2, SEQS, REST), BF16),
            pltpu.VMEM((SEQS, REST), BF16),
            pltpu.VMEM((SEQS, REST), BF16),
            pltpu.VMEM((8, 128), F32),
            pltpu.VMEM((CHIPS, 8, 128), F32),
            pltpu.VMEM((SEQS, 128), F32),
            pltpu.VMEM((SEQS, N), F32),
            pltpu.VMEM((DI, 128), F32),
            pltpu.VMEM((2 * SEQS, N), BF16),
            pltpu.VMEM((SEQS, DI), F32),
            pltpu.VMEM((SEQS, D), BF16),
            pltpu.VMEM((3, SEQS, DI), BF16),
            pltpu.VMEM((3, SEQS, 256), BF16),
            pltpu.VMEM((1, SEQS), jnp.int32),
            pltpu.VMEM((4, DI), F32),
            pltpu.VMEM((4, 256), F32),
            pltpu.VMEM((1, 256), F32),
            pltpu.VMEM((1, HEADS), F32),
            pltpu.VMEM((1, HEADS), F32),
            pltpu.VMEM((1, HEADS), F32),
            pltpu.VMEM((2, D), F32),
            pltpu.VMEM((2, DI), F32),
            pltpu.SemaphoreType.DMA((15,)),
            pltpu.SemaphoreType.DMA((9,)),
            pltpu.SemaphoreType.DMA((9,)),
            pltpu.SemaphoreType.DMA((9,)),
            pltpu.SemaphoreType.DMA((5,)),
            pltpu.SemaphoreType.DMA((6, 7)),
            pltpu.SemaphoreType.DMA((5,)),
            pltpu.SemaphoreType.DMA((5,)),
            pltpu.SemaphoreType.DMA((5,)),
            pltpu.SemaphoreType.DMA((2,)),
            pltpu.SemaphoreType.DMA((8,)),
            pltpu.SemaphoreType.DMA((8,)),
        ],
        compiler_params=pltpu.CompilerParams(
            collective_id=0, has_side_effects=True, vmem_limit_bytes=32 * 1024 * 1024
        ),
    )(*[pltpu.with_memory_space_constraint(array, pltpu.HBM) for array in (
        hidden_in, ssm_state.reshape(SEQS, DI, N), conv_x_state.transpose(1, 0, 2), conv_bc_state.transpose(1, 0, 2),
        row(token_ids), ref_logits, in_z, in_x, in_bc, in_dt.T, out_t, lm_head.T,
        conv_wx, conv_bx, conv_wbc, row(conv_bbc), row(dt_bias), row(a_log), row(skip_gain), norm_in,
        norm_gain, final_gain,
    )])
    held = [pltpu.with_memory_space_constraint(array, pltpu.VMEM) for array in held]
    state, divergence, logprob, roll_z, roll_x, roll_bc, dt_rows, roll_out = pl.pallas_call(
        write_out,
        out_shape=tuple(jax.ShapeDtypeStruct(shape, dtype) for shape, dtype in results),
        in_specs=[VMEM] * len(results),
        out_specs=(ANY,) * len(results),
        scratch_shapes=[pltpu.SemaphoreType.DMA((len(results),))],
        compiler_params=pltpu.CompilerParams(vmem_limit_bytes=1024 * 1024),
    )(*held)
    return (
        state.reshape(ssm_state.shape), divergence.reshape(SEQS), logprob.reshape(SEQS), roll_z, roll_x, roll_bc,
        dt_rows.T, roll_out,
    )


def solution(mesh):
    spread = P("group", "head")
    return jax.shard_map(
        shards,
        mesh=mesh,
        in_specs=(
            P("group", None), P("group", "head", None, None), P("group", None, "head"), P("group", None, None),
            P("group"), spread, spread, spread, P("group", None), spread, spread, P("head", "group"),
            P(None, "head"), P("head"), P(), P(), P("head"), P("head"), P("head"), P(), P("head"), P(),
        ),
        out_specs=(
            P("group", "head", None, None), P("group"), P("group"), P(None, "head"), P(None, "head"), P(),
            P(None, "head"), P(None, "head"),
        ),
        check_vma=False,
    )
```
